32 devices in a mesh: rows: 32 (over z, y, x, core).
Axes of the slice: x: 2, y: 2, z: 4, core: 2. Of those that a mesh axis runs over, the one named last changes fastest.
Arguments:
- right_side: float32 [9, 4096], P(None, 'rows'), may hold values from -30 to 30
- diag_blocks: float32 [9, 9, 4096], P(None, None, 'rows'), may hold values from -40 to 45, as said below
- precond: float32 [9, 9, 4096], P(None, None, 'rows'), may hold values from -5 to 5, as said below
- upper_blocks: float32 [8, 9, 9, 4096], P(None, None, None, 'rows'), may hold values from -0.21875 to 0.21875
- block_cols: int32 [8, 4096], P(None, 'rows'), may hold values from 0 to 4095, as said below
- slot_of_camera: int32 [4096], replicated, may hold values from 0 to 4095, as said below
Outputs:
- solution: float32 [9, 4096], P(None, 'rows')
- residual: float32 [9, 4096], P(None, 'rows')
The draws below stay inside these ranges and needn't reach their ends.
Inputs may be any that keep to these rules, and one draw needn't show every extreme that they name: slot_of_camera is a permutation; slot s is held by the device s // 128. `block_cols`: for every device d and every device e, exactly 32 of the entries of the lists of the rows held by d name cameras whose slot is held by e. A list may name a camera more than once, or the row's own camera; every entry adds its block. `diag_blocks`: each 9 x 9 block over the first two dimensions is symmetric positive definite. `precond`: each 9 x 9 block over the first two dimensions is symmetric positive definite.
All inputs are finite; a program needn't handle non-finite values.
Results may differ from the reference program's by a relative error of at most 0.0001.
Values sent between devices are 32-bit elements; how exact they have to be, the bound alone decides.
No kernel may reach another device: no remote copies, remote signals or barrier semaphores. Data moves between devices by JAX's collectives and lax.ppermute only.
A program may use at most 64 MiB of HBM per device.

```python
import math
import jax
import jax.numpy as jnp
from jax import lax

BLOCK = 9
NB = 8
CAM_DEV = 128
ITERS = 2
CAMERAS = 4096
REFS = 32
N_ROWS = 32


def camera_graph(key):
    base = jax.random.fold_in(key, 11)
    key_home, key_pick, key_order = jax.random.split(base, 3)
    slot_map = jax.random.permutation(key_home, CAMERAS).astype(jnp.int32)
    camera_at_slot = jnp.argsort(slot_map).astype(jnp.int32)
    chosen = jax.random.randint(key_pick, (N_ROWS, N_ROWS, REFS), 0, CAM_DEV)
    targets = chosen + (jnp.arange(N_ROWS, dtype=jnp.int32) * CAM_DEV)[None, :, None]
    targets = targets.reshape(N_ROWS, CAM_DEV * NB)
    shuffles = jax.vmap(lambda subkey: jax.random.permutation(subkey, CAM_DEV * NB))(jax.random.split(key_order, N_ROWS))
    placed = jnp.take_along_axis(targets, shuffles, axis=1).reshape(N_ROWS, NB, CAM_DEV)
    slot_lists = jnp.transpose(placed, (1, 0, 2)).reshape(NB, CAMERAS)
    return (slot_map, camera_at_slot[slot_lists].astype(jnp.int32))


def draw_slot_of_camera(key, part):
    return camera_graph(key)[0]


def draw_block_cols(key, part):
    return camera_graph(key)[1]


def spd_blocks(key, lift, low, high):
    key_factor, key_scale = jax.random.split(key)
    factor = jnp.clip(jax.random.normal(key_factor, (BLOCK, BLOCK, CAMERAS), jnp.float32), -3.0, 3.0)
    blocks = jnp.einsum('ikc,jkc->ijc', factor, factor) / BLOCK + lift * jnp.eye(BLOCK, dtype=jnp.float32)[:, :, None]
    scales = jnp.exp(jax.random.uniform(key_scale, (CAMERAS,), jnp.float32, math.log(low), math.log(high)))
    return blocks * scales[None, None, :]


def draw_diag_blocks(key, part):
    return spd_blocks(jax.random.fold_in(key, 21), 1.5, 1.0, 4.0)


def draw_precond(key, part):
    return spd_blocks(jax.random.fold_in(key, 22), 0.5, 0.1, 0.5)


def draw_right_side(key, part):
    key_value, key_scale = jax.random.split(jax.random.fold_in(key, 31))
    position = jnp.arange(CAMERAS, dtype=jnp.float32) / max(CAMERAS - 1, 1)
    rough = jnp.exp(jax.random.uniform(key_scale, (CAMERAS,), jnp.float32, math.log(0.6), math.log(6.0)))
    scales = (1.0 + 2.0 * position) / 3.0 * rough
    values = jnp.clip(jax.random.normal(key_value, (BLOCK, CAMERAS), jnp.float32), -4.0, 4.0)
    return values * scales[None, :]


def block_levels(own_key, extent, cuts, smallest, high):
    def one(axis_at, shards_of):
        heights = jax.random.uniform(jax.random.fold_in(jax.random.fold_in(own_key, 6), axis_at), (shards_of,), jnp.float32, smallest / len(cuts), high / len(cuts))
        return jnp.repeat(jnp.exp(heights), extent[axis_at] // shards_of).reshape((-1,) + (1,) * (len(extent) - axis_at - 1))

    gain = one(*cuts[0])
    for cut in cuts[1:]:
        gain = gain * one(*cut)
    return gain


def centred(rng, extent, scale, reach, shards=(), kind=jnp.bfloat16):
    values = scale * jax.random.normal(rng, extent, jnp.float32)
    if shards:
        values = values * block_levels(rng, extent, shards, -0.22, 0.18)
    return jnp.clip(values, -reach, reach).astype(kind)


def setup_inputs(seed: int = 0) -> dict:
    keys = jax.random.split(jax.random.key(seed), 7)
    return {
        "right_side": draw_right_side(jax.random.fold_in(keys[6], 71), 0),
        "diag_blocks": draw_diag_blocks(jax.random.fold_in(keys[6], 71), 0),
        "precond": draw_precond(jax.random.fold_in(keys[6], 71), 0),
        "upper_blocks": centred(keys[3], (NB, BLOCK, BLOCK, CAMERAS), (96 * NB) ** -0.5, 0.21875, ((3, 32),), jnp.float32),
        "block_cols": draw_block_cols(jax.random.fold_in(keys[6], 71), 0),
        "slot_of_camera": draw_slot_of_camera(jax.random.fold_in(keys[6], 71), 0),
    }


def apply_system(operand, diag_blocks, upper_blocks, slot_lists):
    highest = lax.Precision.HIGHEST
    result = jnp.einsum('abc,bc->ac', diag_blocks, operand, precision=highest)
    gathered = operand[:, slot_lists]
    result = result + jnp.einsum('kabc,bkc->ac', upper_blocks, gathered, precision=highest)
    spread = jnp.einsum('kabc,ac->bkc', upper_blocks, operand, precision=highest)
    result = result.at[:, slot_lists.reshape(-1)].add(spread.reshape(BLOCK, -1))
    return result


def reference(right_side, diag_blocks, precond, upper_blocks, block_cols, slot_of_camera):
    highest = lax.Precision.HIGHEST
    slot_lists = slot_of_camera[block_cols].astype(jnp.int32)
    solution = jnp.zeros_like(right_side)
    residual = right_side
    precond_res = jnp.einsum('abc,bc->ac', precond, residual, precision=highest)
    direction = precond_res
    res_dot = jnp.sum(residual * precond_res)
    for step in range(ITERS):
        image = apply_system(direction, diag_blocks, upper_blocks, slot_lists)
        step_size = res_dot / jnp.sum(direction * image)
        solution = solution + step_size * direction
        residual = residual - step_size * image
        if step + 1 < ITERS:
            precond_res = jnp.einsum('abc,bc->ac', precond, residual, precision=highest)
            new_dot = jnp.sum(residual * precond_res)
            direction = precond_res + (new_dot / res_dot) * direction
            res_dot = new_dot
    return solution, residual
```

```python
import functools
import math

import jax
import jax.numpy as jnp
from jax import lax
from jax.experimental import pallas as pl
from jax.experimental.pallas import tpu as pltpu
from jax.sharding import PartitionSpec as P

ITERS = 2
F32 = jnp.float32
BF16 = jnp.bfloat16
I32 = jnp.int32


class Sizes:
    def __init__(self, block, lists, cams, devices):
        self.block = block
        self.lists = lists
        self.cams = cams
        self.devices = devices
        self.entries = lists * cams
        self.refs = self.entries // devices
        self.groups = cams // self.refs
        self.values = block + 2
        self.push_rows = -(-self.values // self.groups)
        self.rows = block + self.push_rows
        self.shift = cams.bit_length() - 1
        assert cams == 1 << self.shift and self.refs * devices == self.entries
        assert self.refs * self.groups == cams


def split3(x):
    hi = x.astype(BF16)
    rest = x - hi.astype(F32)
    mid = rest.astype(BF16)
    low = (rest - mid.astype(F32)).astype(BF16)
    return hi, mid, low


def dot(a, b):
    return lax.dot_general(a, b, (((1,), (0,)), ((), ())), preferred_element_type=F32)


def dot_t(a, b):
    return lax.dot_general(a, b, (((1,), (1,)), ((), ())), preferred_element_type=F32)


def iota(shape, axis):
    return lax.broadcasted_iota(I32, shape, axis)


def onehot(mask):
    return jnp.where(mask, 1.0, 0.0).astype(BF16)


def col_sum(x):
    return jnp.sum(x, axis=0, keepdims=True)


def total(x):
    return jnp.sum(col_sum(x), axis=1, keepdims=True)


def block_apply(blocks_ref, v, extra=None, up_ref=None, gathered=None, sz=None):
    rows = []
    for a in range(sz.block):
        acc = blocks_ref[a] * v
        if up_ref is not None:
            for k in range(sz.lists):
                acc = acc + up_ref[k, a] * gathered[k]
        rows.append(col_sum(acc))
    out = jnp.concatenate(rows, axis=0)
    return out if extra is None else out + extra


def push(sz, v, dots, up_ref, off, pos, val_ref, perm_ref, roll_ref, msg_ref):
    c = sz.cams
    height = val_ref.shape[0]
    val_ref[...] = jnp.zeros_like(val_ref)
    for k in range(sz.lists):
        acc = up_ref[k, 0] * v[0:1]
        for a in range(1, sz.block):
            acc = acc + up_ref[k, a] * v[a : a + 1]
        lanes = slice(k * c, (k + 1) * c)
        val_ref[0 : sz.block, lanes] = acc
        val_ref[sz.block : sz.block + 1, lanes] = off[k : k + 1].astype(F32)
        perm_ref[:, lanes] = onehot(iota((sz.entries, c), 0) == pos[k : k + 1])
    parts = jnp.concatenate(split3(val_ref[...]), axis=0)
    moved = dot_t(parts, perm_ref[...])
    moved = moved[:height] + moved[height : 2 * height] + moved[2 * height :]
    if dots is not None:
        lane = iota((height, c), 1) & (sz.refs - 1)
        row = iota((height, c), 0)
    group = iota((sz.push_rows, c), 1) >> (sz.refs.bit_length() - 1)
    for chunk in range(sz.lists):
        x = moved[:, chunk * c : (chunk + 1) * c]
        if dots is not None:
            for at, d in enumerate(dots):
                x = jnp.where((row == sz.block + 1) & (lane == at), d, x)
        for t in range(sz.groups):
            roll_ref[t] = pltpu.roll(x, t * sz.refs, 1) if t else x
        for s in range(sz.groups):
            e = chunk * sz.groups + s
            out = jnp.zeros((sz.push_rows, c), F32)
            for g in range(-(-sz.values // sz.push_rows)):
                part = roll_ref[(g - s) % sz.groups, pl.ds(g * sz.push_rows, sz.push_rows), :]
                out = jnp.where(group == g, part, out)
            msg_ref[pl.ds(e * sz.rows, sz.block), :] = v
            msg_ref[pl.ds(e * sz.rows + sz.block, sz.push_rows), :] = out


def gather(sz, msg_ref, own, off):
    c = sz.cams
    left = jnp.concatenate(split3(msg_ref[...]), axis=1)
    period = math.lcm(sz.rows, 8)
    per = period // sz.rows
    width = 2 * c
    row = iota((period, width), 0)
    owner_at = jnp.zeros((period, width), I32)
    for q in range(1, per):
        owner_at = owner_at + jnp.where(row >= q * sz.rows, 1, 0)
    out = []
    for k in range(0, sz.lists, 2):
        pair = jnp.concatenate([off[k : k + 1], off[k + 1 : k + 2]], axis=1)
        right = onehot(iota((c, width), 0) == pair)
        res = dot(left, jnp.concatenate([right] * 3, axis=0))
        owner = jnp.concatenate([own[k : k + 1], own[k + 1 : k + 2]], axis=1) - owner_at
        acc = jnp.zeros((period, width), F32)
        for m in range(sz.devices // per):
            part = res[m * period : (m + 1) * period]
            acc = jnp.where(owner == m * per, part, acc)
        g = acc[: sz.block]
        for q in range(1, per):
            g = g + acc[q * sz.rows : q * sz.rows + sz.block]
        out += [g[:, :c], g[:, c:]]
    return out


def value_at(sz, v):
    return v // sz.push_rows, v % sz.push_rows


def scatter(sz, msg_ref, flat_ref, hot_ref):
    c = sz.cams
    pushed = [
        msg_ref[pl.ds(sz.block + r, sz.devices, stride=sz.rows), :] for r in range(sz.push_rows)
    ]
    lane_group = iota((sz.devices, c), 1) >> (sz.refs.bit_length() - 1)
    g, r = value_at(sz, sz.block)
    offs = jnp.where(lane_group == g, pushed[r], 0.0)
    step = sz.refs
    while step < c:
        offs = offs + pltpu.roll(offs, step, 1)
        step *= 2
    offs = offs.astype(I32)
    height = flat_ref.shape[0]
    masks = []
    row = iota((height, c), 0)
    group = iota((height, c), 1) >> (sz.refs.bit_length() - 1)
    for r in range(sz.push_rows):
        mask = jnp.zeros((height, c), I32)
        for v in range(sz.block):
            if v % sz.push_rows == r:
                mask = mask + jnp.where((row == v) & (group == v // sz.push_rows), 1, 0)
        masks.append(mask > 0)
    for d in range(sz.devices):
        lanes = slice(d * c, (d + 1) * c)
        tile = jnp.zeros((height, c), F32)
        for r in range(sz.push_rows):
            tile = jnp.where(masks[r], pushed[r][d : d + 1], tile)
        flat_ref[:, lanes] = tile
        hot_ref[:, lanes] = onehot(iota((c, c), 0) == offs[d : d + 1])
    parts = jnp.concatenate(split3(flat_ref[...]), axis=0)
    res = dot_t(parts, hot_ref[...])
    res = res[:height] + res[height : 2 * height] + res[2 * height :]
    return res[: sz.block]


def first_kernel(
    sz, rhs_ref, pre_ref, up_ref, cols_ref, table_ref,
    msg_ref, own_ref, off_ref, pos_ref, z_ref,
    val_ref, perm_ref, roll_ref,
):
    c = sz.cams
    cols = cols_ref[...]
    table = table_ref[...]
    height = table.shape[0]
    low = cols & (c - 1)
    high = cols >> sz.shift
    left = jnp.concatenate([table >> sz.shift, table & (c - 1)], axis=0).astype(F32).astype(BF16)
    owns, offs = [], []
    for k in range(sz.lists):
        res = dot(left, onehot(iota((c, c), 0) == low[k : k + 1]))
        here = iota((height, c), 0) == high[k : k + 1]
        owns.append(col_sum(jnp.where(here, res[:height], 0.0)))
        offs.append(col_sum(jnp.where(here, res[height:], 0.0)))
    own = jnp.concatenate(owns, axis=0).astype(I32)
    off = jnp.concatenate(offs, axis=0).astype(I32)
    own_ref[...] = own
    off_ref[...] = off

    hots = [
        jnp.where(iota((sz.devices, c), 0) == own[k : k + 1], 1.0, 0.0) for k in range(sz.lists)
    ]
    lane = iota((c, 2 * c), 1)
    before = onehot((iota((c, 2 * c), 0) < lane) | (lane >= c))
    counts = dot(jnp.concatenate(hots, axis=0).astype(BF16), before)
    base = jnp.zeros((sz.devices, c), F32)
    places = []
    for k in range(sz.lists):
        part = counts[k * sz.devices : (k + 1) * sz.devices]
        places.append(col_sum(hots[k] * (part[:, :c] + base)))
        base = base + part[:, c:]
    pos = own * sz.refs + jnp.concatenate(places, axis=0).astype(I32)
    pos_ref[...] = pos

    z = block_apply(pre_ref, rhs_ref[...], sz=sz)
    z_ref[...] = z
    push(sz, z, None, up_ref, off, pos, val_ref, perm_ref, roll_ref, msg_ref)


def second_kernel(
    sz, got_ref, rhs_ref, z_ref, own_ref, off_ref, pos_ref, diag_ref, pre_ref, up_ref,
    msg_ref, q_ref, w_ref,
    val_ref, perm_ref, roll_ref, flat_ref, hot_ref,
):
    own, off, pos = own_ref[...], off_ref[...], pos_ref[...]
    b, z = rhs_ref[...], z_ref[...]
    gathered = gather(sz, got_ref, own, off)
    pushed = scatter(sz, got_ref, flat_ref, hot_ref)
    q = block_apply(diag_ref, z, pushed, up_ref, gathered, sz)
    w = block_apply(pre_ref, q, sz=sz)
    q_ref[...] = q
    w_ref[...] = w
    dots = [total(b * z), total(z * q), total(b * w), total(q * w)]
    push(sz, w, dots, up_ref, off, pos, val_ref, perm_ref, roll_ref, msg_ref)


def third_kernel(
    sz, got_ref, rhs_ref, z_ref, q_ref, w_ref, own_ref, off_ref, diag_ref, up_ref,
    part_ref, dot_ref, sol_ref, res_ref, dir_ref, img_ref,
    flat_ref, hot_ref,
):
    own, off = own_ref[...], off_ref[...]
    b, z, q, w = rhs_ref[...], z_ref[...], q_ref[...], w_ref[...]
    gathered = gather(sz, got_ref, own, off)
    pushed = scatter(sz, got_ref, flat_ref, hot_ref)
    y = block_apply(diag_ref, w, pushed, up_ref, gathered, sz)
    g, r = value_at(sz, sz.block + 1)
    sums = col_sum(got_ref[pl.ds(sz.block + r, sz.devices, stride=sz.rows), :])
    lane = iota(sums.shape, 1)
    bz, zq, bw, qw = [
        jnp.sum(jnp.where(lane == g * sz.refs + at, sums, 0.0), axis=1, keepdims=True)
        for at in range(4)
    ]
    step = bz / zq
    new_dot = bz - step * (zq + bw) + step * step * qw
    beta = new_dot / bz
    direction = (1.0 + beta) * z - step * w
    image = (1.0 + beta) * q - step * y
    sol_ref[...] = step * z
    res_ref[...] = b - step * q
    dir_ref[...] = direction
    img_ref[...] = image
    dot_ref[...] = jnp.broadcast_to(new_dot, dot_ref.shape)
    part_ref[...] = jnp.broadcast_to(total(direction * image), part_ref.shape)


def fourth_kernel(part_ref, dot_ref, sol_ref, res_ref, dir_ref, img_ref, out_ref, left_ref):
    step = dot_ref[...] / col_sum(part_ref[...])
    out_ref[...] = sol_ref[...] + step * dir_ref[...]
    left_ref[...] = res_ref[...] - step * img_ref[...]


def call(body, name, outs, scratch, *args):
    spec = pl.BlockSpec(memory_space=pltpu.VMEM)
    return pl.pallas_call(
        body,
        name=name,
        out_shape=[jax.ShapeDtypeStruct(s, t) for s, t in outs],
        in_specs=[spec] * len(args),
        out_specs=[spec] * len(outs),
        scratch_shapes=scratch,
    )(*args)


def exchange(sz, msg, rows):
    tile = math.gcd(rows, 4)
    blocks = msg.reshape(sz.devices, rows // tile, tile, sz.cams)
    got = lax.all_to_all(blocks, "rows", split_axis=0, concat_axis=0, tiled=True)
    return got.reshape(sz.devices * rows, sz.cams)


def local(right_side, diag_blocks, precond, upper_blocks, block_cols, slot_of_camera):
    block, cams = right_side.shape
    sz = Sizes(block, block_cols.shape[0], cams, lax.axis_size("rows"))
    field = ((block, cams), F32)
    index = ((sz.lists, cams), I32)
    message = ((sz.devices * sz.rows, cams), F32)
    height = -(-max(sz.values, -(-sz.values // sz.push_rows) * sz.push_rows) // 16) * 16
    push_scratch = [
        pltpu.VMEM((height, sz.entries), F32),
        pltpu.VMEM((sz.entries, sz.entries), BF16),
        pltpu.VMEM((sz.groups, height, cams), F32),
    ]
    scatter_scratch = [
        pltpu.VMEM((16, sz.devices * cams), F32),
        pltpu.VMEM((cams, sz.devices * cams), BF16),
    ]
    table = slot_of_camera.reshape(-1, cams)
    msg, own, off, pos, z = call(
        functools.partial(first_kernel, sz), "first",
        [message, index, index, index, field], push_scratch,
        right_side, precond, upper_blocks, block_cols, table,
    )
    got = exchange(sz, msg, sz.rows)
    msg, q, w = call(
        functools.partial(second_kernel, sz), "second",
        [message, field, field], push_scratch + scatter_scratch,
        got, right_side, z, own, off, pos, diag_blocks, precond, upper_blocks,
    )
    got = exchange(sz, msg, sz.rows)
    part, new_dot, sol, res, direction, image = call(
        functools.partial(third_kernel, sz), "third",
        [((sz.devices, cams), F32), ((1, cams), F32)] + [field] * 4, scatter_scratch,
        got, right_side, z, q, w, own, off, diag_blocks, upper_blocks,
    )
    parts = exchange(sz, part, 1)
    return tuple(
        call(
            fourth_kernel, "fourth", [field, field], [],
            parts, new_dot, sol, res, direction, image,
        )
    )


def solution(mesh):
    return jax.shard_map(
        local,
        mesh=mesh,
        in_specs=(
            P(None, "rows"),
            P(None, None, "rows"),
            P(None, None, "rows"),
            P(None, None, None, "rows"),
            P(None, "rows"),
            P(),
        ),
        out_specs=(P(None, "rows"), P(None, "rows")),
        check_vma=False,
    )
```

```python
import functools
import math

import jax
import jax.numpy as jnp
from jax import lax
from jax.experimental import pallas as pl
from jax.experimental.pallas import tpu as pltpu
from jax.sharding import PartitionSpec as P

VMEM = 24 << 20
TALL = 16
F32 = jnp.float32
BF16 = jnp.bfloat16
I32 = jnp.int32


class Packing:
    def __init__(self, values, refs, cams, skip):
        self.refs = refs
        self.cams = cams
        self.groups = cams // refs
        self.bits = refs.bit_length() - 1
        self.values = values
        self.rows = -(-values // self.groups)
        self.skip = skip
        self.stride = skip + self.rows

    def at(self, v):
        return v // self.rows, v % self.rows

    def group(self, shape):
        return lax.broadcasted_iota(I32, shape, 1) >> self.bits

    def read(self, msg_ref, r, devices):
        return msg_ref[pl.ds(self.skip + r, devices, stride=self.stride), :]


class Sizes:
    def __init__(self, block, lists, cams, devices):
        self.block = block
        self.lists = lists
        self.cams = cams
        self.devices = devices
        self.entries = lists * cams
        self.refs = self.entries // devices
        self.shift = cams.bit_length() - 1
        assert cams == 1 << self.shift and self.refs * devices == self.entries
        assert self.refs == 1 << (self.refs.bit_length() - 1) and lists <= 8
        self.one = Packing(block + 1, self.refs, cams, block)
        self.two = Packing(2 * block + 1, self.refs, cams, 0)
        self.answer = block + 1
        assert self.answer % self.two.rows == 0


def split3(x):
    hi = x.astype(BF16)
    rest = x - hi.astype(F32)
    mid = rest.astype(BF16)
    low = (rest - mid.astype(F32)).astype(BF16)
    return hi, mid, low


def stacked(x):
    return jnp.concatenate(split3(x), axis=0)


def folded(x):
    height = x.shape[0] // 3
    return x[:height] + x[height : 2 * height] + x[2 * height :]


def dot(a, b):
    return lax.dot_general(a, b, (((1,), (0,)), ((), ())), preferred_element_type=F32)


def dot_t(a, b):
    return lax.dot_general(a, b, (((1,), (1,)), ((), ())), preferred_element_type=F32)


def iota(shape, axis):
    return lax.broadcasted_iota(I32, shape, axis)


def onehot(mask):
    return jnp.where(mask, 1.0, 0.0).astype(BF16)


def col_sum(x):
    return jnp.sum(x, axis=0, keepdims=True)


def total(x):
    return jnp.sum(col_sum(x), axis=1, keepdims=True)


def block_apply(sz, blocks_ref, v):
    return jnp.concatenate([col_sum(blocks_ref[a] * v) for a in range(sz.block)], axis=0)


def upper_apply(sz, up_ref, col_ref):
    gathered = [col_ref[pl.ds(b, sz.lists, stride=TALL), :] for b in range(sz.block)]
    rows = []
    for a in range(sz.block):
        acc = up_ref[a, 0] * gathered[0]
        for b in range(1, sz.block):
            acc = acc + up_ref[a, b] * gathered[b]
        rows.append(col_sum(acc))
    return jnp.concatenate(rows, axis=0)


def flat_lanes(sz, ref):
    return jnp.concatenate([ref[k * TALL : (k + 1) * TALL, :] for k in range(sz.lists)], axis=1)


def bucketed(sz, v, off, up_ref, perm_ref, val_ref):
    val_ref[...] = jnp.zeros_like(val_ref)
    for b in range(sz.block):
        acc = up_ref[0, b] * v[0:1]
        for a in range(1, sz.block):
            acc = acc + up_ref[a, b] * v[a : a + 1]
        val_ref[pl.ds(b, sz.lists, stride=TALL), :] = acc
    if off is not None:
        val_ref[pl.ds(sz.block, sz.lists, stride=TALL), :] = off.astype(F32)
    return folded(dot_t(stacked(flat_lanes(sz, val_ref)), perm_ref[...]))


def packed(sz, pk, values, x, roll_ref):
    group = pk.group((pk.rows, sz.cams))
    for t in range(pk.groups):
        roll_ref[t] = pltpu.roll(x, t * sz.refs, 1) if t else x
    for s in range(pk.groups):
        out = jnp.zeros((pk.rows, sz.cams), F32)
        for g in range(-(-values // pk.rows)):
            part = roll_ref[(g - s) % pk.groups, pl.ds(g * pk.rows, pk.rows), :]
            out = jnp.where(group == g, part, out)
        yield s, out


def scatter(sz, pk, msg_ref, flat_ref, hot_ref, offsets):
    c = sz.cams
    pushed = [pk.read(msg_ref, r, sz.devices) for r in range(pk.rows)]
    if offsets:
        g, r = pk.at(sz.block)
        offs = jnp.where(pk.group((sz.devices, c)) == g, pushed[r], 0.0)
        step = sz.refs
        while step < c:
            offs = offs + pltpu.roll(offs, step, 1)
            step *= 2
        offs = offs.astype(I32)
    row = iota((TALL, c), 0)
    group = pk.group((TALL, c))
    masks = []
    for r in range(pk.rows):
        mask = jnp.zeros((TALL, c), I32)
        for v in range(sz.block):
            if v % pk.rows == r:
                mask = mask + jnp.where((row == v) & (group == v // pk.rows), 1, 0)
        masks.append(mask > 0)
    for d in range(sz.devices):
        lanes = slice(d * c, (d + 1) * c)
        tile = jnp.zeros((TALL, c), F32)
        for r in range(pk.rows):
            tile = jnp.where(masks[r], pushed[r][d : d + 1], tile)
        flat_ref[:, lanes] = tile
        if offsets:
            hot_ref[:, lanes] = onehot(iota((c, c), 0) == offs[d : d + 1])
    return folded(dot_t(stacked(flat_ref[...]), hot_ref[...]))[: sz.block]


def gather(sz, msg_ref, own, off, col_ref):
    c = sz.cams
    rows = sz.one.stride
    left = jnp.concatenate(split3(msg_ref[...]), axis=1)
    period = math.lcm(rows, 8)
    per = period // rows
    width = 2 * c
    row = iota((period, width), 0)
    owner_at = jnp.zeros((period, width), I32)
    for q in range(1, per):
        owner_at = owner_at + jnp.where(row >= q * rows, 1, 0)
    for k in range(0, sz.lists, 2):
        pair = jnp.concatenate([off[k : k + 1], off[k + 1 : k + 2]], axis=1)
        right = onehot(iota((c, width), 0) == pair)
        res = dot(left, jnp.concatenate([right] * 3, axis=0))
        owner = jnp.concatenate([own[k : k + 1], own[k + 1 : k + 2]], axis=1) - owner_at
        acc = jnp.zeros((period, width), F32)
        for m in range(sz.devices // per):
            acc = jnp.where(owner == m * per, res[m * period : (m + 1) * period], acc)
        g = acc[: sz.block]
        for q in range(1, per):
            g = g + acc[q * rows : q * rows + sz.block]
        col_ref[pl.ds(k * TALL, sz.block), :] = g[:, :c]
        col_ref[pl.ds((k + 1) * TALL, sz.block), :] = g[:, c:]


def unpack_answers(sz, msg_ref, perm_ref, turn_ref, val_ref, col_ref):
    pk, c = sz.two, sz.cams
    for r in range(pk.rows):
        x = pk.read(msg_ref, r, sz.devices)
        for t in range(pk.groups):
            turn_ref[r, t] = pltpu.roll(x, t * sz.refs, 1) if t else x
    group = pk.group((sz.lists, c))
    val_ref[...] = jnp.zeros_like(val_ref)
    for b in range(sz.block):
        g, r = pk.at(sz.answer + b)
        out = jnp.zeros((sz.lists, c), F32)
        for s in range(pk.groups):
            part = turn_ref[r, (s - g) % pk.groups, pl.ds(s, sz.lists, stride=pk.groups), :]
            out = jnp.where(group == s, part, out)
        val_ref[pl.ds(b, sz.lists, stride=TALL), :] = out
    res = folded(dot(stacked(flat_lanes(sz, val_ref)), perm_ref[...]))
    for k in range(sz.lists):
        col_ref[k * TALL : (k + 1) * TALL, :] = res[:, k * c : (k + 1) * c]


def first_kernel(
    sz, cols_hbm, table_hbm, rhs_hbm, pre_hbm, up_hbm, diag_hbm,
    msg_ref, own_ref, off_ref, z_ref, perm_ref, rhs_ref, pre_ref, up_ref, diag_ref,
    cols_ref, table_ref, val_ref, roll_ref, sems,
):
    pairs = (
        (cols_hbm, cols_ref), (table_hbm, table_ref), (rhs_hbm, rhs_ref), (pre_hbm, pre_ref),
        (up_hbm, up_ref), (diag_hbm, diag_ref),
    )
    copies = [pltpu.make_async_copy(a, b, sems.at[i]) for i, (a, b) in enumerate(pairs)]
    for copy in copies:
        copy.start()
    copies[0].wait()
    copies[1].wait()
    c = sz.cams
    cols = cols_ref[...]
    table = table_ref[...]
    height = table.shape[0]
    low = cols & (c - 1)
    high = cols >> sz.shift
    left = jnp.concatenate([table >> sz.shift, table & (c - 1)], axis=0).astype(F32).astype(BF16)
    owns, offs = [], []
    for k in range(sz.lists):
        res = dot(left, onehot(iota((c, c), 0) == low[k : k + 1]))
        here = iota((height, c), 0) == high[k : k + 1]
        owns.append(col_sum(jnp.where(here, res[:height], 0.0)))
        offs.append(col_sum(jnp.where(here, res[height:], 0.0)))
    own = jnp.concatenate(owns, axis=0).astype(I32)
    off = jnp.concatenate(offs, axis=0).astype(I32)
    own_ref[...] = own
    off_ref[...] = off

    hots = [
        jnp.where(iota((sz.devices, c), 0) == own[k : k + 1], 1.0, 0.0) for k in range(sz.lists)
    ]
    lane = iota((c, 2 * c), 1)
    before = onehot((iota((c, 2 * c), 0) < lane) | (lane >= c))
    counts = dot(jnp.concatenate(hots, axis=0).astype(BF16), before)
    base = jnp.zeros((sz.devices, c), F32)
    for k in range(sz.lists):
        part = counts[k * sz.devices : (k + 1) * sz.devices]
        place = col_sum(hots[k] * (part[:, :c] + base)).astype(I32)
        base = base + part[:, c:]
        pos = own[k : k + 1] * sz.refs + place
        perm_ref[:, k * c : (k + 1) * c] = onehot(iota((sz.entries, c), 0) == pos)

    copies[2].wait()
    copies[3].wait()
    z = block_apply(sz, pre_ref, rhs_ref[...])
    z_ref[...] = z
    copies[4].wait()
    moved = bucketed(sz, z, off, up_ref, perm_ref, val_ref)
    pk = sz.one
    for chunk in range(sz.lists):
        x = moved[:, chunk * c : (chunk + 1) * c]
        for s, out in packed(sz, pk, pk.values, x, roll_ref):
            e = chunk * pk.groups + s
            msg_ref[pl.ds(e * pk.stride, sz.block), :] = z
            msg_ref[pl.ds(e * pk.stride + sz.block, pk.rows), :] = out
    copies[5].wait()


def second_kernel(
    sz, got_ref, rhs_ref, z_ref, own_ref, off_ref, perm_ref, diag_ref, pre_ref, up_ref,
    msg_ref, q_ref, w_ref, hot_ref,
    val_ref, roll_ref, flat_ref, col_ref, ans_ref,
):
    c, pk = sz.cams, sz.two
    b, z = rhs_ref[...], z_ref[...]
    gather(sz, got_ref, own_ref[...], off_ref[...], col_ref)
    pushed = scatter(sz, sz.one, got_ref, flat_ref, hot_ref, True)
    q = block_apply(sz, diag_ref, z) + upper_apply(sz, up_ref, col_ref) + pushed
    w = block_apply(sz, pre_ref, q)
    q_ref[...] = q
    w_ref[...] = w
    dots = [total(b * z), total(z * q), total(b * w), total(q * w)]
    lane = iota((1, c), 1) & (sz.refs - 1)
    dot_row = jnp.zeros((1, c), F32)
    for at, d in enumerate(dots):
        dot_row = jnp.where(lane == at, d, dot_row)
    tall = jnp.concatenate([w, jnp.zeros((TALL - sz.block, c), F32)], axis=0)
    ans_ref[...] = folded(dot(stacked(tall), hot_ref[...]))
    moved = bucketed(sz, w, None, up_ref, perm_ref, val_ref)
    row = iota((TALL, c), 0)
    group = pk.group((pk.rows, c))
    first = sz.answer // pk.rows
    for chunk in range(sz.lists):
        x = jnp.where(row == sz.block, dot_row, moved[:, chunk * c : (chunk + 1) * c])
        for s, out in packed(sz, pk, sz.answer, x, roll_ref):
            e = chunk * pk.groups + s
            for g in range(-(-sz.block // pk.rows)):
                part = ans_ref[pl.ds(g * pk.rows, pk.rows), e * c : (e + 1) * c]
                out = jnp.where(group == first + g, part, out)
            msg_ref[pl.ds(e * pk.stride, pk.rows), :] = out


def third_kernel(
    sz, got_ref, rhs_ref, z_ref, q_ref, w_ref, perm_ref, hot_ref, diag_ref, up_ref,
    part_ref, dot_ref, sol_ref, res_ref, dir_ref, img_ref,
    val_ref, turn_ref, flat_ref, col_ref,
):
    pk = sz.two
    b, z, q, w = rhs_ref[...], z_ref[...], q_ref[...], w_ref[...]
    unpack_answers(sz, got_ref, perm_ref, turn_ref, val_ref, col_ref)
    pushed = scatter(sz, pk, got_ref, flat_ref, hot_ref, False)
    y = block_apply(sz, diag_ref, w) + upper_apply(sz, up_ref, col_ref) + pushed
    g, r = pk.at(sz.block)
    sums = col_sum(pk.read(got_ref, r, sz.devices))
    lane = iota(sums.shape, 1)
    bz, zq, bw, qw = [
        jnp.sum(jnp.where(lane == g * sz.refs + at, sums, 0.0), axis=1, keepdims=True)
        for at in range(4)
    ]
    step = bz / zq
    new_dot = bz - step * (zq + bw) + step * step * qw
    beta = new_dot / bz
    direction = (1.0 + beta) * z - step * w
    image = (1.0 + beta) * q - step * y
    sol_ref[...] = step * z
    res_ref[...] = b - step * q
    dir_ref[...] = direction
    img_ref[...] = image
    dot_ref[...] = jnp.broadcast_to(new_dot, dot_ref.shape)
    part_ref[...] = jnp.broadcast_to(total(direction * image), part_ref.shape)


def fourth_kernel(part_ref, dot_ref, sol_ref, res_ref, dir_ref, img_ref, out_ref, left_ref):
    step = dot_ref[...] / col_sum(part_ref[...])
    out_ref[...] = sol_ref[...] + step * dir_ref[...]
    left_ref[...] = res_ref[...] - step * img_ref[...]


def call(body, name, outs, scratch, *args, space=pltpu.VMEM):
    return pl.pallas_call(
        body,
        name=name,
        out_shape=[jax.ShapeDtypeStruct(s, t) for s, t in outs],
        in_specs=[pl.BlockSpec(memory_space=space)] * len(args),
        out_specs=[pl.BlockSpec(memory_space=pltpu.VMEM)] * len(outs),
        scratch_shapes=scratch,
        compiler_params=pltpu.CompilerParams(vmem_limit_bytes=VMEM),
    )(*args)


def exchange(sz, msg, rows):
    tile = math.gcd(rows, 4)
    blocks = msg.reshape(sz.devices, rows // tile, tile, sz.cams)
    got = lax.all_to_all(blocks, "rows", split_axis=0, concat_axis=0, tiled=True)
    return got.reshape(sz.devices * rows, sz.cams)


def local(right_side, diag_blocks, precond, upper_blocks, block_cols, slot_of_camera):
    block, cams = right_side.shape
    lists = block_cols.shape[0]
    sz = Sizes(block, lists, cams, lax.axis_size("rows"))
    field = ((block, cams), F32)
    index = ((lists, cams), I32)
    perm_type = ((sz.entries, sz.entries), BF16)
    wide = sz.devices * cams
    upper_blocks = upper_blocks.transpose(1, 2, 0, 3)
    table = slot_of_camera.reshape(-1, cams)
    values = pltpu.VMEM((lists * TALL, cams), F32)
    flat = pltpu.VMEM((TALL, wide), F32)

    def rolls(pk):
        return pltpu.VMEM((pk.groups, TALL, cams), F32)

    ins = (block_cols, table, right_side, precond, upper_blocks, diag_blocks)
    msg, own, off, z, perm, right_side, precond, upper_blocks, diag_blocks = call(
        functools.partial(first_kernel, sz), "first",
        [((sz.devices * sz.one.stride, cams), F32), index, index, field, perm_type]
        + [(x.shape, x.dtype) for x in ins[2:]],
        [pltpu.VMEM(x.shape, x.dtype) for x in ins[:2]]
        + [values, rolls(sz.one), pltpu.SemaphoreType.DMA((len(ins),))],
        *(pltpu.with_memory_space_constraint(x, pltpu.HBM) for x in ins), space=pltpu.HBM,
    )
    got = exchange(sz, msg, sz.one.stride)
    msg, q, w, hot = call(
        functools.partial(second_kernel, sz), "second",
        [((sz.devices * sz.two.stride, cams), F32), field, field, ((cams, wide), BF16)],
        [values, rolls(sz.two), flat, values, flat],
        got, right_side, z, own, off, perm, diag_blocks, precond, upper_blocks,
    )
    got = exchange(sz, msg, sz.two.stride)
    part, new_dot, sol, res, direction, image = call(
        functools.partial(third_kernel, sz), "third",
        [((sz.devices, cams), F32), ((1, cams), F32)] + [field] * 4,
        [values, pltpu.VMEM((sz.two.rows, sz.two.groups, sz.devices, cams), F32), flat, values],
        got, right_side, z, q, w, perm, hot, diag_blocks, upper_blocks,
    )
    parts = exchange(sz, part, 1)
    return tuple(
        call(
            fourth_kernel, "fourth", [field, field], [],
            parts, new_dot, sol, res, direction, image,
        )
    )


def solution(mesh):
    return jax.shard_map(
        local,
        mesh=mesh,
        in_specs=(
            P(None, "rows"),
            P(None, None, "rows"),
            P(None, None, "rows"),
            P(None, None, None, "rows"),
            P(None, "rows"),
            P(),
        ),
        out_specs=(P(None, "rows"), P(None, "rows")),
        check_vma=False,
    )
```

```python
import functools
import math

import jax
import jax.numpy as jnp
from jax import lax
from jax.experimental import pallas as pl
from jax.experimental.pallas import tpu as pltpu
from jax.sharding import PartitionSpec as P

VMEM = 24 << 20
TALL = 16
F32 = jnp.float32
BF16 = jnp.bfloat16
I32 = jnp.int32


class Packing:
    def __init__(self, values, refs, cams, skip):
        self.refs = refs
        self.cams = cams
        self.groups = cams // refs
        self.bits = refs.bit_length() - 1
        self.values = values
        self.rows = -(-values // self.groups)
        self.skip = skip
        self.stride = skip + self.rows

    def at(self, v):
        return v // self.rows, v % self.rows

    def group(self, shape):
        return lax.broadcasted_iota(I32, shape, 1) >> self.bits

    def read(self, msg_ref, r, devices):
        return msg_ref[pl.ds(self.skip + r, devices, stride=self.stride), :]


class Sizes:
    def __init__(self, block, lists, cams, devices):
        self.block = block
        self.lists = lists
        self.cams = cams
        self.devices = devices
        self.entries = lists * cams
        self.refs = self.entries // devices
        self.shift = cams.bit_length() - 1
        assert cams == 1 << self.shift and self.refs * devices == self.entries
        assert self.refs == 1 << (self.refs.bit_length() - 1) and lists <= 8
        self.one = Packing(block + 1, self.refs, cams, block)
        self.two = Packing(2 * block + 1, self.refs, cams, 0)
        self.answer = block + 1
        assert self.answer % self.two.rows == 0


def split3(x):
    hi = x.astype(BF16)
    rest = x - hi.astype(F32)
    mid = rest.astype(BF16)
    low = (rest - mid.astype(F32)).astype(BF16)
    return hi, mid, low


def stacked(x):
    return jnp.concatenate(split3(x), axis=0)


def folded(x):
    height = x.shape[0] // 3
    return x[:height] + x[height : 2 * height] + x[2 * height :]


def dot(a, b):
    return lax.dot_general(a, b, (((1,), (0,)), ((), ())), preferred_element_type=F32)


def dot_t(a, b):
    return lax.dot_general(a, b, (((1,), (1,)), ((), ())), preferred_element_type=F32)


def iota(shape, axis):
    return lax.broadcasted_iota(I32, shape, axis)


def onehot(mask):
    return jnp.where(mask, 1.0, 0.0).astype(BF16)


def hot_rows(places, shape):
    rows = iota(shape, 0).astype(F32).astype(BF16)
    same = rows == jnp.broadcast_to(places.astype(F32).astype(BF16), shape)
    return jnp.where(same, jnp.ones(shape, BF16), jnp.zeros(shape, BF16))


def col_sum(x):
    return jnp.sum(x, axis=0, keepdims=True)


def total(x):
    return jnp.sum(col_sum(x), axis=1, keepdims=True)


def block_apply(sz, blocks_ref, v):
    return jnp.concatenate([col_sum(blocks_ref[a] * v) for a in range(sz.block)], axis=0)


def upper_apply(sz, up_ref, col_ref):
    gathered = [col_ref[pl.ds(b, sz.lists, stride=TALL), :] for b in range(sz.block)]
    rows = []
    for a in range(sz.block):
        acc = up_ref[a, 0] * gathered[0]
        for b in range(1, sz.block):
            acc = acc + up_ref[a, b] * gathered[b]
        rows.append(col_sum(acc))
    return jnp.concatenate(rows, axis=0)


def side_by_side(ref, height):
    blocks = [ref[at : at + height, :] for at in range(0, ref.shape[0], height)]
    return jnp.concatenate(blocks, axis=1)


def bucketed(sz, v, off, up_ref, chunk, lane_ref, val_ref):
    for b in range(sz.block):
        acc = up_ref[0, b] * v[0:1]
        for a in range(1, sz.block):
            acc = acc + up_ref[a, b] * v[a : a + 1]
        val_ref[pl.ds(b, sz.lists, stride=TALL), :] = acc
    if off is not None:
        val_ref[pl.ds(sz.block, sz.lists, stride=TALL), :] = off.astype(F32)
    parts = stacked(side_by_side(val_ref, TALL))
    where = jnp.concatenate([chunk[k : k + 1] for k in range(sz.lists)], axis=1)
    where = jnp.broadcast_to(where.astype(F32).astype(BF16), parts.shape)
    left = [
        jnp.where(where == jnp.full(parts.shape, at, BF16), parts, jnp.zeros(parts.shape, BF16))
        for at in range(sz.lists)
    ]
    res = dot_t(jnp.concatenate(left, axis=0), side_by_side(lane_ref, sz.cams))
    return [folded(res[at * 3 * TALL : (at + 1) * 3 * TALL]) for at in range(sz.lists)]


def pack(sz, pk, value_of, msg_ref):
    group = pk.group((sz.lists, sz.cams))
    values = [value_of(v) for v in range(pk.values)]
    turned = [
        [pltpu.roll(x, t * sz.refs, 1) if t else x for t in range(pk.groups)] for x in values
    ]
    for s in range(pk.groups):
        for r in range(pk.rows):
            out = jnp.zeros((sz.lists, sz.cams), F32)
            for g in range(pk.groups):
                v = g * pk.rows + r
                if v < pk.values:
                    out = jnp.where(group == g, turned[v][(g - s) % pk.groups], out)
            at = pl.ds(s * pk.stride + pk.skip + r, sz.lists, stride=pk.groups * pk.stride)
            msg_ref[at, :] = out


def unpack(sz, pk, msg_ref, turn_ref):
    for r in range(pk.rows):
        x = pk.read(msg_ref, r, sz.devices)
        for t in range(pk.groups):
            turn_ref[r, t] = pltpu.roll(x, t * sz.refs, 1) if t else x
    group = pk.group((sz.lists, sz.cams))
    out = []
    for v in range(pk.values):
        g, r = pk.at(v)
        value = None
        for s in range(pk.groups):
            part = turn_ref[r, (s - g) % pk.groups, pl.ds(s, sz.lists, stride=pk.groups), :]
            value = part if value is None else jnp.where(group == s, part, value)
        out.append(value)
    return out


def scatter(sz, values, tall_ref, hot_ref):
    for b in range(sz.block):
        tall_ref[pl.ds(b, sz.lists, stride=TALL), :] = values[b]
    parts = stacked(side_by_side(tall_ref, TALL))
    return folded(dot_t(parts, side_by_side(hot_ref, sz.cams)))[: sz.block]


def gather(sz, msg_ref, own, off, col_ref):
    c = sz.cams
    rows = sz.one.stride
    left = jnp.concatenate(split3(msg_ref[...]), axis=1)
    period = math.lcm(rows, 8)
    per = period // rows
    width = 2 * c
    row = iota((period, width), 0)
    owner_at = jnp.zeros((period, width), I32)
    for q in range(1, per):
        owner_at = owner_at + jnp.where(row >= q * rows, 1, 0)
    for k in range(0, sz.lists, 2):
        pair = jnp.concatenate([off[k : k + 1], off[k + 1 : k + 2]], axis=1)
        right = hot_rows(pair, (c, width))
        res = dot(left, jnp.concatenate([right] * 3, axis=0))
        owner = jnp.concatenate([own[k : k + 1], own[k + 1 : k + 2]], axis=1) - owner_at
        acc = jnp.zeros((period, width), F32)
        for m in range(sz.devices // per):
            acc = jnp.where(owner == m * per, res[m * period : (m + 1) * period], acc)
        g = acc[: sz.block]
        for q in range(1, per):
            g = g + acc[q * rows : q * rows + sz.block]
        col_ref[pl.ds(k * TALL, sz.block), :] = g[:, :c]
        col_ref[pl.ds((k + 1) * TALL, sz.block), :] = g[:, c:]


def to_lists(sz, values, chunk, lane_ref, tall_ref, col_ref):
    for b in range(sz.block):
        tall_ref[pl.ds(b, sz.lists, stride=TALL), :] = values[b]
    left = jnp.concatenate(split3(tall_ref[...]), axis=1)
    right = jnp.concatenate([side_by_side(lane_ref, sz.cams)] * 3, axis=0)
    res = dot(left, right)
    for k in range(sz.lists):
        lanes = slice(k * sz.cams, (k + 1) * sz.cams)
        out = res[:TALL, lanes]
        for at in range(1, sz.lists):
            out = jnp.where(chunk[k : k + 1] == at, res[at * TALL : (at + 1) * TALL, lanes], out)
        col_ref[k * TALL : (k + 1) * TALL, :] = out


def first_kernel(
    sz, cols_hbm, table_hbm, rhs_hbm, pre_hbm, up_hbm, diag_hbm,
    msg_ref, own_ref, off_ref, chunk_ref, z_ref, lane_ref, rhs_ref, pre_ref, up_ref, diag_ref,
    cols_ref, table_ref, val_ref, tall_ref, sems,
):
    pairs = (
        (cols_hbm, cols_ref), (table_hbm, table_ref), (rhs_hbm, rhs_ref), (pre_hbm, pre_ref),
        (up_hbm, up_ref), (diag_hbm, diag_ref),
    )
    copies = [pltpu.make_async_copy(a, b, sems.at[i]) for i, (a, b) in enumerate(pairs)]
    for copy in copies:
        copy.start()
    copies[0].wait()
    copies[1].wait()
    c = sz.cams
    cols = cols_ref[...]
    table = table_ref[...]
    height = table.shape[0]
    low = cols & (c - 1)
    high = cols >> sz.shift
    left = jnp.concatenate([table >> sz.shift, table & (c - 1)], axis=0).astype(F32).astype(BF16)
    owns, offs = [], []
    for k in range(sz.lists):
        res = dot(left, hot_rows(low[k : k + 1], (c, c)))
        here = iota((height, c), 0) == high[k : k + 1]
        owns.append(col_sum(jnp.where(here, res[:height], 0.0)))
        offs.append(col_sum(jnp.where(here, res[height:], 0.0)))
    own = jnp.concatenate(owns, axis=0).astype(I32)
    off = jnp.concatenate(offs, axis=0).astype(I32)
    own_ref[...] = own
    off_ref[...] = off

    hots = [
        jnp.where(iota((sz.devices, c), 0) == own[k : k + 1], 1.0, 0.0) for k in range(sz.lists)
    ]
    lane = iota((c, 2 * c), 1)
    before = onehot((iota((c, 2 * c), 0) < lane) | (lane >= c))
    counts = dot(jnp.concatenate(hots, axis=0).astype(BF16), before)
    base = jnp.zeros((sz.devices, c), F32)
    places = []
    for k in range(sz.lists):
        part = counts[k * sz.devices : (k + 1) * sz.devices]
        places.append(col_sum(hots[k] * (part[:, :c] + base)))
        base = base + part[:, c:]
    pos = own * sz.refs + jnp.concatenate(places, axis=0).astype(I32)
    chunk = pos >> sz.shift
    place = pos & (c - 1)
    chunk_ref[...] = chunk
    for k in range(sz.lists):
        lane_ref[k * c : (k + 1) * c, :] = hot_rows(place[k : k + 1], (c, c))

    for copy in copies[2:]:
        copy.wait()
    pk = sz.one
    z = block_apply(sz, pre_ref, rhs_ref[...])
    z_ref[...] = z
    for b in range(sz.block):
        at = pl.ds(b, sz.devices, stride=pk.stride)
        msg_ref[at, :] = jnp.broadcast_to(z[b : b + 1], (sz.devices, c))
    for at, x in enumerate(bucketed(sz, z, off, up_ref, chunk, lane_ref, val_ref)):
        tall_ref[at * TALL : (at + 1) * TALL, :] = x
    pack(sz, pk, lambda v: tall_ref[pl.ds(v, sz.lists, stride=TALL), :], msg_ref)


def second_kernel(
    sz, got_ref, rhs_ref, z_ref, own_ref, off_ref, chunk_ref, lane_ref, diag_ref, pre_ref, up_ref,
    msg_ref, q_ref, w_ref, hot_ref,
    val_ref, tall_ref, ans_ref, col_ref, turn_ref,
):
    c = sz.cams
    b, z = rhs_ref[...], z_ref[...]
    values = unpack(sz, sz.one, got_ref, turn_ref)
    wanted = values[sz.block].astype(I32)
    for at in range(sz.lists):
        hot_ref[at * c : (at + 1) * c, :] = hot_rows(wanted[at : at + 1], (c, c))
    pushed = scatter(sz, values, val_ref, hot_ref)
    gather(sz, got_ref, own_ref[...], off_ref[...], col_ref)
    q = block_apply(sz, diag_ref, z) + upper_apply(sz, up_ref, col_ref) + pushed
    w = block_apply(sz, pre_ref, q)
    q_ref[...] = q
    w_ref[...] = w
    dots = [total(b * z), total(z * q), total(b * w), total(q * w)]
    lane = iota((sz.lists, c), 1) & (sz.refs - 1)
    dot_rows = jnp.zeros((sz.lists, c), F32)
    for at, d in enumerate(dots):
        dot_rows = jnp.where(lane == at, d, dot_rows)
    tall = jnp.concatenate([w, jnp.zeros((TALL - sz.block, c), F32)], axis=0)
    answers = folded(dot(stacked(tall), side_by_side(hot_ref, c)))
    for at in range(sz.lists):
        ans_ref[at * TALL : (at + 1) * TALL, :] = answers[:, at * c : (at + 1) * c]
    for at, x in enumerate(bucketed(sz, w, None, up_ref, chunk_ref[...], lane_ref, val_ref)):
        tall_ref[at * TALL : (at + 1) * TALL, :] = x

    def value_of(v):
        if v < sz.block:
            return tall_ref[pl.ds(v, sz.lists, stride=TALL), :]
        if v == sz.block:
            return dot_rows
        return ans_ref[pl.ds(v - sz.answer, sz.lists, stride=TALL), :]

    pack(sz, sz.two, value_of, msg_ref)


def third_kernel(
    sz, got_ref, rhs_ref, z_ref, q_ref, w_ref, chunk_ref, lane_ref, hot_ref, diag_ref, up_ref,
    part_ref, dot_ref, sol_ref, res_ref, dir_ref, img_ref,
    val_ref, tall_ref, col_ref, turn_ref,
):
    b, z, q, w = rhs_ref[...], z_ref[...], q_ref[...], w_ref[...]
    values = unpack(sz, sz.two, got_ref, turn_ref)
    to_lists(sz, values[sz.answer :], chunk_ref[...], lane_ref, tall_ref, col_ref)
    pushed = scatter(sz, values, val_ref, hot_ref)
    y = block_apply(sz, diag_ref, w) + upper_apply(sz, up_ref, col_ref) + pushed
    sums = col_sum(values[sz.block])
    lane = iota(sums.shape, 1) & (sz.refs - 1)
    bz, zq, bw, qw = [
        jnp.sum(jnp.where(lane == at, sums, 0.0), axis=1, keepdims=True) for at in range(4)
    ]
    step = bz / zq
    new_dot = bz - step * (zq + bw) + step * step * qw
    beta = new_dot / bz
    direction = (1.0 + beta) * z - step * w
    image = (1.0 + beta) * q - step * y
    sol_ref[...] = step * z
    res_ref[...] = b - step * q
    dir_ref[...] = direction
    img_ref[...] = image
    dot_ref[...] = jnp.broadcast_to(new_dot, dot_ref.shape)
    part_ref[...] = jnp.broadcast_to(total(direction * image), part_ref.shape)


def fourth_kernel(part_ref, dot_ref, sol_ref, res_ref, dir_ref, img_ref, out_ref, left_ref):
    step = dot_ref[...] / col_sum(part_ref[...])
    out_ref[...] = sol_ref[...] + step * dir_ref[...]
    left_ref[...] = res_ref[...] - step * img_ref[...]


def call(body, name, outs, scratch, *args, space=pltpu.VMEM):
    return pl.pallas_call(
        body,
        name=name,
        out_shape=[jax.ShapeDtypeStruct(s, t) for s, t in outs],
        in_specs=[pl.BlockSpec(memory_space=space)] * len(args),
        out_specs=[pl.BlockSpec(memory_space=pltpu.VMEM)] * len(outs),
        scratch_shapes=scratch,
        compiler_params=pltpu.CompilerParams(vmem_limit_bytes=VMEM),
    )(*args)


def exchange(sz, msg, rows):
    blocks = msg.reshape(sz.devices, 1, rows * sz.cams)
    got = lax.all_to_all(blocks, "rows", split_axis=0, concat_axis=0, tiled=True)
    return got.reshape(sz.devices * rows, sz.cams)


def local(right_side, diag_blocks, precond, upper_blocks, block_cols, slot_of_camera):
    block, cams = right_side.shape
    lists = block_cols.shape[0]
    sz = Sizes(block, lists, cams, lax.axis_size("rows"))
    field = ((block, cams), F32)
    index = ((lists, cams), I32)
    hot_type = ((sz.entries, cams), BF16)
    upper_blocks = upper_blocks.transpose(1, 2, 0, 3)
    table = slot_of_camera.reshape(-1, cams)
    tall = pltpu.VMEM((lists * TALL, cams), F32)

    def turns(pk):
        return pltpu.VMEM((pk.rows, pk.groups, sz.devices, cams), F32)

    ins = (block_cols, table, right_side, precond, upper_blocks, diag_blocks)
    msg, own, off, chunk, z, lane, right_side, precond, upper_blocks, diag_blocks = call(
        functools.partial(first_kernel, sz), "first",
        [((sz.devices * sz.one.stride, cams), F32), index, index, index, field, hot_type]
        + [(x.shape, x.dtype) for x in ins[2:]],
        [pltpu.VMEM(x.shape, x.dtype) for x in ins[:2]]
        + [tall, tall, pltpu.SemaphoreType.DMA((len(ins),))],
        *(pltpu.with_memory_space_constraint(x, pltpu.HBM) for x in ins), space=pltpu.HBM,
    )
    got = exchange(sz, msg, sz.one.stride)
    msg, q, w, hot = call(
        functools.partial(second_kernel, sz), "second",
        [((sz.devices * sz.two.stride, cams), F32), field, field, hot_type],
        [tall] * 4 + [turns(sz.one)],
        got, right_side, z, own, off, chunk, lane, diag_blocks, precond, upper_blocks,
    )
    got = exchange(sz, msg, sz.two.stride)
    part, new_dot, sol, res, direction, image = call(
        functools.partial(third_kernel, sz), "third",
        [((sz.devices, cams), F32), ((1, cams), F32)] + [field] * 4,
        [tall] * 3 + [turns(sz.two)],
        got, right_side, z, q, w, chunk, lane, hot, diag_blocks, upper_blocks,
    )
    parts = exchange(sz, part, 1)
    return tuple(
        call(
            fourth_kernel, "fourth", [field, field], [],
            parts, new_dot, sol, res, direction, image,
        )
    )


def solution(mesh):
    return jax.shard_map(
        local,
        mesh=mesh,
        in_specs=(
            P(None, "rows"),
            P(None, None, "rows"),
            P(None, None, "rows"),
            P(None, None, None, "rows"),
            P(None, "rows"),
            P(),
        ),
        out_specs=(P(None, "rows"), P(None, "rows")),
        check_vma=False,
    )
```

```python
import functools
import math

import jax
import jax.numpy as jnp
from jax import lax
from jax.experimental import pallas as pl
from jax.experimental.pallas import tpu as pltpu
from jax.sharding import PartitionSpec as P

VMEM = 24 << 20
TALL = 16
F32 = jnp.float32
BF16 = jnp.bfloat16
I32 = jnp.int32


class Packing:
    def __init__(self, values, refs, cams, skip):
        self.refs = refs
        self.cams = cams
        self.groups = cams // refs
        self.bits = refs.bit_length() - 1
        self.values = values
        self.rows = -(-values // self.groups)
        self.skip = skip
        self.stride = skip + self.rows

    def at(self, v):
        return v // self.rows, v % self.rows

    def group(self, shape):
        return lax.broadcasted_iota(I32, shape, 1) >> self.bits

    def read(self, msg_ref, r, devices):
        return msg_ref[pl.ds(self.skip + r, devices, stride=self.stride), :]


class Sizes:
    def __init__(self, block, lists, cams, devices):
        self.block = block
        self.lists = lists
        self.cams = cams
        self.devices = devices
        self.entries = lists * cams
        self.refs = self.entries // devices
        self.shift = cams.bit_length() - 1
        assert cams == 1 << self.shift and self.refs * devices == self.entries
        assert self.refs == 1 << (self.refs.bit_length() - 1) and lists <= 8
        self.one = Packing(block + 1, self.refs, cams, block)
        self.two = Packing(2 * block + 1, self.refs, cams, 0)
        self.answer = block + 1
        assert self.answer % self.two.rows == 0


def split3(x):
    hi = x.astype(BF16)
    rest = x - hi.astype(F32)
    mid = rest.astype(BF16)
    low = (rest - mid.astype(F32)).astype(BF16)
    return hi, mid, low


def stacked(x):
    parts = [p.astype(F32) for p in split3(x)]
    row = lax.broadcasted_iota(I32, (8, x.shape[1]), 0)
    tail = parts[0][8:]
    for at in (1, 2):
        tail = jnp.where(row < 2 * at, tail, pltpu.roll(parts[at][8:], 2 * at, 0))
    return jnp.concatenate([p[:8] for p in parts] + [tail], axis=0).astype(BF16)


def folded(x):
    tail = x[24:]
    tail = tail + pltpu.roll(tail, 6, 0) + pltpu.roll(tail, 4, 0)
    return jnp.concatenate([x[:8] + x[8:16] + x[16:24], tail], axis=0)


def row_sums(arrays):
    shape = arrays[0].shape
    if len(arrays) != 8 or shape[0] != 8:
        return jnp.concatenate([col_sum(x) for x in arrays], axis=0)
    row = lax.broadcasted_iota(I32, shape, 0)
    step = 4
    while step:
        low = (row & step) == 0
        arrays = [
            jnp.where(low, a, b)
            + jnp.where(low, pltpu.roll(a, 8 - step, 0), pltpu.roll(b, step, 0))
            for a, b in zip(arrays[: len(arrays) // 2], arrays[len(arrays) // 2 :])
        ]
        step //= 2
    return arrays[0]


def dot(a, b):
    return lax.dot_general(a, b, (((1,), (0,)), ((), ())), preferred_element_type=F32)


def dot_t(a, b):
    return lax.dot_general(a, b, (((1,), (1,)), ((), ())), preferred_element_type=F32)


def iota(shape, axis):
    return lax.broadcasted_iota(I32, shape, axis)


def onehot(mask):
    return jnp.where(mask, 1.0, 0.0).astype(BF16)


def hot_rows(places, shape):
    rows = iota(shape, 0).astype(F32).astype(BF16)
    same = rows == jnp.broadcast_to(places.astype(F32).astype(BF16), shape)
    return jnp.where(same, jnp.ones(shape, BF16), jnp.zeros(shape, BF16))


def col_sum(x):
    return jnp.sum(x, axis=0, keepdims=True)


def total(x):
    return jnp.sum(col_sum(x), axis=1, keepdims=True)


def block_apply(sz, blocks_ref, v):
    acc = blocks_ref[0] * v[0:1]
    for b in range(1, sz.block):
        acc = acc + blocks_ref[b] * v[b : b + 1]
    return acc


def upper_apply(sz, up_ref, gathered):
    rows = []
    for a in range(sz.block):
        acc = up_ref[a, 0] * gathered[0]
        for b in range(1, sz.block):
            acc = acc + up_ref[a, b] * gathered[b]
        rows.append(acc)
    return jnp.concatenate([row_sums(rows[:8])] + [col_sum(x) for x in rows[8:]], axis=0)


def side_by_side(ref, height):
    blocks = [ref[at : at + height, :] for at in range(0, ref.shape[0], height)]
    return jnp.concatenate(blocks, axis=1)


def bucketed(sz, v, off, up_ref, chunk, lane_ref, val_ref):
    for b in range(sz.block):
        acc = up_ref[0, b] * v[0:1]
        for a in range(1, sz.block):
            acc = acc + up_ref[a, b] * v[a : a + 1]
        val_ref[pl.ds(b, sz.lists, stride=TALL), :] = acc
    if off is not None:
        val_ref[pl.ds(sz.block, sz.lists, stride=TALL), :] = off.astype(F32)
    parts = stacked(side_by_side(val_ref, TALL))
    where = jnp.concatenate([chunk[k : k + 1] for k in range(sz.lists)], axis=1)
    where = jnp.broadcast_to(where.astype(F32).astype(BF16), parts.shape)
    left = [
        jnp.where(where == jnp.full(parts.shape, at, BF16), parts, jnp.zeros(parts.shape, BF16))
        for at in range(sz.lists)
    ]
    res = dot_t(jnp.concatenate(left, axis=0), side_by_side(lane_ref, sz.cams))
    height = parts.shape[0]
    return [folded(res[at * height : (at + 1) * height]) for at in range(sz.lists)]


def pack(sz, pk, value_of, msg_ref):
    group = pk.group((sz.lists, sz.cams))
    values = [value_of(v) for v in range(pk.values)]
    turned = [
        [pltpu.roll(x, t * sz.refs, 1) if t else x for t in range(pk.groups)] for x in values
    ]
    for s in range(pk.groups):
        for r in range(pk.rows):
            out = jnp.zeros((sz.lists, sz.cams), F32)
            for g in range(pk.groups):
                v = g * pk.rows + r
                if v < pk.values:
                    out = jnp.where(group == g, turned[v][(g - s) % pk.groups], out)
            at = pl.ds(s * pk.stride + pk.skip + r, sz.lists, stride=pk.groups * pk.stride)
            msg_ref[at, :] = out


def unpack(sz, pk, msg_ref, turn_ref):
    for r in range(pk.rows):
        x = pk.read(msg_ref, r, sz.devices)
        for t in range(pk.groups):
            turn_ref[r, t] = pltpu.roll(x, t * sz.refs, 1) if t else x
    group = pk.group((sz.lists, sz.cams))
    out = []
    for v in range(pk.values):
        g, r = pk.at(v)
        value = None
        for s in range(pk.groups):
            part = turn_ref[r, (s - g) % pk.groups, pl.ds(s, sz.lists, stride=pk.groups), :]
            value = part if value is None else jnp.where(group == s, part, value)
        out.append(value)
    return out


def scatter(sz, values, tall_ref, hot_ref):
    for b in range(sz.block):
        tall_ref[pl.ds(b, sz.lists, stride=TALL), :] = values[b]
    parts = stacked(side_by_side(tall_ref, TALL))
    return folded(dot_t(parts, side_by_side(hot_ref, sz.cams)))[: sz.block]


def gather(sz, msg_ref, own, off):
    c, stride = sz.cams, sz.one.stride
    high = sz.devices // 4
    left = []
    for low in range(4):
        rows = []
        for b in range(sz.block):
            x = msg_ref[pl.ds(low * stride + b, high, stride=4 * stride), :]
            rows += [p.astype(F32) for p in split3(x)]
        left.append(jnp.concatenate(rows, axis=0))
    left = jnp.concatenate(left, axis=1).astype(BF16)
    out = [[] for _ in range(sz.block)]
    zeros = jnp.zeros((c, 2 * c), BF16)
    for k in range(0, sz.lists, 2):
        pair = jnp.concatenate([off[k : k + 1], off[k + 1 : k + 2]], axis=1)
        owner = jnp.concatenate([own[k : k + 1], own[k + 1 : k + 2]], axis=1)
        hot = hot_rows(pair, (c, 2 * c))
        low = jnp.broadcast_to((owner & 3).astype(F32).astype(BF16), hot.shape)
        right = [jnp.where(low == jnp.full(hot.shape, at, BF16), hot, zeros) for at in range(4)]
        res = dot(left, jnp.concatenate(right, axis=0))
        here = iota((high, 2 * c), 0) == (owner >> 2)
        for b in range(sz.block):
            at = 3 * high * b
            x = res[at : at + high] + res[at + high : at + 2 * high] + res[at + 2 * high :][:high]
            x = jnp.where(here, x, 0.0)
            x = sum(x[i : i + 8] for i in range(0, high, 8))
            out[b] += [x[:, :c], x[:, c:]]
    return [row_sums(x) for x in out]


def to_lists(sz, values, chunk, lane_ref, tall_ref, col_ref):
    for b in range(sz.block):
        tall_ref[pl.ds(b, sz.lists, stride=TALL), :] = values[b]
    left = jnp.concatenate(split3(tall_ref[...]), axis=1)
    right = jnp.concatenate([side_by_side(lane_ref, sz.cams)] * 3, axis=0)
    res = dot(left, right)
    for k in range(sz.lists):
        lanes = slice(k * sz.cams, (k + 1) * sz.cams)
        out = res[:TALL, lanes]
        for at in range(1, sz.lists):
            out = jnp.where(chunk[k : k + 1] == at, res[at * TALL : (at + 1) * TALL, lanes], out)
        col_ref[k * TALL : (k + 1) * TALL, :] = out
    return [col_ref[pl.ds(b, sz.lists, stride=TALL), :] for b in range(sz.block)]


def first_kernel(
    sz, cols_hbm, table_hbm, rhs_hbm, pre_hbm, up_hbm, diag_hbm,
    msg_ref, own_ref, off_ref, chunk_ref, z_ref, lane_ref, rhs_ref, pre_ref, up_ref, diag_ref,
    cols_ref, table_ref, val_ref, tall_ref, sems,
):
    pairs = (
        (cols_hbm, cols_ref), (table_hbm, table_ref), (rhs_hbm, rhs_ref), (pre_hbm, pre_ref),
        (up_hbm, up_ref), (diag_hbm, diag_ref),
    )
    copies = [pltpu.make_async_copy(a, b, sems.at[i]) for i, (a, b) in enumerate(pairs)]
    for copy in copies:
        copy.start()
    for copy in copies[:4]:
        copy.wait()
    c = sz.cams
    pk = sz.one
    z = block_apply(sz, pre_ref, rhs_ref[...])
    z_ref[...] = z
    for b in range(sz.block):
        at = pl.ds(b, sz.devices, stride=pk.stride)
        msg_ref[at, :] = jnp.broadcast_to(z[b : b + 1], (sz.devices, c))
    cols = cols_ref[...]
    table = table_ref[...]
    height = table.shape[0]
    low = cols & (c - 1)
    high = cols >> sz.shift
    left = jnp.concatenate([table >> sz.shift, table & (c - 1)], axis=0).astype(F32).astype(BF16)
    owns, offs = [], []
    for k in range(sz.lists):
        res = dot(left, hot_rows(low[k : k + 1], (c, c)))
        here = iota((height, c), 0) == high[k : k + 1]
        owns.append(col_sum(jnp.where(here, res[:height], 0.0)))
        offs.append(col_sum(jnp.where(here, res[height:], 0.0)))
    own = jnp.concatenate(owns, axis=0).astype(I32)
    off = jnp.concatenate(offs, axis=0).astype(I32)
    own_ref[...] = own
    off_ref[...] = off

    hots = [
        jnp.where(iota((sz.devices, c), 0) == own[k : k + 1], 1.0, 0.0) for k in range(sz.lists)
    ]
    lane = iota((c, 2 * c), 1)
    before = onehot((iota((c, 2 * c), 0) < lane) | (lane >= c))
    counts = dot(jnp.concatenate(hots, axis=0).astype(BF16), before)
    base = jnp.zeros((sz.devices, c), F32)
    places = []
    for k in range(sz.lists):
        part = counts[k * sz.devices : (k + 1) * sz.devices]
        places.append(col_sum(hots[k] * (part[:, :c] + base)))
        base = base + part[:, c:]
    pos = own * sz.refs + jnp.concatenate(places, axis=0).astype(I32)
    chunk = pos >> sz.shift
    place = pos & (c - 1)
    chunk_ref[...] = chunk
    for k in range(sz.lists):
        lane_ref[k * c : (k + 1) * c, :] = hot_rows(place[k : k + 1], (c, c))

    for copy in copies[4:]:
        copy.wait()
    for at, x in enumerate(bucketed(sz, z, off, up_ref, chunk, lane_ref, val_ref)):
        tall_ref[at * TALL : (at + 1) * TALL, :] = x
    pack(sz, pk, lambda v: tall_ref[pl.ds(v, sz.lists, stride=TALL), :], msg_ref)


def second_kernel(
    sz, got_ref, rhs_ref, z_ref, own_ref, off_ref, chunk_ref, lane_ref, diag_ref, pre_ref, up_ref,
    msg_ref, q_ref, w_ref, hot_ref,
    val_ref, tall_ref, ans_ref, turn_ref,
):
    c = sz.cams
    b, z = rhs_ref[...], z_ref[...]
    values = unpack(sz, sz.one, got_ref, turn_ref)
    wanted = values[sz.block].astype(I32)
    for at in range(sz.lists):
        hot_ref[at * c : (at + 1) * c, :] = hot_rows(wanted[at : at + 1], (c, c))
    pushed = scatter(sz, values, val_ref, hot_ref)
    gathered = gather(sz, got_ref, own_ref[...], off_ref[...])
    q = block_apply(sz, diag_ref, z) + upper_apply(sz, up_ref, gathered) + pushed
    w = block_apply(sz, pre_ref, q)
    q_ref[...] = q
    w_ref[...] = w
    dots = [total(b * z), total(z * q), total(b * w), total(q * w)]
    lane = iota((sz.lists, c), 1) & (sz.refs - 1)
    dot_rows = jnp.zeros((sz.lists, c), F32)
    for at, d in enumerate(dots):
        dot_rows = jnp.where(lane == at, d, dot_rows)
    tall = jnp.concatenate([w, jnp.zeros((TALL - sz.block, c), F32)], axis=0)
    answers = folded(dot(stacked(tall), side_by_side(hot_ref, c)))
    for at in range(sz.lists):
        ans_ref[at * TALL : (at + 1) * TALL, :] = answers[:, at * c : (at + 1) * c]
    for at, x in enumerate(bucketed(sz, w, None, up_ref, chunk_ref[...], lane_ref, val_ref)):
        tall_ref[at * TALL : (at + 1) * TALL, :] = x

    def value_of(v):
        if v < sz.block:
            return tall_ref[pl.ds(v, sz.lists, stride=TALL), :]
        if v == sz.block:
            return dot_rows
        return ans_ref[pl.ds(v - sz.answer, sz.lists, stride=TALL), :]

    pack(sz, sz.two, value_of, msg_ref)


def third_kernel(
    sz, got_ref, rhs_ref, z_ref, q_ref, w_ref, chunk_ref, lane_ref, hot_ref, diag_ref, up_ref,
    part_ref, dot_ref, sol_ref, res_ref, dir_ref, img_ref,
    val_ref, tall_ref, col_ref, turn_ref,
):
    b, z, q, w = rhs_ref[...], z_ref[...], q_ref[...], w_ref[...]
    values = unpack(sz, sz.two, got_ref, turn_ref)
    gathered = to_lists(
        sz, values[sz.answer :], chunk_ref[...], lane_ref, tall_ref, col_ref
    )
    pushed = scatter(sz, values, val_ref, hot_ref)
    y = block_apply(sz, diag_ref, w) + upper_apply(sz, up_ref, gathered) + pushed
    sums = col_sum(values[sz.block])
    lane = iota(sums.shape, 1) & (sz.refs - 1)
    bz, zq, bw, qw = [
        jnp.sum(jnp.where(lane == at, sums, 0.0), axis=1, keepdims=True) for at in range(4)
    ]
    step = bz / zq
    new_dot = bz - step * (zq + bw) + step * step * qw
    beta = new_dot / bz
    direction = (1.0 + beta) * z - step * w
    image = (1.0 + beta) * q - step * y
    sol_ref[...] = step * z
    res_ref[...] = b - step * q
    dir_ref[...] = direction
    img_ref[...] = image
    dot_ref[...] = jnp.broadcast_to(new_dot, dot_ref.shape)
    part_ref[...] = jnp.broadcast_to(total(direction * image), part_ref.shape)


def fourth_kernel(part_ref, dot_ref, sol_ref, res_ref, dir_ref, img_ref, out_ref, left_ref):
    step = dot_ref[...] / col_sum(part_ref[...])
    out_ref[...] = sol_ref[...] + step * dir_ref[...]
    left_ref[...] = res_ref[...] - step * img_ref[...]


def call(body, name, outs, scratch, *args, space=pltpu.VMEM):
    return pl.pallas_call(
        body,
        name=name,
        out_shape=[jax.ShapeDtypeStruct(s, t) for s, t in outs],
        in_specs=[pl.BlockSpec(memory_space=space)] * len(args),
        out_specs=[pl.BlockSpec(memory_space=pltpu.VMEM)] * len(outs),
        scratch_shapes=scratch,
        compiler_params=pltpu.CompilerParams(vmem_limit_bytes=VMEM),
    )(*args)


def exchange(sz, msg, rows):
    blocks = msg.reshape(sz.devices, 1, rows * sz.cams)
    got = lax.all_to_all(blocks, "rows", split_axis=0, concat_axis=0, tiled=True)
    return got.reshape(sz.devices * rows, sz.cams)


def local(right_side, diag_blocks, precond, upper_blocks, block_cols, slot_of_camera):
    block, cams = right_side.shape
    lists = block_cols.shape[0]
    sz = Sizes(block, lists, cams, lax.axis_size("rows"))
    field = ((block, cams), F32)
    index = ((lists, cams), I32)
    hot_type = ((sz.entries, cams), BF16)
    upper_blocks = upper_blocks.transpose(1, 2, 0, 3)
    table = slot_of_camera.reshape(-1, cams)
    tall = pltpu.VMEM((lists * TALL, cams), F32)

    def turns(pk):
        return pltpu.VMEM((pk.rows, pk.groups, sz.devices, cams), F32)

    ins = (block_cols, table, right_side, precond, upper_blocks, diag_blocks)
    msg, own, off, chunk, z, lane, right_side, precond, upper_blocks, diag_blocks = call(
        functools.partial(first_kernel, sz), "first",
        [((sz.devices * sz.one.stride, cams), F32), index, index, index, field, hot_type]
        + [(x.shape, x.dtype) for x in ins[2:]],
        [pltpu.VMEM(x.shape, x.dtype) for x in ins[:2]]
        + [tall, tall, pltpu.SemaphoreType.DMA((len(ins),))],
        *(pltpu.with_memory_space_constraint(x, pltpu.HBM) for x in ins), space=pltpu.HBM,
    )
    got = exchange(sz, msg, sz.one.stride)
    msg, q, w, hot = call(
        functools.partial(second_kernel, sz), "second",
        [((sz.devices * sz.two.stride, cams), F32), field, field, hot_type],
        [tall] * 3 + [turns(sz.one)],
        got, right_side, z, own, off, chunk, lane, diag_blocks, precond, upper_blocks,
    )
    got = exchange(sz, msg, sz.two.stride)
    part, new_dot, sol, res, direction, image = call(
        functools.partial(third_kernel, sz), "third",
        [((sz.devices, cams), F32), ((1, cams), F32)] + [field] * 4,
        [tall] * 3 + [turns(sz.two)],
        got, right_side, z, q, w, chunk, lane, hot, diag_blocks, upper_blocks,
    )
    parts = exchange(sz, part, 1)
    return tuple(
        call(
            fourth_kernel, "fourth", [field, field], [],
            parts, new_dot, sol, res, direction, image,
        )
    )


def solution(mesh):
    return jax.shard_map(
        local,
        mesh=mesh,
        in_specs=(
            P(None, "rows"),
            P(None, None, "rows"),
            P(None, None, "rows"),
            P(None, None, None, "rows"),
            P(None, "rows"),
            P(),
        ),
        out_specs=(P(None, "rows"), P(None, "rows")),
        check_vma=False,
    )
```

```python
import functools
import math

import jax
import jax.numpy as jnp
from jax import lax
from jax.experimental import pallas as pl
from jax.experimental.pallas import tpu as pltpu
from jax.sharding import PartitionSpec as P

VMEM = 24 << 20
TALL = 16
F32 = jnp.float32
BF16 = jnp.bfloat16
I32 = jnp.int32


class Packing:
    def __init__(self, values, refs, cams, skip):
        self.refs = refs
        self.cams = cams
        self.groups = cams // refs
        self.bits = refs.bit_length() - 1
        self.values = values
        self.rows = -(-values // self.groups)
        self.skip = skip
        self.stride = skip + self.rows

    def at(self, v):
        return v // self.rows, v % self.rows

    def group(self, shape):
        return lax.broadcasted_iota(I32, shape, 1) >> self.bits

    def read(self, msg_ref, r, devices):
        return msg_ref[pl.ds(self.skip + r, devices, stride=self.stride), :]


class Sizes:
    def __init__(self, block, lists, cams, devices):
        self.block = block
        self.lists = lists
        self.cams = cams
        self.devices = devices
        self.entries = lists * cams
        self.refs = self.entries // devices
        self.shift = cams.bit_length() - 1
        assert cams == 1 << self.shift and self.refs * devices == self.entries
        assert self.refs == 1 << (self.refs.bit_length() - 1) and lists <= 8
        self.one = Packing(block + 1, self.refs, cams, block)
        self.two = Packing(2 * block + 1, self.refs, cams, 0)
        self.answer = block + 1
        assert self.answer % self.two.rows == 0


def split3(x):
    hi = x.astype(BF16)
    rest = x - hi.astype(F32)
    mid = rest.astype(BF16)
    low = (rest - mid.astype(F32)).astype(BF16)
    return hi, mid, low


def stacked(x):
    parts = [p.astype(F32) for p in split3(x)]
    row = lax.broadcasted_iota(I32, (8, x.shape[1]), 0)
    tail = parts[0][8:]
    for at in (1, 2):
        tail = jnp.where(row < 2 * at, tail, pltpu.roll(parts[at][8:], 2 * at, 0))
    return jnp.concatenate([p[:8] for p in parts] + [tail], axis=0).astype(BF16)


def folded(x):
    tail = x[24:]
    tail = tail + pltpu.roll(tail, 6, 0) + pltpu.roll(tail, 4, 0)
    return jnp.concatenate([x[:8] + x[8:16] + x[16:24], tail], axis=0)


def row_sums(arrays):
    shape = arrays[0].shape
    if len(arrays) != 8 or shape[0] != 8:
        return jnp.concatenate([col_sum(x) for x in arrays], axis=0)
    row = lax.broadcasted_iota(I32, shape, 0)
    step = 4
    while step:
        low = (row & step) == 0
        arrays = [
            jnp.where(low, a, b)
            + jnp.where(low, pltpu.roll(a, 8 - step, 0), pltpu.roll(b, step, 0))
            for a, b in zip(arrays[: len(arrays) // 2], arrays[len(arrays) // 2 :])
        ]
        step //= 2
    return arrays[0]


def dot(a, b):
    return lax.dot_general(a, b, (((1,), (0,)), ((), ())), preferred_element_type=F32)


def dot_t(a, b):
    return lax.dot_general(a, b, (((1,), (1,)), ((), ())), preferred_element_type=F32)


def iota(shape, axis):
    return lax.broadcasted_iota(I32, shape, axis)


def onehot(mask):
    return jnp.where(mask, 1.0, 0.0).astype(BF16)


def hot_rows(places, shape):
    rows = iota(shape, 0).astype(F32).astype(BF16)
    same = rows == jnp.broadcast_to(places.astype(F32).astype(BF16), shape)
    return jnp.where(same, jnp.ones(shape, BF16), jnp.zeros(shape, BF16))


def col_sum(x):
    return jnp.sum(x, axis=0, keepdims=True)


def total(x):
    return jnp.sum(col_sum(x), axis=1, keepdims=True)


def block_apply(sz, blocks_ref, v):
    acc = blocks_ref[0] * v[0:1]
    for b in range(1, sz.block):
        acc = acc + blocks_ref[b] * v[b : b + 1]
    return acc


def upper_apply(sz, up_ref, gathered):
    rows = []
    for a in range(sz.block):
        acc = up_ref[a, 0] * gathered[0]
        for b in range(1, sz.block):
            acc = acc + up_ref[a, b] * gathered[b]
        rows.append(acc)
    return jnp.concatenate([row_sums(rows[:8])] + [col_sum(x) for x in rows[8:]], axis=0)


def side_by_side(ref, height):
    blocks = [ref[at : at + height, :] for at in range(0, ref.shape[0], height)]
    return jnp.concatenate(blocks, axis=1)


def bucketed(sz, v, off, up_ref, chunk, lane_ref, val_ref):
    for b in range(sz.block):
        acc = up_ref[0, b] * v[0:1]
        for a in range(1, sz.block):
            acc = acc + up_ref[a, b] * v[a : a + 1]
        val_ref[pl.ds(b, sz.lists, stride=TALL), :] = acc
    if off is not None:
        val_ref[pl.ds(sz.block, sz.lists, stride=TALL), :] = off.astype(F32)
    parts = stacked(side_by_side(val_ref, TALL))
    where = jnp.concatenate([chunk[k : k + 1] for k in range(sz.lists)], axis=1)
    where = jnp.broadcast_to(where.astype(F32).astype(BF16), parts.shape)
    left = [
        jnp.where(where == jnp.full(parts.shape, at, BF16), parts, jnp.zeros(parts.shape, BF16))
        for at in range(sz.lists)
    ]
    res = dot_t(jnp.concatenate(left, axis=0), side_by_side(lane_ref, sz.cams))
    height = parts.shape[0]
    return [folded(res[at * height : (at + 1) * height]) for at in range(sz.lists)]


def pack(sz, pk, value_of, msg_ref):
    group = pk.group((sz.lists, sz.cams))
    values = [value_of(v) for v in range(pk.values)]
    turned = [
        [pltpu.roll(x, t * sz.refs, 1) if t else x for t in range(pk.groups)] for x in values
    ]
    for s in range(pk.groups):
        for r in range(pk.rows):
            out = jnp.zeros((sz.lists, sz.cams), F32)
            for g in range(pk.groups):
                v = g * pk.rows + r
                if v < pk.values:
                    out = jnp.where(group == g, turned[v][(g - s) % pk.groups], out)
            at = pl.ds(s * pk.stride + pk.skip + r, sz.lists, stride=pk.groups * pk.stride)
            msg_ref[at, :] = out


def unpack(sz, pk, msg_ref, turn_ref):
    for r in range(pk.rows):
        x = pk.read(msg_ref, r, sz.devices)
        for t in range(pk.groups):
            turn_ref[r, t] = pltpu.roll(x, t * sz.refs, 1) if t else x
    group = pk.group((sz.lists, sz.cams))
    out = []
    for v in range(pk.values):
        g, r = pk.at(v)
        value = None
        for s in range(pk.groups):
            part = turn_ref[r, (s - g) % pk.groups, pl.ds(s, sz.lists, stride=pk.groups), :]
            value = part if value is None else jnp.where(group == s, part, value)
        out.append(value)
    return out


def scatter(sz, values, tall_ref, hot_ref):
    for b in range(sz.block):
        tall_ref[pl.ds(b, sz.lists, stride=TALL), :] = values[b]
    parts = stacked(side_by_side(tall_ref, TALL))
    return folded(dot_t(parts, side_by_side(hot_ref, sz.cams)))[: sz.block]


def gather(sz, msg_ref, own, off):
    c, stride = sz.cams, sz.one.stride
    high = sz.devices // 4
    left = []
    for low in range(4):
        rows = []
        for b in range(sz.block):
            x = msg_ref[pl.ds(low * stride + b, high, stride=4 * stride), :]
            rows += [p.astype(F32) for p in split3(x)]
        left.append(jnp.concatenate(rows, axis=0))
    left = jnp.concatenate(left, axis=1).astype(BF16)
    out = [[] for _ in range(sz.block)]
    zeros = jnp.zeros((c, 2 * c), BF16)
    for k in range(0, sz.lists, 2):
        pair = jnp.concatenate([off[k : k + 1], off[k + 1 : k + 2]], axis=1)
        owner = jnp.concatenate([own[k : k + 1], own[k + 1 : k + 2]], axis=1)
        hot = hot_rows(pair, (c, 2 * c))
        low = jnp.broadcast_to((owner & 3).astype(F32).astype(BF16), hot.shape)
        right = [jnp.where(low == jnp.full(hot.shape, at, BF16), hot, zeros) for at in range(4)]
        res = dot(left, jnp.concatenate(right, axis=0))
        here = iota((high, 2 * c), 0) == (owner >> 2)
        for b in range(sz.block):
            at = 3 * high * b
            x = res[at : at + high] + res[at + high : at + 2 * high] + res[at + 2 * high :][:high]
            x = jnp.where(here, x, 0.0)
            x = sum(x[i : i + 8] for i in range(0, high, 8))
            out[b] += [x[:, :c], x[:, c:]]
    return [row_sums(x) for x in out]


def to_lists(sz, values, chunk, lane_ref, tall_ref, col_ref):
    for b in range(sz.block):
        tall_ref[pl.ds(b, sz.lists, stride=TALL), :] = values[b]
    left = jnp.concatenate(split3(tall_ref[...]), axis=1)
    right = jnp.concatenate([side_by_side(lane_ref, sz.cams)] * 3, axis=0)
    res = dot(left, right)
    for k in range(sz.lists):
        lanes = slice(k * sz.cams, (k + 1) * sz.cams)
        out = res[:TALL, lanes]
        for at in range(1, sz.lists):
            out = jnp.where(chunk[k : k + 1] == at, res[at * TALL : (at + 1) * TALL, lanes], out)
        col_ref[k * TALL : (k + 1) * TALL, :] = out
    return [col_ref[pl.ds(b, sz.lists, stride=TALL), :] for b in range(sz.block)]


def first_kernel(
    sz, cols_hbm, table_hbm, rhs_hbm, pre_hbm, up_hbm, diag_hbm,
    msg_ref, own_ref, off_ref, chunk_ref, z_ref, lane_ref, rhs_ref, pre_ref, up_ref, diag_ref,
    cols_ref, table_ref, val_ref, tall_ref, sems,
):
    pairs = (
        (cols_hbm, cols_ref), (table_hbm, table_ref), (rhs_hbm, rhs_ref), (pre_hbm, pre_ref),
        (up_hbm, up_ref), (diag_hbm, diag_ref),
    )
    copies = [pltpu.make_async_copy(a, b, sems.at[i]) for i, (a, b) in enumerate(pairs)]
    for copy in copies:
        copy.start()
    for copy in copies[:4]:
        copy.wait()
    c = sz.cams
    pk = sz.one
    z = block_apply(sz, pre_ref, rhs_ref[...])
    z_ref[...] = z
    for b in range(sz.block):
        at = pl.ds(b, sz.devices, stride=pk.stride)
        msg_ref[at, :] = jnp.broadcast_to(z[b : b + 1], (sz.devices, c))
    cols = cols_ref[...]
    table = table_ref[...]
    height = table.shape[0]
    low = cols & (c - 1)
    high = cols >> sz.shift
    left = jnp.concatenate([table >> sz.shift, table & (c - 1)], axis=0).astype(F32).astype(BF16)
    owns, offs = [], []
    for k in range(sz.lists):
        res = dot(left, hot_rows(low[k : k + 1], (c, c)))
        here = iota((height, c), 0) == high[k : k + 1]
        owns.append(col_sum(jnp.where(here, res[:height], 0.0)))
        offs.append(col_sum(jnp.where(here, res[height:], 0.0)))
    own = jnp.concatenate(owns, axis=0).astype(I32)
    off = jnp.concatenate(offs, axis=0).astype(I32)
    own_ref[...] = own
    off_ref[...] = off

    hots = [
        jnp.where(iota((sz.devices, c), 0) == own[k : k + 1], 1.0, 0.0) for k in range(sz.lists)
    ]
    lane = iota((c, 2 * c), 1)
    before = onehot((iota((c, 2 * c), 0) < lane) | (lane >= c))
    counts = dot(jnp.concatenate(hots, axis=0).astype(BF16), before)
    base = jnp.zeros((sz.devices, c), F32)
    places = []
    for k in range(sz.lists):
        part = counts[k * sz.devices : (k + 1) * sz.devices]
        places.append(col_sum(hots[k] * (part[:, :c] + base)))
        base = base + part[:, c:]
    pos = own * sz.refs + jnp.concatenate(places, axis=0).astype(I32)
    chunk = pos >> sz.shift
    place = pos & (c - 1)
    chunk_ref[...] = chunk
    for k in range(sz.lists):
        lane_ref[k * c : (k + 1) * c, :] = hot_rows(place[k : k + 1], (c, c))

    for copy in copies[4:]:
        copy.wait()
    for at, x in enumerate(bucketed(sz, z, off, up_ref, chunk, lane_ref, val_ref)):
        tall_ref[at * TALL : (at + 1) * TALL, :] = x
    pack(sz, pk, lambda v: tall_ref[pl.ds(v, sz.lists, stride=TALL), :], msg_ref)


def second_kernel(
    sz, got_ref, rhs_ref, z_ref, own_ref, off_ref, chunk_ref, lane_ref, diag_ref, pre_ref, up_ref,
    msg_ref, q_ref, w_ref, hot_ref,
    val_ref, tall_ref, ans_ref, turn_ref,
):
    c = sz.cams
    b, z = rhs_ref[...], z_ref[...]
    values = unpack(sz, sz.one, got_ref, turn_ref)
    wanted = values[sz.block].astype(I32)
    for at in range(sz.lists):
        hot_ref[at * c : (at + 1) * c, :] = hot_rows(wanted[at : at + 1], (c, c))
    pushed = scatter(sz, values, val_ref, hot_ref)
    gathered = gather(sz, got_ref, own_ref[...], off_ref[...])
    q = block_apply(sz, diag_ref, z) + upper_apply(sz, up_ref, gathered) + pushed
    w = block_apply(sz, pre_ref, q)
    q_ref[...] = q
    w_ref[...] = w
    dots = [total(b * z), total(z * q)]
    lane = iota((sz.lists, c), 1) & (sz.refs - 1)
    dot_rows = jnp.zeros((sz.lists, c), F32)
    for at, d in enumerate(dots):
        dot_rows = jnp.where(lane == at, d, dot_rows)
    tall = jnp.concatenate([w, jnp.zeros((TALL - sz.block, c), F32)], axis=0)
    answers = folded(dot(stacked(tall), side_by_side(hot_ref, c)))
    for at in range(sz.lists):
        ans_ref[at * TALL : (at + 1) * TALL, :] = answers[:, at * c : (at + 1) * c]
    for at, x in enumerate(bucketed(sz, w, None, up_ref, chunk_ref[...], lane_ref, val_ref)):
        tall_ref[at * TALL : (at + 1) * TALL, :] = x

    def value_of(v):
        if v < sz.block:
            return tall_ref[pl.ds(v, sz.lists, stride=TALL), :]
        if v == sz.block:
            return dot_rows
        return ans_ref[pl.ds(v - sz.answer, sz.lists, stride=TALL), :]

    pack(sz, sz.two, value_of, msg_ref)


def third_kernel(
    sz, got_ref, rhs_ref, z_ref, q_ref, w_ref, chunk_ref, lane_ref, hot_ref, diag_ref, up_ref,
    part_ref, known_ref, res_ref, pre_ref, img_ref,
    val_ref, tall_ref, col_ref, turn_ref,
):
    b, z, q, w = rhs_ref[...], z_ref[...], q_ref[...], w_ref[...]
    values = unpack(sz, sz.two, got_ref, turn_ref)
    sums = col_sum(values[sz.block])
    lane = iota(sums.shape, 1) & (sz.refs - 1)
    res_dot, curve = [
        jnp.sum(jnp.where(lane == at, sums, 0.0), axis=1, keepdims=True) for at in range(2)
    ]
    step = res_dot / curve
    gathered = to_lists(
        sz, values[sz.answer :], chunk_ref[...], lane_ref, tall_ref, col_ref
    )
    pushed = scatter(sz, values, val_ref, hot_ref)
    y = block_apply(sz, diag_ref, w) + upper_apply(sz, up_ref, gathered) + pushed
    residual = b - step * q
    pre = z - step * w
    image = q - step * y
    res_ref[...] = residual
    pre_ref[...] = pre
    img_ref[...] = image
    known = [res_dot, curve, step]
    known_ref[...] = jnp.concatenate([jnp.broadcast_to(x, (1, sz.cams)) for x in known], axis=0)
    dots = [total(residual * pre), total(pre * image), total(pre * q + z * image)]
    row = dots[2]
    lane = iota((1, sz.cams), 1) & 3
    for at in (1, 0):
        row = jnp.where(lane == at, dots[at], row)
    part_ref[...] = jnp.broadcast_to(row, part_ref.shape)


def fourth_kernel(
    part_ref, known_ref, z_ref, q_ref, res_ref, pre_ref, img_ref, out_ref, left_ref
):
    sums = col_sum(part_ref[...])
    lane = iota(sums.shape, 1)
    new_dot, pre_curve, cross = [
        jnp.sum(jnp.where(lane == at, sums, 0.0), axis=1, keepdims=True) for at in range(3)
    ]
    res_dot, curve, step = known_ref[0:1], known_ref[1:2], known_ref[2:3]
    z = z_ref[...]
    beta = new_dot / res_dot
    next_step = new_dot / (pre_curve + beta * (cross + beta * curve))
    out_ref[...] = step * z + next_step * (pre_ref[...] + beta * z)
    left_ref[...] = res_ref[...] - next_step * (img_ref[...] + beta * q_ref[...])


def call(body, name, outs, scratch, *args, space=pltpu.VMEM):
    return pl.pallas_call(
        body,
        name=name,
        out_shape=[jax.ShapeDtypeStruct(s, t) for s, t in outs],
        in_specs=[pl.BlockSpec(memory_space=space)] * len(args),
        out_specs=[pl.BlockSpec(memory_space=pltpu.VMEM)] * len(outs),
        scratch_shapes=scratch,
        compiler_params=pltpu.CompilerParams(vmem_limit_bytes=VMEM),
    )(*args)


def exchange(sz, msg, rows):
    blocks = msg.reshape(sz.devices, 1, rows * sz.cams)
    got = lax.all_to_all(blocks, "rows", split_axis=0, concat_axis=0, tiled=True)
    return got.reshape(sz.devices * rows, sz.cams)


def local(right_side, diag_blocks, precond, upper_blocks, block_cols, slot_of_camera):
    block, cams = right_side.shape
    lists = block_cols.shape[0]
    sz = Sizes(block, lists, cams, lax.axis_size("rows"))
    field = ((block, cams), F32)
    index = ((lists, cams), I32)
    hot_type = ((sz.entries, cams), BF16)
    upper_blocks = upper_blocks.transpose(1, 2, 0, 3)
    table = slot_of_camera.reshape(-1, cams)
    tall = pltpu.VMEM((lists * TALL, cams), F32)

    def turns(pk):
        return pltpu.VMEM((pk.rows, pk.groups, sz.devices, cams), F32)

    ins = (block_cols, table, right_side, precond, upper_blocks, diag_blocks)
    msg, own, off, chunk, z, lane, right_side, precond, upper_blocks, diag_blocks = call(
        functools.partial(first_kernel, sz), "first",
        [((sz.devices * sz.one.stride, cams), F32), index, index, index, field, hot_type]
        + [(x.shape, x.dtype) for x in ins[2:]],
        [pltpu.VMEM(x.shape, x.dtype) for x in ins[:2]]
        + [tall, tall, pltpu.SemaphoreType.DMA((len(ins),))],
        *(pltpu.with_memory_space_constraint(x, pltpu.HBM) for x in ins), space=pltpu.HBM,
    )
    got = exchange(sz, msg, sz.one.stride)
    msg, q, w, hot = call(
        functools.partial(second_kernel, sz), "second",
        [((sz.devices * sz.two.stride, cams), F32), field, field, hot_type],
        [tall] * 3 + [turns(sz.one)],
        got, right_side, z, own, off, chunk, lane, diag_blocks, precond, upper_blocks,
    )
    got = exchange(sz, msg, sz.two.stride)
    part, known, res, pre, image = call(
        functools.partial(third_kernel, sz), "third",
        [((sz.devices, cams), F32), ((3, cams), F32)] + [field] * 3,
        [tall] * 3 + [turns(sz.two)],
        got, right_side, z, q, w, chunk, lane, hot, diag_blocks, upper_blocks,
    )
    parts = exchange(sz, part, 1)
    return tuple(
        call(
            fourth_kernel, "fourth", [field, field], [],
            parts, known, z, q, res, pre, image,
        )
    )


def solution(mesh):
    return jax.shard_map(
        local,
        mesh=mesh,
        in_specs=(
            P(None, "rows"),
            P(None, None, "rows"),
            P(None, None, "rows"),
            P(None, None, None, "rows"),
            P(None, "rows"),
            P(),
        ),
        out_specs=(P(None, "rows"), P(None, "rows")),
        check_vma=False,
    )
```

```python
import functools
import math

import jax
import jax.numpy as jnp
from jax import lax
from jax.experimental import pallas as pl
from jax.experimental.pallas import tpu as pltpu
from jax.sharding import PartitionSpec as P

VMEM = 24 << 20
TALL = 16
F32 = jnp.float32
BF16 = jnp.bfloat16
I32 = jnp.int32


class Packing:
    def __init__(self, values, refs, cams, skip):
        self.refs = refs
        self.cams = cams
        self.groups = cams // refs
        self.bits = refs.bit_length() - 1
        self.values = values
        self.rows = -(-values // self.groups)
        self.skip = skip
        self.stride = skip + self.rows

    def at(self, v):
        return v // self.rows, v % self.rows

    def group(self, shape):
        return lax.broadcasted_iota(I32, shape, 1) >> self.bits

    def read(self, msg_ref, r, devices):
        return msg_ref[pl.ds(self.skip + r, devices, stride=self.stride), :]


class Sizes:
    def __init__(self, block, lists, cams, devices):
        self.block = block
        self.lists = lists
        self.cams = cams
        self.devices = devices
        self.entries = lists * cams
        self.refs = self.entries // devices
        self.shift = cams.bit_length() - 1
        assert cams == 1 << self.shift and self.refs * devices == self.entries
        assert self.refs == 1 << (self.refs.bit_length() - 1) and lists <= 8
        self.one = Packing(block + 1, self.refs, cams, block)
        self.two = Packing(2 * block + 1, self.refs, cams, 0)
        self.answer = block + 1
        assert self.answer % self.two.rows == 0


def split3(x):
    hi = x.astype(BF16)
    rest = x - hi.astype(F32)
    mid = rest.astype(BF16)
    low = (rest - mid.astype(F32)).astype(BF16)
    return hi, mid, low


def stacked(x):
    parts = [p.astype(F32) for p in split3(x)]
    row = lax.broadcasted_iota(I32, (8, x.shape[1]), 0)
    tail = parts[0][8:]
    for at in (1, 2):
        tail = jnp.where(row < 2 * at, tail, pltpu.roll(parts[at][8:], 2 * at, 0))
    return jnp.concatenate([p[:8] for p in parts] + [tail], axis=0).astype(BF16)


def folded(x):
    tail = x[24:]
    tail = tail + pltpu.roll(tail, 6, 0) + pltpu.roll(tail, 4, 0)
    return jnp.concatenate([x[:8] + x[8:16] + x[16:24], tail], axis=0)


def row_sums(arrays):
    shape = arrays[0].shape
    if len(arrays) != 8 or shape[0] != 8:
        return jnp.concatenate([col_sum(x) for x in arrays], axis=0)
    row = lax.broadcasted_iota(I32, shape, 0)
    step = 4
    while step:
        low = (row & step) == 0
        arrays = [
            jnp.where(low, a, b)
            + jnp.where(low, pltpu.roll(a, 8 - step, 0), pltpu.roll(b, step, 0))
            for a, b in zip(arrays[: len(arrays) // 2], arrays[len(arrays) // 2 :])
        ]
        step //= 2
    return arrays[0]


def dot(a, b):
    return lax.dot_general(a, b, (((1,), (0,)), ((), ())), preferred_element_type=F32)


def dot_t(a, b):
    return lax.dot_general(a, b, (((1,), (1,)), ((), ())), preferred_element_type=F32)


def iota(shape, axis):
    return lax.broadcasted_iota(I32, shape, axis)


def onehot(mask):
    return jnp.where(mask, 1.0, 0.0).astype(BF16)


def hot_rows(places, shape):
    rows = iota(shape, 0).astype(F32).astype(BF16)
    same = rows == jnp.broadcast_to(places.astype(F32).astype(BF16), shape)
    return jnp.where(same, jnp.ones(shape, BF16), jnp.zeros(shape, BF16))


def col_sum(x):
    return jnp.sum(x, axis=0, keepdims=True)


def total(x):
    return jnp.sum(col_sum(x), axis=1, keepdims=True)


def block_apply(sz, blocks_ref, v):
    acc = blocks_ref[0] * v[0:1]
    for b in range(1, sz.block):
        acc = acc + blocks_ref[b] * v[b : b + 1]
    return acc


def upper_apply(sz, up_ref, gathered):
    rows = []
    for a in range(sz.block):
        acc = up_ref[a, 0] * gathered[0]
        for b in range(1, sz.block):
            acc = acc + up_ref[a, b] * gathered[b]
        rows.append(acc)
    return jnp.concatenate([row_sums(rows[:8])] + [col_sum(x) for x in rows[8:]], axis=0)


def side_by_side(ref, height):
    blocks = [ref[at : at + height, :] for at in range(0, ref.shape[0], height)]
    return jnp.concatenate(blocks, axis=1)


def bucketed(sz, v, off, up_ref, chunk, lane_ref, val_ref):
    for b in range(sz.block):
        acc = up_ref[0, b] * v[0:1]
        for a in range(1, sz.block):
            acc = acc + up_ref[a, b] * v[a : a + 1]
        val_ref[pl.ds(b, sz.lists, stride=TALL), :] = acc
    if off is not None:
        val_ref[pl.ds(sz.block, sz.lists, stride=TALL), :] = off.astype(F32)
    parts = stacked(side_by_side(val_ref, TALL))
    where = jnp.concatenate([chunk[k : k + 1] for k in range(sz.lists)], axis=1)
    where = jnp.broadcast_to(where.astype(F32).astype(BF16), parts.shape)
    left = [
        jnp.where(where == jnp.full(parts.shape, at, BF16), parts, jnp.zeros(parts.shape, BF16))
        for at in range(sz.lists)
    ]
    res = dot_t(jnp.concatenate(left, axis=0), side_by_side(lane_ref, sz.cams))
    height = parts.shape[0]
    return [folded(res[at * height : (at + 1) * height]) for at in range(sz.lists)]


def pack(sz, pk, value_of, msg_ref):
    group = pk.group((sz.lists, sz.cams))
    values = [value_of(v) for v in range(pk.values)]
    turned = [
        [pltpu.roll(x, t * sz.refs, 1) if t else x for t in range(pk.groups)] for x in values
    ]
    for s in range(pk.groups):
        for r in range(pk.rows):
            out = jnp.zeros((sz.lists, sz.cams), F32)
            for g in range(pk.groups):
                v = g * pk.rows + r
                if v < pk.values:
                    out = jnp.where(group == g, turned[v][(g - s) % pk.groups], out)
            at = pl.ds(s * pk.stride + pk.skip + r, sz.lists, stride=pk.groups * pk.stride)
            msg_ref[at, :] = out


def unpack(sz, pk, msg_ref, turn_ref):
    for r in range(pk.rows):
        x = pk.read(msg_ref, r, sz.devices)
        for t in range(pk.groups):
            turn_ref[r, t] = pltpu.roll(x, t * sz.refs, 1) if t else x
    group = pk.group((sz.lists, sz.cams))
    out = []
    for v in range(pk.values):
        g, r = pk.at(v)
        value = None
        for s in range(pk.groups):
            part = turn_ref[r, (s - g) % pk.groups, pl.ds(s, sz.lists, stride=pk.groups), :]
            value = part if value is None else jnp.where(group == s, part, value)
        out.append(value)
    return out


def scatter(sz, values, tall_ref, hot_ref):
    for b in range(sz.block):
        tall_ref[pl.ds(b, sz.lists, stride=TALL), :] = values[b]
    parts = stacked(side_by_side(tall_ref, TALL))
    return folded(dot_t(parts, side_by_side(hot_ref, sz.cams)))[: sz.block]


def gather(sz, msg_ref, own, off):
    c, stride = sz.cams, sz.one.stride
    high = sz.devices // 4
    left = []
    for low in range(4):
        rows = []
        for b in range(sz.block):
            x = msg_ref[pl.ds(low * stride + b, high, stride=4 * stride), :]
            rows += [p.astype(F32) for p in split3(x)]
        left.append(jnp.concatenate(rows, axis=0))
    left = jnp.concatenate(left, axis=1).astype(BF16)
    out = [[] for _ in range(sz.block)]
    zeros = jnp.zeros((c, 2 * c), BF16)
    for k in range(0, sz.lists, 2):
        pair = jnp.concatenate([off[k : k + 1], off[k + 1 : k + 2]], axis=1)
        owner = jnp.concatenate([own[k : k + 1], own[k + 1 : k + 2]], axis=1)
        hot = hot_rows(pair, (c, 2 * c))
        low = jnp.broadcast_to((owner & 3).astype(F32).astype(BF16), hot.shape)
        right = [jnp.where(low == jnp.full(hot.shape, at, BF16), hot, zeros) for at in range(4)]
        res = dot(left, jnp.concatenate(right, axis=0))
        here = iota((high, 2 * c), 0) == (owner >> 2)
        for b in range(sz.block):
            at = 3 * high * b
            x = res[at : at + high] + res[at + high : at + 2 * high] + res[at + 2 * high :][:high]
            x = jnp.where(here, x, 0.0)
            x = sum(x[i : i + 8] for i in range(0, high, 8))
            out[b] += [x[:, :c], x[:, c:]]
    return [row_sums(x) for x in out]


def to_lists(sz, values, chunk, lane_ref, tall_ref, col_ref):
    for b in range(sz.block):
        tall_ref[pl.ds(b, sz.lists, stride=TALL), :] = values[b]
    left = jnp.concatenate(split3(tall_ref[...]), axis=1)
    right = jnp.concatenate([side_by_side(lane_ref, sz.cams)] * 3, axis=0)
    res = dot(left, right)
    for k in range(sz.lists):
        lanes = slice(k * sz.cams, (k + 1) * sz.cams)
        out = res[:TALL, lanes]
        for at in range(1, sz.lists):
            out = jnp.where(chunk[k : k + 1] == at, res[at * TALL : (at + 1) * TALL, lanes], out)
        col_ref[k * TALL : (k + 1) * TALL, :] = out
    return [col_ref[pl.ds(b, sz.lists, stride=TALL), :] for b in range(sz.block)]


def first_kernel(
    sz, cols_hbm, table_hbm, rhs_hbm, pre_hbm, up_hbm, diag_hbm,
    msg_ref, own_ref, off_ref, chunk_ref, z_ref, lane_ref, rhs_ref, pre_ref, up_ref, diag_ref,
    cols_ref, table_ref, val_ref, tall_ref, sems,
):
    pairs = (
        (cols_hbm, cols_ref), (table_hbm, table_ref), (rhs_hbm, rhs_ref), (pre_hbm, pre_ref),
        (up_hbm, up_ref), (diag_hbm, diag_ref),
    )
    copies = [pltpu.make_async_copy(a, b, sems.at[i]) for i, (a, b) in enumerate(pairs)]
    for copy in copies:
        copy.start()
    for copy in copies[:4]:
        copy.wait()
    c = sz.cams
    pk = sz.one
    z = block_apply(sz, pre_ref, rhs_ref[...])
    z_ref[...] = z
    for b in range(sz.block):
        at = pl.ds(b, sz.devices, stride=pk.stride)
        msg_ref[at, :] = jnp.broadcast_to(z[b : b + 1], (sz.devices, c))
    cols = cols_ref[...]
    table = table_ref[...]
    height = table.shape[0]
    low = cols & (c - 1)
    high = cols >> sz.shift
    left = jnp.concatenate([table >> sz.shift, table & (c - 1)], axis=0).astype(F32).astype(BF16)
    owns, offs = [], []
    for k in range(sz.lists):
        res = dot(left, hot_rows(low[k : k + 1], (c, c)))
        here = iota((height, c), 0) == high[k : k + 1]
        owns.append(col_sum(jnp.where(here, res[:height], 0.0)))
        offs.append(col_sum(jnp.where(here, res[height:], 0.0)))
    own = jnp.concatenate(owns, axis=0).astype(I32)
    off = jnp.concatenate(offs, axis=0).astype(I32)
    own_ref[...] = own
    off_ref[...] = off

    hots = [
        jnp.where(iota((sz.devices, c), 0) == own[k : k + 1], 1.0, 0.0) for k in range(sz.lists)
    ]
    lane = iota((c, 2 * c), 1)
    before = onehot((iota((c, 2 * c), 0) < lane) | (lane >= c))
    counts = dot(jnp.concatenate(hots, axis=0).astype(BF16), before)
    base = jnp.zeros((sz.devices, c), F32)
    places = []
    for k in range(sz.lists):
        part = counts[k * sz.devices : (k + 1) * sz.devices]
        places.append(col_sum(hots[k] * (part[:, :c] + base)))
        base = base + part[:, c:]
    pos = own * sz.refs + jnp.concatenate(places, axis=0).astype(I32)
    chunk = pos >> sz.shift
    place = pos & (c - 1)
    chunk_ref[...] = chunk
    for k in range(sz.lists):
        lane_ref[k * c : (k + 1) * c, :] = hot_rows(place[k : k + 1], (c, c))

    for copy in copies[4:]:
        copy.wait()
    for at, x in enumerate(bucketed(sz, z, off, up_ref, chunk, lane_ref, val_ref)):
        tall_ref[at * TALL : (at + 1) * TALL, :] = x
    pack(sz, pk, lambda v: tall_ref[pl.ds(v, sz.lists, stride=TALL), :], msg_ref)


def second_kernel(
    sz, got_ref, rhs_ref, z_ref, own_ref, off_ref, chunk_ref, lane_ref, diag_ref, pre_ref, up_ref,
    msg_ref, q_ref, side_ref, hot_ref,
    val_ref, tall_ref, ans_ref, turn_ref,
):
    c = sz.cams
    b, z = rhs_ref[...], z_ref[...]
    values = unpack(sz, sz.one, got_ref, turn_ref)
    wanted = values[sz.block].astype(I32)
    for at in range(sz.lists):
        hot_ref[at * c : (at + 1) * c, :] = hot_rows(wanted[at : at + 1], (c, c))
    pushed = scatter(sz, values, val_ref, hot_ref)
    gathered = gather(sz, got_ref, own_ref[...], off_ref[...])
    side = upper_apply(sz, up_ref, gathered) + pushed
    q = block_apply(sz, diag_ref, z) + side
    w = block_apply(sz, pre_ref, q)
    q_ref[...] = q
    side_ref[...] = side
    dots = [total(b * z), total(z * q)]
    lane = iota((sz.lists, c), 1) & (sz.refs - 1)
    dot_rows = jnp.zeros((sz.lists, c), F32)
    for at, d in enumerate(dots):
        dot_rows = jnp.where(lane == at, d, dot_rows)
    tall = jnp.concatenate([w, jnp.zeros((TALL - sz.block, c), F32)], axis=0)
    answers = folded(dot(stacked(tall), side_by_side(hot_ref, c)))
    for at in range(sz.lists):
        ans_ref[at * TALL : (at + 1) * TALL, :] = answers[:, at * c : (at + 1) * c]
    for at, x in enumerate(bucketed(sz, w, None, up_ref, chunk_ref[...], lane_ref, val_ref)):
        tall_ref[at * TALL : (at + 1) * TALL, :] = x

    def value_of(v):
        if v < sz.block:
            return tall_ref[pl.ds(v, sz.lists, stride=TALL), :]
        if v == sz.block:
            return dot_rows
        return ans_ref[pl.ds(v - sz.answer, sz.lists, stride=TALL), :]

    pack(sz, sz.two, value_of, msg_ref)


def third_kernel(
    sz, got_ref, rhs_ref, z_ref, q_ref, side_ref, chunk_ref, lane_ref, hot_ref,
    diag_ref, pre_ref, up_ref,
    part_ref, known_ref, res_ref, dir_ref, img_ref,
    val_ref, tall_ref, col_ref, turn_ref,
):
    b, z, q = rhs_ref[...], z_ref[...], q_ref[...]
    values = unpack(sz, sz.two, got_ref, turn_ref)
    sums = col_sum(values[sz.block])
    lane = iota(sums.shape, 1) & (sz.refs - 1)
    res_dot, curve = [
        jnp.sum(jnp.where(lane == at, sums, 0.0), axis=1, keepdims=True) for at in range(2)
    ]
    step = res_dot / curve
    residual = b - step * q
    pre = block_apply(sz, pre_ref, residual)
    gathered = to_lists(
        sz, values[sz.answer :], chunk_ref[...], lane_ref, tall_ref, col_ref
    )
    pushed = scatter(sz, values, val_ref, hot_ref)
    side = side_ref[...] - step * (upper_apply(sz, up_ref, gathered) + pushed)
    image = block_apply(sz, diag_ref, pre) + side
    res_ref[...] = residual
    dir_ref[...] = pre
    img_ref[...] = image
    known = [res_dot, curve, step]
    known_ref[...] = jnp.concatenate([jnp.broadcast_to(x, (1, sz.cams)) for x in known], axis=0)
    dots = [total(residual * pre), total(pre * image), total(pre * q + z * image)]
    row = dots[2]
    lane = iota((1, sz.cams), 1) & 3
    for at in (1, 0):
        row = jnp.where(lane == at, dots[at], row)
    part_ref[...] = jnp.broadcast_to(row, part_ref.shape)


def fourth_kernel(
    part_ref, known_ref, z_ref, q_ref, res_ref, pre_ref, img_ref, out_ref, left_ref
):
    sums = col_sum(part_ref[...])
    lane = iota(sums.shape, 1)
    new_dot, pre_curve, cross = [
        jnp.sum(jnp.where(lane == at, sums, 0.0), axis=1, keepdims=True) for at in range(3)
    ]
    res_dot, curve, step = known_ref[0:1], known_ref[1:2], known_ref[2:3]
    z = z_ref[...]
    beta = new_dot / res_dot
    next_step = new_dot / (pre_curve + beta * (cross + beta * curve))
    out_ref[...] = step * z + next_step * (pre_ref[...] + beta * z)
    left_ref[...] = res_ref[...] - next_step * (img_ref[...] + beta * q_ref[...])


def call(body, name, outs, scratch, *args, space=pltpu.VMEM):
    return pl.pallas_call(
        body,
        name=name,
        out_shape=[jax.ShapeDtypeStruct(s, t) for s, t in outs],
        in_specs=[pl.BlockSpec(memory_space=space)] * len(args),
        out_specs=[pl.BlockSpec(memory_space=pltpu.VMEM)] * len(outs),
        scratch_shapes=scratch,
        compiler_params=pltpu.CompilerParams(vmem_limit_bytes=VMEM),
    )(*args)


def exchange(sz, msg, rows):
    blocks = msg.reshape(sz.devices, 1, rows * sz.cams)
    got = lax.all_to_all(blocks, "rows", split_axis=0, concat_axis=0, tiled=True)
    return got.reshape(sz.devices * rows, sz.cams)


def local(right_side, diag_blocks, precond, upper_blocks, block_cols, slot_of_camera):
    block, cams = right_side.shape
    lists = block_cols.shape[0]
    sz = Sizes(block, lists, cams, lax.axis_size("rows"))
    field = ((block, cams), F32)
    index = ((lists, cams), I32)
    hot_type = ((sz.entries, cams), BF16)
    upper_blocks = upper_blocks.transpose(1, 2, 0, 3)
    table = slot_of_camera.reshape(-1, cams)
    tall = pltpu.VMEM((lists * TALL, cams), F32)

    def turns(pk):
        return pltpu.VMEM((pk.rows, pk.groups, sz.devices, cams), F32)

    ins = (block_cols, table, right_side, precond, upper_blocks, diag_blocks)
    msg, own, off, chunk, z, lane, right_side, precond, upper_blocks, diag_blocks = call(
        functools.partial(first_kernel, sz), "first",
        [((sz.devices * sz.one.stride, cams), F32), index, index, index, field, hot_type]
        + [(x.shape, x.dtype) for x in ins[2:]],
        [pltpu.VMEM(x.shape, x.dtype) for x in ins[:2]]
        + [tall, tall, pltpu.SemaphoreType.DMA((len(ins),))],
        *(pltpu.with_memory_space_constraint(x, pltpu.HBM) for x in ins), space=pltpu.HBM,
    )
    got = exchange(sz, msg, sz.one.stride)
    msg, q, side, hot = call(
        functools.partial(second_kernel, sz), "second",
        [((sz.devices * sz.two.stride, cams), F32), field, field, hot_type],
        [tall] * 3 + [turns(sz.one)],
        got, right_side, z, own, off, chunk, lane, diag_blocks, precond, upper_blocks,
    )
    got = exchange(sz, msg, sz.two.stride)
    part, known, res, pre, image = call(
        functools.partial(third_kernel, sz), "third",
        [((sz.devices, cams), F32), ((3, cams), F32)] + [field] * 3,
        [tall] * 3 + [turns(sz.two)],
        got, right_side, z, q, side, chunk, lane, hot, diag_blocks, precond, upper_blocks,
    )
    parts = exchange(sz, part, 1)
    return tuple(
        call(
            fourth_kernel, "fourth", [field, field], [],
            parts, known, z, q, res, pre, image,
        )
    )


def solution(mesh):
    return jax.shard_map(
        local,
        mesh=mesh,
        in_specs=(
            P(None, "rows"),
            P(None, None, "rows"),
            P(None, None, "rows"),
            P(None, None, None, "rows"),
            P(None, "rows"),
            P(),
        ),
        out_specs=(P(None, "rows"), P(None, "rows")),
        check_vma=False,
    )
```

```python
import functools
import math

import jax
import jax.numpy as jnp
from jax import lax
from jax.experimental import pallas as pl
from jax.experimental.pallas import tpu as pltpu
from jax.sharding import PartitionSpec as P

VMEM = 24 << 20
TALL = 16
F32 = jnp.float32
BF16 = jnp.bfloat16
I32 = jnp.int32


class Packing:
    def __init__(self, values, refs, cams, skip):
        self.refs = refs
        self.cams = cams
        self.groups = cams // refs
        self.bits = refs.bit_length() - 1
        self.values = values
        self.rows = -(-values // self.groups)
        self.skip = skip
        self.stride = skip + self.rows

    def at(self, v):
        return v // self.rows, v % self.rows

    def group(self, shape):
        return lax.broadcasted_iota(I32, shape, 1) >> self.bits

    def read(self, msg_ref, r, devices):
        return msg_ref[pl.ds(self.skip + r, devices, stride=self.stride), :]


class Sizes:
    def __init__(self, block, lists, cams, devices):
        self.block = block
        self.lists = lists
        self.cams = cams
        self.devices = devices
        self.entries = lists * cams
        self.refs = self.entries // devices
        self.shift = cams.bit_length() - 1
        assert cams == 1 << self.shift and self.refs * devices == self.entries
        assert self.refs == 1 << (self.refs.bit_length() - 1) and lists <= 8
        self.one = Packing(block + 1, self.refs, cams, block)
        self.two = Packing(2 * block + 1, self.refs, cams, 0)
        self.answer = block + 1
        assert self.answer % self.two.rows == 0


def split3(x):
    hi = x.astype(BF16)
    rest = x - hi.astype(F32)
    mid = rest.astype(BF16)
    low = (rest - mid.astype(F32)).astype(BF16)
    return hi, mid, low


def stacked(x):
    parts = [p.astype(F32) for p in split3(x)]
    row = lax.broadcasted_iota(I32, (8, x.shape[1]), 0)
    tail = parts[0][8:]
    for at in (1, 2):
        tail = jnp.where(row < 2 * at, tail, pltpu.roll(parts[at][8:], 2 * at, 0))
    return jnp.concatenate([p[:8] for p in parts] + [tail], axis=0).astype(BF16)


def folded(x):
    tail = x[24:]
    tail = tail + pltpu.roll(tail, 6, 0) + pltpu.roll(tail, 4, 0)
    return jnp.concatenate([x[:8] + x[8:16] + x[16:24], tail], axis=0)


def row_sums(arrays):
    shape = arrays[0].shape
    if len(arrays) != 8 or shape[0] != 8:
        return jnp.concatenate([col_sum(x) for x in arrays], axis=0)
    row = lax.broadcasted_iota(I32, shape, 0)
    step = 4
    while step:
        low = (row & step) == 0
        arrays = [
            jnp.where(low, a, b)
            + jnp.where(low, pltpu.roll(a, 8 - step, 0), pltpu.roll(b, step, 0))
            for a, b in zip(arrays[: len(arrays) // 2], arrays[len(arrays) // 2 :])
        ]
        step //= 2
    return arrays[0]


def dot(a, b):
    return lax.dot_general(a, b, (((1,), (0,)), ((), ())), preferred_element_type=F32)


def dot_t(a, b):
    return lax.dot_general(a, b, (((1,), (1,)), ((), ())), preferred_element_type=F32)


def iota(shape, axis):
    return lax.broadcasted_iota(I32, shape, axis)


def onehot(mask):
    return jnp.where(mask, 1.0, 0.0).astype(BF16)


def hot_rows(places, shape):
    rows = iota(shape, 0).astype(F32).astype(BF16)
    same = rows == jnp.broadcast_to(places.astype(F32).astype(BF16), shape)
    return jnp.where(same, jnp.ones(shape, BF16), jnp.zeros(shape, BF16))


def col_sum(x):
    return jnp.sum(x, axis=0, keepdims=True)


def total(x):
    return jnp.sum(col_sum(x), axis=1, keepdims=True)


def eight(x):
    return sum(x[at : at + 8] for at in range(8, x.shape[0], 8)) + x[:8] if x.shape[0] > 8 else x


def block_apply(sz, blocks_ref, v):
    acc = blocks_ref[0] * v[0:1]
    for b in range(1, sz.block):
        acc = acc + blocks_ref[b] * v[b : b + 1]
    return acc


def upper_apply(sz, up_ref, gathered):
    rows = []
    for a in range(sz.block):
        acc = up_ref[a, 0] * gathered[0]
        for b in range(1, sz.block):
            acc = acc + up_ref[a, b] * gathered[b]
        rows.append(acc)
    return jnp.concatenate([row_sums(rows[:8])] + [col_sum(x) for x in rows[8:]], axis=0)


def side_by_side(ref, height):
    blocks = [ref[at : at + height, :] for at in range(0, ref.shape[0], height)]
    return jnp.concatenate(blocks, axis=1)


def bucketed(sz, v, off, up_ref, chunk, lane, val_ref):
    for b in range(sz.block):
        acc = up_ref[0, b] * v[0:1]
        for a in range(1, sz.block):
            acc = acc + up_ref[a, b] * v[a : a + 1]
        val_ref[pl.ds(b, sz.lists, stride=TALL), :] = acc
    if off is not None:
        val_ref[pl.ds(sz.block, sz.lists, stride=TALL), :] = off.astype(F32)
    parts = stacked(side_by_side(val_ref, TALL))
    where = jnp.concatenate([chunk[k : k + 1] for k in range(sz.lists)], axis=1)
    where = jnp.broadcast_to(where.astype(F32).astype(BF16), parts.shape)
    left = [
        jnp.where(where == jnp.full(parts.shape, at, BF16), parts, jnp.zeros(parts.shape, BF16))
        for at in range(sz.lists)
    ]
    res = dot_t(jnp.concatenate(left, axis=0), lane)
    height = parts.shape[0]
    return [folded(res[at * height : (at + 1) * height]) for at in range(sz.lists)]


def pack(sz, pk, value_of, msg_ref):
    group = pk.group((sz.lists, sz.cams))
    values = [value_of(v) for v in range(pk.values)]
    turned = [
        [pltpu.roll(x, t * sz.refs, 1) if t else x for t in range(pk.groups)] for x in values
    ]
    for s in range(pk.groups):
        for r in range(pk.rows):
            out = jnp.zeros((sz.lists, sz.cams), F32)
            for g in range(pk.groups):
                v = g * pk.rows + r
                if v < pk.values:
                    out = jnp.where(group == g, turned[v][(g - s) % pk.groups], out)
            at = pl.ds(s * pk.stride + pk.skip + r, sz.lists, stride=pk.groups * pk.stride)
            msg_ref[at, :] = out


def unpack(sz, pk, msg_ref, turn_ref):
    for r in range(pk.rows):
        x = pk.read(msg_ref, r, sz.devices)
        for t in range(pk.groups):
            at = (r * pk.groups + t) * sz.devices
            turn_ref[at : at + sz.devices, :] = pltpu.roll(x, t * sz.refs, 1) if t else x
    group = pk.group((sz.lists, sz.cams))
    out = []
    for v in range(pk.values):
        g, r = pk.at(v)
        value = None
        for s in range(pk.groups):
            at = (r * pk.groups + (s - g) % pk.groups) * sz.devices + s
            part = turn_ref[pl.ds(at, sz.lists, stride=pk.groups), :]
            value = part if value is None else jnp.where(group == s, part, value)
        out.append(value)
    return out


def scatter(sz, values, tall_ref, hot_ref):
    for b in range(sz.block):
        tall_ref[pl.ds(b, sz.lists, stride=TALL), :] = values[b]
    parts = stacked(side_by_side(tall_ref, TALL))
    return folded(dot_t(parts, side_by_side(hot_ref, sz.cams)))[: sz.block]


def gather(sz, msg_ref, own, off):
    c, stride = sz.cams, sz.one.stride
    high = sz.devices // 4
    left = []
    for low in range(4):
        rows = []
        for b in range(sz.block):
            x = msg_ref[pl.ds(low * stride + b, high, stride=4 * stride), :]
            rows += [p.astype(F32) for p in split3(x)]
        left.append(jnp.concatenate(rows, axis=0))
    left = jnp.concatenate(left, axis=1).astype(BF16)
    out = [[] for _ in range(sz.block)]
    zeros = jnp.zeros((c, 2 * c), BF16)
    for k in range(0, sz.lists, 2):
        pair = jnp.concatenate([off[k : k + 1], off[k + 1 : k + 2]], axis=1)
        owner = jnp.concatenate([own[k : k + 1], own[k + 1 : k + 2]], axis=1)
        hot = hot_rows(pair, (c, 2 * c))
        low = jnp.broadcast_to((owner & 3).astype(F32).astype(BF16), hot.shape)
        right = [jnp.where(low == jnp.full(hot.shape, at, BF16), hot, zeros) for at in range(4)]
        res = dot(left, jnp.concatenate(right, axis=0))
        here = iota((high, 2 * c), 0) == (owner >> 2)
        for b in range(sz.block):
            at = 3 * high * b
            x = res[at : at + high] + res[at + high : at + 2 * high] + res[at + 2 * high :][:high]
            x = jnp.where(here, x, 0.0)
            x = eight(x)
            out[b] += [x[:, :c], x[:, c:]]
    return [row_sums(x) for x in out]


def to_lists(sz, values, chunk, lane_ref, tall_ref, col_ref):
    for b in range(sz.block):
        tall_ref[pl.ds(b, sz.lists, stride=TALL), :] = values[b]
    left = jnp.concatenate(split3(tall_ref[...]), axis=1)
    right = jnp.concatenate([side_by_side(lane_ref, sz.cams)] * 3, axis=0)
    res = dot(left, right)
    for k in range(sz.lists):
        lanes = slice(k * sz.cams, (k + 1) * sz.cams)
        out = res[:TALL, lanes]
        for at in range(1, sz.lists):
            out = jnp.where(chunk[k : k + 1] == at, res[at * TALL : (at + 1) * TALL, lanes], out)
        col_ref[k * TALL : (k + 1) * TALL, :] = out
    return [col_ref[pl.ds(b, sz.lists, stride=TALL), :] for b in range(sz.block)]


def first_kernel(
    sz, cols_hbm, table_hbm, rhs_hbm, pre_hbm, up_hbm, diag_hbm,
    msg_ref, own_ref, off_ref, chunk_ref, z_ref, lane_ref, rhs_ref, pre_ref, up_ref, diag_ref,
    cols_ref, table_ref, val_ref, tall_ref, sems,
):
    pairs = (
        (cols_hbm, cols_ref), (table_hbm, table_ref), (rhs_hbm, rhs_ref), (pre_hbm, pre_ref),
        (up_hbm, up_ref), (diag_hbm, diag_ref),
    )
    copies = [pltpu.make_async_copy(a, b, sems.at[i]) for i, (a, b) in enumerate(pairs)]
    for copy in copies:
        copy.start()
    for copy in copies[:2]:
        copy.wait()
    c = sz.cams
    cols = cols_ref[...]
    table = table_ref[...]
    height = table.shape[0]
    low = cols & (c - 1)
    high = cols >> sz.shift
    left = jnp.concatenate([table >> sz.shift, table & (c - 1)], axis=0).astype(F32).astype(BF16)
    hot = jnp.concatenate([hot_rows(low[k : k + 1], (c, c)) for k in range(sz.lists)], axis=1)
    res = dot(left, hot)
    owns, offs = [], []
    for k in range(sz.lists):
        here = iota((height, c), 0) == high[k : k + 1]
        lanes = slice(k * c, (k + 1) * c)
        owns.append(eight(jnp.where(here, res[:height, lanes], 0.0)))
        offs.append(eight(jnp.where(here, res[height:, lanes], 0.0)))
    own = row_sums(owns).astype(I32)
    off = row_sums(offs).astype(I32)
    own_ref[...] = own
    off_ref[...] = off

    hots = [
        jnp.where(iota((sz.devices, c), 0) == own[k : k + 1], 1.0, 0.0) for k in range(sz.lists)
    ]
    lane = iota((c, 2 * c), 1)
    before = onehot((iota((c, 2 * c), 0) < lane) | (lane >= c))
    counts = dot(jnp.concatenate(hots, axis=0).astype(BF16), before)
    base = jnp.zeros((sz.devices, c), F32)
    places = []
    for k in range(sz.lists):
        part = counts[k * sz.devices : (k + 1) * sz.devices]
        places.append(eight(hots[k] * (part[:, :c] + base)))
        base = base + part[:, c:]
    pos = own * sz.refs + row_sums(places).astype(I32)
    chunk = pos >> sz.shift
    place = pos & (c - 1)
    chunk_ref[...] = chunk
    lanes = [hot_rows(place[k : k + 1], (c, c)) for k in range(sz.lists)]
    for k in range(sz.lists):
        lane_ref[k * c : (k + 1) * c, :] = lanes[k]
    lanes = jnp.concatenate(lanes, axis=1)

    for copy in copies[2:]:
        copy.wait()
    pk = sz.one
    z = block_apply(sz, pre_ref, rhs_ref[...])
    z_ref[...] = z
    for b in range(sz.block):
        at = pl.ds(b, sz.devices, stride=pk.stride)
        msg_ref[at, :] = jnp.broadcast_to(z[b : b + 1], (sz.devices, c))
    for at, x in enumerate(bucketed(sz, z, off, up_ref, chunk, lanes, val_ref)):
        tall_ref[at * TALL : (at + 1) * TALL, :] = x
    pack(sz, pk, lambda v: tall_ref[pl.ds(v, sz.lists, stride=TALL), :], msg_ref)


def second_kernel(
    sz, got_ref, rhs_ref, z_ref, own_ref, off_ref, chunk_ref, lane_ref, diag_ref, pre_ref, up_ref,
    msg_ref, q_ref, side_ref, hot_ref,
    val_ref, tall_ref, ans_ref, turn_ref,
):
    c = sz.cams
    b, z = rhs_ref[...], z_ref[...]
    values = unpack(sz, sz.one, got_ref, turn_ref)
    wanted = values[sz.block].astype(I32)
    for at in range(sz.lists):
        hot_ref[at * c : (at + 1) * c, :] = hot_rows(wanted[at : at + 1], (c, c))
    pushed = scatter(sz, values, val_ref, hot_ref)
    gathered = gather(sz, got_ref, own_ref[...], off_ref[...])
    side = upper_apply(sz, up_ref, gathered) + pushed
    q = block_apply(sz, diag_ref, z) + side
    w = block_apply(sz, pre_ref, q)
    q_ref[...] = q
    side_ref[...] = side
    dots = [total(b * z), total(z * q)]
    lane = iota((sz.lists, c), 1) & (sz.refs - 1)
    dot_rows = jnp.zeros((sz.lists, c), F32)
    for at, d in enumerate(dots):
        dot_rows = jnp.where(lane == at, d, dot_rows)
    tall = jnp.concatenate([w, jnp.zeros((TALL - sz.block, c), F32)], axis=0)
    answers = folded(dot(stacked(tall), side_by_side(hot_ref, c)))
    for at in range(sz.lists):
        ans_ref[at * TALL : (at + 1) * TALL, :] = answers[:, at * c : (at + 1) * c]
    lanes = side_by_side(lane_ref, c)
    for at, x in enumerate(bucketed(sz, w, None, up_ref, chunk_ref[...], lanes, val_ref)):
        tall_ref[at * TALL : (at + 1) * TALL, :] = x

    def value_of(v):
        if v < sz.block:
            return tall_ref[pl.ds(v, sz.lists, stride=TALL), :]
        if v == sz.block:
            return dot_rows
        return ans_ref[pl.ds(v - sz.answer, sz.lists, stride=TALL), :]

    pack(sz, sz.two, value_of, msg_ref)


def third_kernel(
    sz, got_ref, rhs_ref, z_ref, q_ref, side_ref, chunk_ref, lane_ref, hot_ref,
    diag_ref, pre_ref, up_ref,
    part_ref, known_ref, res_ref, dir_ref, img_ref,
    val_ref, tall_ref, col_ref, turn_ref,
):
    b, z, q = rhs_ref[...], z_ref[...], q_ref[...]
    values = unpack(sz, sz.two, got_ref, turn_ref)
    sums = col_sum(values[sz.block])
    lane = iota(sums.shape, 1) & (sz.refs - 1)
    res_dot, curve = [
        jnp.sum(jnp.where(lane == at, sums, 0.0), axis=1, keepdims=True) for at in range(2)
    ]
    step = res_dot / curve
    residual = b - step * q
    pre = block_apply(sz, pre_ref, residual)
    gathered = to_lists(
        sz, values[sz.answer :], chunk_ref[...], lane_ref, tall_ref, col_ref
    )
    pushed = scatter(sz, values, val_ref, hot_ref)
    side = side_ref[...] - step * (upper_apply(sz, up_ref, gathered) + pushed)
    image = block_apply(sz, diag_ref, pre) + side
    res_ref[...] = residual
    dir_ref[...] = pre
    img_ref[...] = image
    known = [res_dot, curve, step]
    known_ref[...] = jnp.concatenate([jnp.broadcast_to(x, (1, sz.cams)) for x in known], axis=0)
    dots = [total(residual * pre), total(pre * image), total(pre * q + z * image)]
    row = dots[2]
    lane = iota((1, sz.cams), 1) & 3
    for at in (1, 0):
        row = jnp.where(lane == at, dots[at], row)
    part_ref[...] = jnp.broadcast_to(row, part_ref.shape)


def fourth_kernel(
    part_ref, known_ref, z_ref, q_ref, res_ref, pre_ref, img_ref, out_ref, left_ref
):
    sums = col_sum(part_ref[...])
    lane = iota(sums.shape, 1)
    new_dot, pre_curve, cross = [
        jnp.sum(jnp.where(lane == at, sums, 0.0), axis=1, keepdims=True) for at in range(3)
    ]
    res_dot, curve, step = known_ref[0:1], known_ref[1:2], known_ref[2:3]
    z = z_ref[...]
    beta = new_dot / res_dot
    next_step = new_dot / (pre_curve + beta * (cross + beta * curve))
    out_ref[...] = step * z + next_step * (pre_ref[...] + beta * z)
    left_ref[...] = res_ref[...] - next_step * (img_ref[...] + beta * q_ref[...])


def call(body, name, outs, scratch, *args, space=pltpu.VMEM):
    return pl.pallas_call(
        body,
        name=name,
        out_shape=[jax.ShapeDtypeStruct(s, t) for s, t in outs],
        in_specs=[pl.BlockSpec(memory_space=space)] * len(args),
        out_specs=[pl.BlockSpec(memory_space=pltpu.VMEM)] * len(outs),
        scratch_shapes=scratch,
        compiler_params=pltpu.CompilerParams(vmem_limit_bytes=VMEM),
    )(*args)


def exchange(sz, msg, rows):
    blocks = msg.reshape(sz.devices, 1, rows * sz.cams)
    got = lax.all_to_all(blocks, "rows", split_axis=0, concat_axis=0, tiled=True)
    return got.reshape(sz.devices * rows, sz.cams)


def local(right_side, diag_blocks, precond, upper_blocks, block_cols, slot_of_camera):
    block, cams = right_side.shape
    lists = block_cols.shape[0]
    sz = Sizes(block, lists, cams, lax.axis_size("rows"))
    field = ((block, cams), F32)
    index = ((lists, cams), I32)
    hot_type = ((sz.entries, cams), BF16)
    upper_blocks = upper_blocks.transpose(1, 2, 0, 3)
    table = slot_of_camera.reshape(-1, cams)
    tall = pltpu.VMEM((lists * TALL, cams), F32)

    def turns(pk):
        return pltpu.VMEM((pk.rows * pk.groups * sz.devices, cams), F32)

    ins = (block_cols, table, right_side, precond, upper_blocks, diag_blocks)
    msg, own, off, chunk, z, lane, right_side, precond, upper_blocks, diag_blocks = call(
        functools.partial(first_kernel, sz), "first",
        [((sz.devices * sz.one.stride, cams), F32), index, index, index, field, hot_type]
        + [(x.shape, x.dtype) for x in ins[2:]],
        [pltpu.VMEM(x.shape, x.dtype) for x in ins[:2]]
        + [tall, tall, pltpu.SemaphoreType.DMA((len(ins),))],
        *(pltpu.with_memory_space_constraint(x, pltpu.HBM) for x in ins), space=pltpu.HBM,
    )
    got = exchange(sz, msg, sz.one.stride)
    msg, q, side, hot = call(
        functools.partial(second_kernel, sz), "second",
        [((sz.devices * sz.two.stride, cams), F32), field, field, hot_type],
        [tall] * 3 + [turns(sz.one)],
        got, right_side, z, own, off, chunk, lane, diag_blocks, precond, upper_blocks,
    )
    got = exchange(sz, msg, sz.two.stride)
    part, known, res, pre, image = call(
        functools.partial(third_kernel, sz), "third",
        [((sz.devices, cams), F32), ((3, cams), F32)] + [field] * 3,
        [tall] * 3 + [turns(sz.two)],
        got, right_side, z, q, side, chunk, lane, hot, diag_blocks, precond, upper_blocks,
    )
    parts = exchange(sz, part, 1)
    return tuple(
        call(
            fourth_kernel, "fourth", [field, field], [],
            parts, known, z, q, res, pre, image,
        )
    )


def solution(mesh):
    return jax.shard_map(
        local,
        mesh=mesh,
        in_specs=(
            P(None, "rows"),
            P(None, None, "rows"),
            P(None, None, "rows"),
            P(None, None, None, "rows"),
            P(None, "rows"),
            P(),
        ),
        out_specs=(P(None, "rows"), P(None, "rows")),
        check_vma=False,
    )
```

```python
import functools
import math

import jax
import jax.numpy as jnp
from jax import lax
from jax.experimental import pallas as pl
from jax.experimental.pallas import tpu as pltpu
from jax.sharding import PartitionSpec as P

VMEM = 24 << 20
TALL = 16
F32 = jnp.float32
BF16 = jnp.bfloat16
I32 = jnp.int32


class Packing:
    def __init__(self, values, refs, cams, skip):
        self.refs = refs
        self.cams = cams
        self.groups = cams // refs
        self.bits = refs.bit_length() - 1
        self.values = values
        self.rows = -(-values // self.groups)
        self.skip = skip
        self.stride = skip + self.rows

    def at(self, v):
        return v // self.rows, v % self.rows

    def group(self, shape):
        return lax.broadcasted_iota(I32, shape, 1) >> self.bits

    def read(self, msg_ref, r, devices):
        return msg_ref[pl.ds(self.skip + r, devices, stride=self.stride), :]


class Sizes:
    def __init__(self, block, lists, cams, devices):
        self.block = block
        self.lists = lists
        self.cams = cams
        self.devices = devices
        self.entries = lists * cams
        self.refs = self.entries // devices
        self.shift = cams.bit_length() - 1
        assert cams == 1 << self.shift and self.refs * devices == self.entries
        assert self.refs == 1 << (self.refs.bit_length() - 1) and lists <= 8
        self.half = (block + 1) // 2
        self.one = Packing(block + 1, self.refs, cams, self.half)
        self.two = Packing(2 * block + 1, self.refs, cams, 0)
        self.answer = block + 1
        assert self.answer % self.two.rows == 0


def split3(x):
    hi = x.astype(BF16)
    rest = x - hi.astype(F32)
    mid = rest.astype(BF16)
    low = (rest - mid.astype(F32)).astype(BF16)
    return hi, mid, low


def stacked(x):
    parts = [p.astype(F32) for p in split3(x)]
    row = lax.broadcasted_iota(I32, (8, x.shape[1]), 0)
    tail = parts[0][8:]
    for at in (1, 2):
        tail = jnp.where(row < 2 * at, tail, pltpu.roll(parts[at][8:], 2 * at, 0))
    return jnp.concatenate([p[:8] for p in parts] + [tail], axis=0).astype(BF16)


def folded(x):
    tail = x[24:]
    tail = tail + pltpu.roll(tail, 6, 0) + pltpu.roll(tail, 4, 0)
    return jnp.concatenate([x[:8] + x[8:16] + x[16:24], tail], axis=0)


def row_sums(arrays):
    shape = arrays[0].shape
    if len(arrays) != 8 or shape[0] != 8:
        return jnp.concatenate([col_sum(x) for x in arrays], axis=0)
    row = lax.broadcasted_iota(I32, shape, 0)
    step = 4
    while step:
        low = (row & step) == 0
        arrays = [
            jnp.where(low, a, b)
            + jnp.where(low, pltpu.roll(a, 8 - step, 0), pltpu.roll(b, step, 0))
            for a, b in zip(arrays[: len(arrays) // 2], arrays[len(arrays) // 2 :])
        ]
        step //= 2
    return arrays[0]


def dot(a, b):
    return lax.dot_general(a, b, (((1,), (0,)), ((), ())), preferred_element_type=F32)


def dot_t(a, b):
    return lax.dot_general(a, b, (((1,), (1,)), ((), ())), preferred_element_type=F32)


def iota(shape, axis):
    return lax.broadcasted_iota(I32, shape, axis)


def onehot(mask):
    return jnp.where(mask, 1.0, 0.0).astype(BF16)


def hot_rows(places, shape):
    rows = iota(shape, 0).astype(F32).astype(BF16)
    same = rows == jnp.broadcast_to(places.astype(F32).astype(BF16), shape)
    return jnp.where(same, jnp.ones(shape, BF16), jnp.zeros(shape, BF16))


def col_sum(x):
    return jnp.sum(x, axis=0, keepdims=True)


def total(x):
    return jnp.sum(col_sum(x), axis=1, keepdims=True)


def eight(x):
    return sum(x[at : at + 8] for at in range(8, x.shape[0], 8)) + x[:8] if x.shape[0] > 8 else x


def block_apply(sz, blocks_ref, v):
    acc = blocks_ref[0] * v[0:1]
    for b in range(1, sz.block):
        acc = acc + blocks_ref[b] * v[b : b + 1]
    return acc


def upper_apply(sz, up_ref, gathered):
    rows = []
    for a in range(sz.block):
        acc = up_ref[a, 0] * gathered[0]
        for b in range(1, sz.block):
            acc = acc + up_ref[a, b] * gathered[b]
        rows.append(acc)
    return jnp.concatenate([row_sums(rows[:8])] + [col_sum(x) for x in rows[8:]], axis=0)


def side_by_side(ref, height):
    blocks = [ref[at : at + height, :] for at in range(0, ref.shape[0], height)]
    return jnp.concatenate(blocks, axis=1)


def bucketed(sz, v, off, up_ref, chunk, lane, val_ref):
    for b in range(sz.block):
        acc = up_ref[0, b] * v[0:1]
        for a in range(1, sz.block):
            acc = acc + up_ref[a, b] * v[a : a + 1]
        val_ref[pl.ds(b, sz.lists, stride=TALL), :] = acc
    if off is not None:
        val_ref[pl.ds(sz.block, sz.lists, stride=TALL), :] = off.astype(F32)
    parts = stacked(side_by_side(val_ref, TALL))
    where = jnp.concatenate([chunk[k : k + 1] for k in range(sz.lists)], axis=1)
    where = jnp.broadcast_to(where.astype(F32).astype(BF16), parts.shape)
    left = [
        jnp.where(where == jnp.full(parts.shape, at, BF16), parts, jnp.zeros(parts.shape, BF16))
        for at in range(sz.lists)
    ]
    res = dot_t(jnp.concatenate(left, axis=0), lane)
    height = parts.shape[0]
    return [folded(res[at * height : (at + 1) * height]) for at in range(sz.lists)]


def pack(sz, pk, value_of, msg_ref):
    group = pk.group((sz.lists, sz.cams))
    values = [value_of(v) for v in range(pk.values)]
    turned = [
        [pltpu.roll(x, t * sz.refs, 1) if t else x for t in range(pk.groups)] for x in values
    ]
    for s in range(pk.groups):
        for r in range(pk.rows):
            out = jnp.zeros((sz.lists, sz.cams), F32)
            for g in range(pk.groups):
                v = g * pk.rows + r
                if v < pk.values:
                    out = jnp.where(group == g, turned[v][(g - s) % pk.groups], out)
            at = pl.ds(s * pk.stride + pk.skip + r, sz.lists, stride=pk.groups * pk.stride)
            msg_ref[at, :] = out


def unpack(sz, pk, msg_ref, turn_ref):
    for r in range(pk.rows):
        x = pk.read(msg_ref, r, sz.devices)
        for t in range(pk.groups):
            at = (r * pk.groups + t) * sz.devices
            turn_ref[at : at + sz.devices, :] = pltpu.roll(x, t * sz.refs, 1) if t else x
    group = pk.group((sz.lists, sz.cams))
    out = []
    for v in range(pk.values):
        g, r = pk.at(v)
        value = None
        for s in range(pk.groups):
            at = (r * pk.groups + (s - g) % pk.groups) * sz.devices + s
            part = turn_ref[pl.ds(at, sz.lists, stride=pk.groups), :]
            value = part if value is None else jnp.where(group == s, part, value)
        out.append(value)
    return out


def scatter(sz, values, tall_ref, hot_ref):
    for b in range(sz.block):
        tall_ref[pl.ds(b, sz.lists, stride=TALL), :] = values[b]
    parts = stacked(side_by_side(tall_ref, TALL))
    return folded(dot_t(parts, side_by_side(hot_ref, sz.cams)))[: sz.block]


def pick_owners(sz, own, off, pick_ref):
    c = sz.cams
    zeros = jnp.zeros((c, c), BF16)
    for k in range(sz.lists):
        hot = hot_rows(off[k : k + 1], (c, c))
        low = jnp.broadcast_to((own[k : k + 1] & 3).astype(F32).astype(BF16), hot.shape)
        for at in range(4):
            row = (k * 4 + at) * c
            pick_ref[row : row + c, :] = jnp.where(low == jnp.full(hot.shape, at, BF16), hot, zeros)


def gather(sz, read, count, own, pick_ref):
    c = sz.cams
    high = sz.devices // 4
    left = []
    for low in range(4):
        rows = []
        for b in range(count):
            rows += [p.astype(F32) for p in split3(read(b, low))]
        left.append(jnp.concatenate(rows, axis=0))
    left = jnp.concatenate(left, axis=1).astype(BF16)
    out = [[] for _ in range(count)]
    for k in range(0, sz.lists, 2):
        owner = jnp.concatenate([own[k : k + 1], own[k + 1 : k + 2]], axis=1)
        right = [pick_ref[at * 4 * c : (at + 1) * 4 * c, :] for at in (k, k + 1)]
        res = dot(left, jnp.concatenate(right, axis=1))
        here = iota((high, 2 * c), 0) == (owner >> 2)
        for b in range(count):
            at = 3 * high * b
            x = res[at : at + high] + res[at + high : at + 2 * high] + res[at + 2 * high :][:high]
            x = eight(jnp.where(here, x, 0.0))
            out[b] += [x[:, :c], x[:, c:]]
    return [row_sums(x) for x in out]


def to_lists(sz, values, chunk, lane_ref, tall_ref, col_ref):
    for b in range(sz.block):
        tall_ref[pl.ds(b, sz.lists, stride=TALL), :] = values[b]
    left = jnp.concatenate(split3(tall_ref[...]), axis=1)
    right = jnp.concatenate([side_by_side(lane_ref, sz.cams)] * 3, axis=0)
    res = dot(left, right)
    for k in range(sz.lists):
        lanes = slice(k * sz.cams, (k + 1) * sz.cams)
        out = res[:TALL, lanes]
        for at in range(1, sz.lists):
            out = jnp.where(chunk[k : k + 1] == at, res[at * TALL : (at + 1) * TALL, lanes], out)
        col_ref[k * TALL : (k + 1) * TALL, :] = out
    return [col_ref[pl.ds(b, sz.lists, stride=TALL), :] for b in range(sz.block)]


def first_kernel(
    sz, cols_hbm, table_hbm, rhs_hbm, pre_hbm, up_hbm, diag_hbm,
    msg_ref, own_ref, off_ref, chunk_ref, z_ref, lane_ref, rhs_ref, pre_ref, up_ref, diag_ref,
    cols_ref, table_ref, val_ref, tall_ref, sems,
):
    pairs = (
        (cols_hbm, cols_ref), (table_hbm, table_ref), (rhs_hbm, rhs_ref), (pre_hbm, pre_ref),
        (up_hbm, up_ref), (diag_hbm, diag_ref),
    )
    copies = [pltpu.make_async_copy(a, b, sems.at[i]) for i, (a, b) in enumerate(pairs)]
    for copy in copies:
        copy.start()
    for copy in copies[:2]:
        copy.wait()
    c = sz.cams
    cols = cols_ref[...]
    table = table_ref[...]
    height = table.shape[0]
    low = cols & (c - 1)
    high = cols >> sz.shift
    left = jnp.concatenate([table >> sz.shift, table & (c - 1)], axis=0).astype(F32).astype(BF16)
    hot = jnp.concatenate([hot_rows(low[k : k + 1], (c, c)) for k in range(sz.lists)], axis=1)
    res = dot(left, hot)
    owns, offs = [], []
    for k in range(sz.lists):
        here = iota((height, c), 0) == high[k : k + 1]
        lanes = slice(k * c, (k + 1) * c)
        owns.append(eight(jnp.where(here, res[:height, lanes], 0.0)))
        offs.append(eight(jnp.where(here, res[height:, lanes], 0.0)))
    own = row_sums(owns).astype(I32)
    off = row_sums(offs).astype(I32)
    own_ref[...] = own
    off_ref[...] = off

    hots = [
        jnp.where(iota((sz.devices, c), 0) == own[k : k + 1], 1.0, 0.0) for k in range(sz.lists)
    ]
    lane = iota((c, 2 * c), 1)
    before = onehot((iota((c, 2 * c), 0) < lane) | (lane >= c))
    counts = dot(jnp.concatenate(hots, axis=0).astype(BF16), before)
    base = jnp.zeros((sz.devices, c), F32)
    places = []
    for k in range(sz.lists):
        part = counts[k * sz.devices : (k + 1) * sz.devices]
        places.append(eight(hots[k] * (part[:, :c] + base)))
        base = base + part[:, c:]
    pos = own * sz.refs + row_sums(places).astype(I32)
    chunk = pos >> sz.shift
    place = pos & (c - 1)
    chunk_ref[...] = chunk
    lanes = [hot_rows(place[k : k + 1], (c, c)) for k in range(sz.lists)]
    for k in range(sz.lists):
        lane_ref[k * c : (k + 1) * c, :] = lanes[k]
    lanes = jnp.concatenate(lanes, axis=1)

    for copy in copies[2:]:
        copy.wait()
    pk = sz.one
    z = block_apply(sz, pre_ref, rhs_ref[...])
    z_ref[...] = z
    for r in range(sz.half):
        for core in range(2):
            row = r + core * (sz.block - sz.half)
            at = pl.ds(core * pk.stride + r, sz.devices // 2, stride=2 * pk.stride)
            msg_ref[at, :] = jnp.broadcast_to(z[row : row + 1], (sz.devices // 2, c))
    for at, x in enumerate(bucketed(sz, z, off, up_ref, chunk, lanes, val_ref)):
        tall_ref[at * TALL : (at + 1) * TALL, :] = x
    pack(sz, pk, lambda v: tall_ref[pl.ds(v, sz.lists, stride=TALL), :], msg_ref)


def meanwhile_kernel(
    sz, got_ref, own_ref, off_ref,
    pushed_ref, hot_ref, mine_ref, pick_ref,
    val_ref, turn_ref,
):
    c, stride = sz.cams, sz.one.stride
    own = own_ref[...]
    values = unpack(sz, sz.one, got_ref, turn_ref)
    wanted = values[sz.block].astype(I32)
    for at in range(sz.lists):
        hot_ref[at * c : (at + 1) * c, :] = hot_rows(wanted[at : at + 1], (c, c))
    pushed_ref[...] = scatter(sz, values, val_ref, hot_ref)
    pick_owners(sz, own, off_ref[...], pick_ref)

    def read(b, low):
        return got_ref[pl.ds(low * stride + b, sz.devices // 4, stride=4 * stride), :]

    for b, x in enumerate(gather(sz, read, sz.half, own, pick_ref)):
        mine_ref[b * sz.lists : (b + 1) * sz.lists, :] = x


def second_kernel(
    sz, near_ref, pushed_ref, hot_ref, mine_ref, pick_ref, rhs_ref, z_ref, own_ref, chunk_ref,
    lane_ref, diag_ref, pre_ref, up_ref,
    msg_ref, q_ref, side_ref,
    val_ref, tall_ref, ans_ref,
):
    c, stride = sz.cams, sz.one.stride
    b, z = rhs_ref[...], z_ref[...]
    pushed = pushed_ref[...]
    odd = (lax.axis_index("rows") & 1) == 1
    rest = sz.block - sz.half
    shift = sz.half - rest

    def read(row, low):
        first, later = [
            near_ref[pl.ds(low * stride + at, sz.devices // 4, stride=4 * stride), :]
            for at in (row, row + shift)
        ]
        return jnp.where(odd, first, later)

    near = gather(sz, read, rest, own_ref[...], pick_ref)
    mine = [mine_ref[at * sz.lists : (at + 1) * sz.lists, :] for at in range(sz.half)]
    gathered = [jnp.where(odd, x, y) for x, y in zip(near + mine, mine + near)]
    side = upper_apply(sz, up_ref, gathered) + pushed
    q = block_apply(sz, diag_ref, z) + side
    w = block_apply(sz, pre_ref, q)
    q_ref[...] = q
    side_ref[...] = side
    dots = [total(b * z), total(z * q)]
    lane = iota((sz.lists, c), 1) & (sz.refs - 1)
    dot_rows = jnp.zeros((sz.lists, c), F32)
    for at, d in enumerate(dots):
        dot_rows = jnp.where(lane == at, d, dot_rows)
    tall = jnp.concatenate([w, jnp.zeros((TALL - sz.block, c), F32)], axis=0)
    answers = folded(dot(stacked(tall), side_by_side(hot_ref, c)))
    for at in range(sz.lists):
        ans_ref[at * TALL : (at + 1) * TALL, :] = answers[:, at * c : (at + 1) * c]
    lanes = side_by_side(lane_ref, c)
    for at, x in enumerate(bucketed(sz, w, None, up_ref, chunk_ref[...], lanes, val_ref)):
        tall_ref[at * TALL : (at + 1) * TALL, :] = x

    def value_of(v):
        if v < sz.block:
            return tall_ref[pl.ds(v, sz.lists, stride=TALL), :]
        if v == sz.block:
            return dot_rows
        return ans_ref[pl.ds(v - sz.answer, sz.lists, stride=TALL), :]

    pack(sz, sz.two, value_of, msg_ref)


def third_kernel(
    sz, got_ref, rhs_ref, z_ref, q_ref, side_ref, chunk_ref, lane_ref, hot_ref,
    diag_ref, pre_ref, up_ref,
    part_ref, known_ref, res_ref, dir_ref, img_ref,
    val_ref, tall_ref, col_ref, turn_ref,
):
    b, z, q = rhs_ref[...], z_ref[...], q_ref[...]
    values = unpack(sz, sz.two, got_ref, turn_ref)
    sums = col_sum(values[sz.block])
    lane = iota(sums.shape, 1) & (sz.refs - 1)
    res_dot, curve = [
        jnp.sum(jnp.where(lane == at, sums, 0.0), axis=1, keepdims=True) for at in range(2)
    ]
    step = res_dot / curve
    residual = b - step * q
    pre = block_apply(sz, pre_ref, residual)
    gathered = to_lists(
        sz, values[sz.answer :], chunk_ref[...], lane_ref, tall_ref, col_ref
    )
    pushed = scatter(sz, values, val_ref, hot_ref)
    side = side_ref[...] - step * (upper_apply(sz, up_ref, gathered) + pushed)
    image = block_apply(sz, diag_ref, pre) + side
    res_ref[...] = residual
    dir_ref[...] = pre
    img_ref[...] = image
    known = [res_dot, curve, step]
    known_ref[...] = jnp.concatenate([jnp.broadcast_to(x, (1, sz.cams)) for x in known], axis=0)
    dots = [total(residual * pre), total(pre * image), total(pre * q + z * image)]
    row = dots[2]
    lane = iota((1, sz.cams), 1) & 3
    for at in (1, 0):
        row = jnp.where(lane == at, dots[at], row)
    part_ref[...] = jnp.broadcast_to(row, part_ref.shape)


def fourth_kernel(
    part_ref, known_ref, z_ref, q_ref, res_ref, pre_ref, img_ref, out_ref, left_ref
):
    sums = col_sum(part_ref[...])
    lane = iota(sums.shape, 1)
    new_dot, pre_curve, cross = [
        jnp.sum(jnp.where(lane == at, sums, 0.0), axis=1, keepdims=True) for at in range(3)
    ]
    res_dot, curve, step = known_ref[0:1], known_ref[1:2], known_ref[2:3]
    z = z_ref[...]
    beta = new_dot / res_dot
    next_step = new_dot / (pre_curve + beta * (cross + beta * curve))
    out_ref[...] = step * z + next_step * (pre_ref[...] + beta * z)
    left_ref[...] = res_ref[...] - next_step * (img_ref[...] + beta * q_ref[...])


def call(body, name, outs, scratch, *args, space=pltpu.VMEM, cost=0):
    return pl.pallas_call(
        body,
        name=name,
        out_shape=[jax.ShapeDtypeStruct(s, t) for s, t in outs],
        in_specs=[pl.BlockSpec(memory_space=space)] * len(args),
        out_specs=[pl.BlockSpec(memory_space=pltpu.VMEM)] * len(outs),
        scratch_shapes=scratch,
        compiler_params=pltpu.CompilerParams(vmem_limit_bytes=VMEM),
        cost_estimate=pl.CostEstimate(flops=cost, bytes_accessed=cost, transcendentals=0),
    )(*args)


def exchange(sz, msg, rows):
    blocks = msg.reshape(sz.devices, 1, rows * sz.cams)
    got = lax.all_to_all(blocks, "rows", split_axis=0, concat_axis=0, tiled=True)
    return got.reshape(sz.devices * rows, sz.cams)


def local(right_side, diag_blocks, precond, upper_blocks, block_cols, slot_of_camera):
    block, cams = right_side.shape
    lists = block_cols.shape[0]
    sz = Sizes(block, lists, cams, lax.axis_size("rows"))
    field = ((block, cams), F32)
    index = ((lists, cams), I32)
    hot_type = ((sz.entries, cams), BF16)
    upper_blocks = upper_blocks.transpose(1, 2, 0, 3)
    table = slot_of_camera.reshape(-1, cams)
    tall = pltpu.VMEM((lists * TALL, cams), F32)

    def turns(pk):
        return pltpu.VMEM((pk.rows * pk.groups * sz.devices, cams), F32)

    ins = (block_cols, table, right_side, precond, upper_blocks, diag_blocks)
    msg, own, off, chunk, z, lane, right_side, precond, upper_blocks, diag_blocks = call(
        functools.partial(first_kernel, sz), "first",
        [((sz.devices * sz.one.stride, cams), F32), index, index, index, field, hot_type]
        + [(x.shape, x.dtype) for x in ins[2:]],
        [pltpu.VMEM(x.shape, x.dtype) for x in ins[:2]]
        + [tall, tall, pltpu.SemaphoreType.DMA((len(ins),))],
        *(pltpu.with_memory_space_constraint(x, pltpu.HBM) for x in ins), space=pltpu.HBM,
    )
    got = exchange(sz, msg, sz.one.stride)
    cores = [(i, i ^ 1) for i in range(sz.devices)]
    near = lax.ppermute(got, "rows", cores)
    pushed, hot, mine, pick = call(
        functools.partial(meanwhile_kernel, sz), "meanwhile",
        [field, hot_type, ((sz.half * lists, cams), F32), ((4 * sz.entries, cams), BF16)],
        [tall, turns(sz.one)],
        got, own, off, cost=4_000_000,
    )
    msg, q, side = call(
        functools.partial(second_kernel, sz), "second",
        [((sz.devices * sz.two.stride, cams), F32), field, field],
        [tall] * 3,
        near, pushed, hot, mine, pick, right_side, z, own, chunk, lane, diag_blocks, precond,
        upper_blocks,
    )
    got = exchange(sz, msg, sz.two.stride)
    part, known, res, pre, image = call(
        functools.partial(third_kernel, sz), "third",
        [((sz.devices, cams), F32), ((3, cams), F32)] + [field] * 3,
        [tall] * 3 + [turns(sz.two)],
        got, right_side, z, q, side, chunk, lane, hot, diag_blocks, precond, upper_blocks,
    )
    parts = exchange(sz, part, 1)
    return tuple(
        call(
            fourth_kernel, "fourth", [field, field], [],
            parts, known, z, q, res, pre, image,
        )
    )


def solution(mesh):
    return jax.shard_map(
        local,
        mesh=mesh,
        in_specs=(
            P(None, "rows"),
            P(None, None, "rows"),
            P(None, None, "rows"),
            P(None, None, None, "rows"),
            P(None, "rows"),
            P(),
        ),
        out_specs=(P(None, "rows"), P(None, "rows")),
        check_vma=False,
    )
```

```python
import functools
import math

import jax
import jax.numpy as jnp
from jax import lax
from jax.experimental import pallas as pl
from jax.experimental.pallas import tpu as pltpu
from jax.sharding import PartitionSpec as P

VMEM = 24 << 20
TALL = 16
F32 = jnp.float32
BF16 = jnp.bfloat16
I32 = jnp.int32


class Packing:
    def __init__(self, values, refs, cams, skip):
        self.refs = refs
        self.cams = cams
        self.groups = cams // refs
        self.bits = refs.bit_length() - 1
        self.values = values
        self.rows = -(-values // self.groups)
        self.skip = skip
        self.stride = skip + self.rows

    def at(self, v):
        return v // self.rows, v % self.rows

    def group(self, shape):
        return lax.broadcasted_iota(I32, shape, 1) >> self.bits

    def read(self, msg_ref, r, devices):
        return msg_ref[pl.ds(self.skip + r, devices, stride=self.stride), :]


class Sizes:
    def __init__(self, block, lists, cams, devices):
        self.block = block
        self.lists = lists
        self.cams = cams
        self.devices = devices
        self.entries = lists * cams
        self.refs = self.entries // devices
        self.shift = cams.bit_length() - 1
        assert cams == 1 << self.shift and self.refs * devices == self.entries
        assert self.refs == 1 << (self.refs.bit_length() - 1) and lists <= 8
        self.half = (block + 1) // 2
        self.one = Packing(block + 1, self.refs, cams, self.half)
        self.two = Packing(2 * block + 1, self.refs, cams, 0)
        self.answer = block + 1
        assert self.answer % self.two.rows == 0


def split3(x):
    hi = x.astype(BF16)
    rest = x - hi.astype(F32)
    mid = rest.astype(BF16)
    low = (rest - mid.astype(F32)).astype(BF16)
    return hi, mid, low


def stacked(x):
    parts = [p.astype(F32) for p in split3(x)]
    row = lax.broadcasted_iota(I32, (8, x.shape[1]), 0)
    tail = parts[0][8:]
    for at in (1, 2):
        tail = jnp.where(row < 2 * at, tail, pltpu.roll(parts[at][8:], 2 * at, 0))
    return jnp.concatenate([p[:8] for p in parts] + [tail], axis=0).astype(BF16)


def folded(x):
    tail = x[24:]
    tail = tail + pltpu.roll(tail, 6, 0) + pltpu.roll(tail, 4, 0)
    return jnp.concatenate([x[:8] + x[8:16] + x[16:24], tail], axis=0)


def row_sums(arrays):
    shape = arrays[0].shape
    if len(arrays) != 8 or shape[0] != 8:
        return jnp.concatenate([col_sum(x) for x in arrays], axis=0)
    row = lax.broadcasted_iota(I32, shape, 0)
    step = 4
    while step:
        low = (row & step) == 0
        arrays = [
            jnp.where(low, a, b)
            + jnp.where(low, pltpu.roll(a, 8 - step, 0), pltpu.roll(b, step, 0))
            for a, b in zip(arrays[: len(arrays) // 2], arrays[len(arrays) // 2 :])
        ]
        step //= 2
    return arrays[0]


def dot(a, b):
    return lax.dot_general(a, b, (((1,), (0,)), ((), ())), preferred_element_type=F32)


def dot_t(a, b):
    return lax.dot_general(a, b, (((1,), (1,)), ((), ())), preferred_element_type=F32)


def iota(shape, axis):
    return lax.broadcasted_iota(I32, shape, axis)


def onehot(mask):
    return jnp.where(mask, 1.0, 0.0).astype(BF16)


def hot_rows(places, shape):
    rows = iota(shape, 0).astype(F32).astype(BF16)
    same = rows == jnp.broadcast_to(places.astype(F32).astype(BF16), shape)
    return jnp.where(same, jnp.ones(shape, BF16), jnp.zeros(shape, BF16))


def col_sum(x):
    return jnp.sum(x, axis=0, keepdims=True)


def total(x):
    return jnp.sum(col_sum(x), axis=1, keepdims=True)


def eight(x):
    return sum(x[at : at + 8] for at in range(8, x.shape[0], 8)) + x[:8] if x.shape[0] > 8 else x


def block_apply(sz, blocks_ref, v):
    acc = blocks_ref[0] * v[0:1]
    for b in range(1, sz.block):
        acc = acc + blocks_ref[b] * v[b : b + 1]
    return acc


def upper_apply(sz, up_ref, gathered, start=0, partial=None):
    rows = []
    for a in range(sz.block):
        acc = None if partial is None else partial[a]
        for i, x in enumerate(gathered):
            term = up_ref[a, start + i] * x
            acc = term if acc is None else acc + term
        rows.append(acc)
    return rows


def list_sums(rows):
    return jnp.concatenate([row_sums(rows[:8])] + [col_sum(x) for x in rows[8:]], axis=0)


def side_by_side(ref, height):
    blocks = [ref[at : at + height, :] for at in range(0, ref.shape[0], height)]
    return jnp.concatenate(blocks, axis=1)


def bucketed(sz, v, off, up_ref, chunk, lane, val_ref):
    for b in range(sz.block):
        acc = up_ref[0, b] * v[0:1]
        for a in range(1, sz.block):
            acc = acc + up_ref[a, b] * v[a : a + 1]
        val_ref[pl.ds(b, sz.lists, stride=TALL), :] = acc
    if off is not None:
        val_ref[pl.ds(sz.block, sz.lists, stride=TALL), :] = off.astype(F32)
    parts = stacked(side_by_side(val_ref, TALL))
    where = jnp.concatenate([chunk[k : k + 1] for k in range(sz.lists)], axis=1)
    where = jnp.broadcast_to(where.astype(F32).astype(BF16), parts.shape)
    left = [
        jnp.where(where == jnp.full(parts.shape, at, BF16), parts, jnp.zeros(parts.shape, BF16))
        for at in range(sz.lists)
    ]
    res = dot_t(jnp.concatenate(left, axis=0), lane)
    height = parts.shape[0]
    return [folded(res[at * height : (at + 1) * height]) for at in range(sz.lists)]


def pack(sz, pk, value_of, msg_ref):
    group = pk.group((sz.lists, sz.cams))
    values = [value_of(v) for v in range(pk.values)]
    turned = [
        [pltpu.roll(x, t * sz.refs, 1) if t else x for t in range(pk.groups)] for x in values
    ]
    for s in range(pk.groups):
        for r in range(pk.rows):
            out = jnp.zeros((sz.lists, sz.cams), F32)
            for g in range(pk.groups):
                v = g * pk.rows + r
                if v < pk.values:
                    out = jnp.where(group == g, turned[v][(g - s) % pk.groups], out)
            at = pl.ds(s * pk.stride + pk.skip + r, sz.lists, stride=pk.groups * pk.stride)
            msg_ref[at, :] = out


def unpack(sz, pk, msg_ref, turn_ref):
    for r in range(pk.rows):
        x = pk.read(msg_ref, r, sz.devices)
        for t in range(pk.groups):
            at = (r * pk.groups + t) * sz.devices
            turn_ref[at : at + sz.devices, :] = pltpu.roll(x, t * sz.refs, 1) if t else x
    group = pk.group((sz.lists, sz.cams))
    out = []
    for v in range(pk.values):
        g, r = pk.at(v)
        value = None
        for s in range(pk.groups):
            at = (r * pk.groups + (s - g) % pk.groups) * sz.devices + s
            part = turn_ref[pl.ds(at, sz.lists, stride=pk.groups), :]
            value = part if value is None else jnp.where(group == s, part, value)
        out.append(value)
    return out


def scatter(sz, values, tall_ref, hot_ref):
    for b in range(sz.block):
        tall_ref[pl.ds(b, sz.lists, stride=TALL), :] = values[b]
    parts = stacked(side_by_side(tall_ref, TALL))
    return folded(dot_t(parts, side_by_side(hot_ref, sz.cams)))[: sz.block]


def pick_owners(sz, own, off, pick_ref):
    c = sz.cams
    zeros = jnp.zeros((c, c), BF16)
    for k in range(sz.lists):
        hot = hot_rows(off[k : k + 1], (c, c))
        low = jnp.broadcast_to((own[k : k + 1] & 3).astype(F32).astype(BF16), hot.shape)
        for at in range(4):
            row = (k * 4 + at) * c
            pick_ref[row : row + c, :] = jnp.where(low == jnp.full(hot.shape, at, BF16), hot, zeros)


def gather(sz, read, count, own, pick_ref):
    c = sz.cams
    high = sz.devices // 4
    left = []
    for low in range(4):
        rows = []
        for b in range(count):
            rows += [p.astype(F32) for p in split3(read(b, low))]
        left.append(jnp.concatenate(rows, axis=0))
    left = jnp.concatenate(left, axis=1).astype(BF16)
    out = [[] for _ in range(count)]
    for k in range(0, sz.lists, 2):
        owner = jnp.concatenate([own[k : k + 1], own[k + 1 : k + 2]], axis=1)
        right = [pick_ref[at * 4 * c : (at + 1) * 4 * c, :] for at in (k, k + 1)]
        res = dot(left, jnp.concatenate(right, axis=1))
        here = iota((high, 2 * c), 0) == (owner >> 2)
        for b in range(count):
            at = 3 * high * b
            x = res[at : at + high] + res[at + high : at + 2 * high] + res[at + 2 * high :][:high]
            x = eight(jnp.where(here, x, 0.0))
            out[b] += [x[:, :c], x[:, c:]]
    return [row_sums(x) for x in out]


def to_lists(sz, values, chunk, lane_ref, tall_ref, col_ref):
    for b in range(sz.block):
        tall_ref[pl.ds(b, sz.lists, stride=TALL), :] = values[b]
    left = jnp.concatenate(split3(tall_ref[...]), axis=1)
    right = jnp.concatenate([side_by_side(lane_ref, sz.cams)] * 3, axis=0)
    res = dot(left, right)
    for k in range(sz.lists):
        lanes = slice(k * sz.cams, (k + 1) * sz.cams)
        out = res[:TALL, lanes]
        for at in range(1, sz.lists):
            out = jnp.where(chunk[k : k + 1] == at, res[at * TALL : (at + 1) * TALL, lanes], out)
        col_ref[k * TALL : (k + 1) * TALL, :] = out
    return [col_ref[pl.ds(b, sz.lists, stride=TALL), :] for b in range(sz.block)]


def first_kernel(
    sz, cols_hbm, table_hbm, rhs_hbm, pre_hbm, up_hbm, diag_hbm,
    msg_ref, own_ref, off_ref, chunk_ref, z_ref, lane_ref, rhs_ref, pre_ref, up_ref, diag_ref,
    cols_ref, table_ref, val_ref, tall_ref, sems,
):
    pairs = (
        (cols_hbm, cols_ref), (table_hbm, table_ref), (rhs_hbm, rhs_ref), (pre_hbm, pre_ref),
        (up_hbm, up_ref), (diag_hbm, diag_ref),
    )
    copies = [pltpu.make_async_copy(a, b, sems.at[i]) for i, (a, b) in enumerate(pairs)]
    for copy in copies:
        copy.start()
    for copy in copies[:2]:
        copy.wait()
    c = sz.cams
    cols = cols_ref[...]
    table = table_ref[...]
    height = table.shape[0]
    low = cols & (c - 1)
    high = cols >> sz.shift
    left = jnp.concatenate([table >> sz.shift, table & (c - 1)], axis=0).astype(F32).astype(BF16)
    hot = jnp.concatenate([hot_rows(low[k : k + 1], (c, c)) for k in range(sz.lists)], axis=1)
    res = dot(left, hot)
    owns, offs = [], []
    for k in range(sz.lists):
        here = iota((height, c), 0) == high[k : k + 1]
        lanes = slice(k * c, (k + 1) * c)
        owns.append(eight(jnp.where(here, res[:height, lanes], 0.0)))
        offs.append(eight(jnp.where(here, res[height:, lanes], 0.0)))
    own = row_sums(owns).astype(I32)
    off = row_sums(offs).astype(I32)
    own_ref[...] = own
    off_ref[...] = off

    hots = [
        jnp.where(iota((sz.devices, c), 0) == own[k : k + 1], 1.0, 0.0) for k in range(sz.lists)
    ]
    lane = iota((c, 2 * c), 1)
    before = onehot((iota((c, 2 * c), 0) < lane) | (lane >= c))
    counts = dot(jnp.concatenate(hots, axis=0).astype(BF16), before)
    base = jnp.zeros((sz.devices, c), F32)
    places = []
    for k in range(sz.lists):
        part = counts[k * sz.devices : (k + 1) * sz.devices]
        places.append(eight(hots[k] * (part[:, :c] + base)))
        base = base + part[:, c:]
    pos = own * sz.refs + row_sums(places).astype(I32)
    chunk = pos >> sz.shift
    place = pos & (c - 1)
    chunk_ref[...] = chunk
    lanes = [hot_rows(place[k : k + 1], (c, c)) for k in range(sz.lists)]
    for k in range(sz.lists):
        lane_ref[k * c : (k + 1) * c, :] = lanes[k]
    lanes = jnp.concatenate(lanes, axis=1)

    for copy in copies[2:]:
        copy.wait()
    pk = sz.one
    z = block_apply(sz, pre_ref, rhs_ref[...])
    z_ref[...] = z
    for r in range(sz.half):
        for core in range(2):
            row = r + core * (sz.block - sz.half)
            at = pl.ds(core * pk.stride + r, sz.devices // 2, stride=2 * pk.stride)
            msg_ref[at, :] = jnp.broadcast_to(z[row : row + 1], (sz.devices // 2, c))
    for at, x in enumerate(bucketed(sz, z, off, up_ref, chunk, lanes, val_ref)):
        tall_ref[at * TALL : (at + 1) * TALL, :] = x
    pack(sz, pk, lambda v: tall_ref[pl.ds(v, sz.lists, stride=TALL), :], msg_ref)


def meanwhile_kernel(
    sz, got_ref, own_ref, off_ref, rhs_ref, z_ref, diag_ref, up_ref,
    pushed_ref, hot_ref, mine_ref, pick_ref, part_ref, dot_ref,
    val_ref, turn_ref,
):
    c, stride = sz.cams, sz.one.stride
    own = own_ref[...]
    values = unpack(sz, sz.one, got_ref, turn_ref)
    wanted = values[sz.block].astype(I32)
    for at in range(sz.lists):
        hot_ref[at * c : (at + 1) * c, :] = hot_rows(wanted[at : at + 1], (c, c))
    pushed_ref[...] = scatter(sz, values, val_ref, hot_ref)
    pick_owners(sz, own, off_ref[...], pick_ref)

    def read(b, low):
        return got_ref[pl.ds(low * stride + b, sz.devices // 4, stride=4 * stride), :]

    start = (lax.axis_index("rows") & 1) * (sz.block - sz.half)
    mine = gather(sz, read, sz.half, own, pick_ref)
    for a, x in enumerate(upper_apply(sz, up_ref, mine, start)):
        mine_ref[a * sz.lists : (a + 1) * sz.lists, :] = x
    z = z_ref[...]
    part_ref[...] = block_apply(sz, diag_ref, z)
    dot_ref[...] = jnp.broadcast_to(total(rhs_ref[...] * z), dot_ref.shape)


def second_kernel(
    sz, near_ref, pushed_ref, hot_ref, mine_ref, pick_ref, dot_ref, z_ref, own_ref, chunk_ref,
    lane_ref, part_ref, pre_ref, up_ref,
    msg_ref, q_ref, side_ref,
    val_ref, tall_ref, ans_ref,
):
    c, stride = sz.cams, sz.one.stride
    z = z_ref[...]
    odd = (lax.axis_index("rows") & 1) == 1
    rest = sz.block - sz.half
    shift = sz.half - rest

    def read(row, low):
        first, later = [
            near_ref[pl.ds(low * stride + at, sz.devices // 4, stride=4 * stride), :]
            for at in (row, row + shift)
        ]
        return jnp.where(odd, first, later)

    near = gather(sz, read, rest, own_ref[...], pick_ref)
    mine = [mine_ref[at * sz.lists : (at + 1) * sz.lists, :] for at in range(sz.block)]
    start = (1 - (lax.axis_index("rows") & 1)) * sz.half
    upper = list_sums(upper_apply(sz, up_ref, near, start, mine))
    side = upper + pushed_ref[...]
    q = part_ref[...] + side
    w = block_apply(sz, pre_ref, q)
    q_ref[...] = q
    side_ref[...] = side
    dots = [dot_ref[...], total(z * q)]
    lane = iota((sz.lists, c), 1) & (sz.refs - 1)
    dot_rows = jnp.zeros((sz.lists, c), F32)
    for at, d in enumerate(dots):
        dot_rows = jnp.where(lane == at, d, dot_rows)
    tall = jnp.concatenate([w, jnp.zeros((TALL - sz.block, c), F32)], axis=0)
    answers = folded(dot(stacked(tall), side_by_side(hot_ref, c)))
    for at in range(sz.lists):
        ans_ref[at * TALL : (at + 1) * TALL, :] = answers[:, at * c : (at + 1) * c]
    lanes = side_by_side(lane_ref, c)
    for at, x in enumerate(bucketed(sz, w, None, up_ref, chunk_ref[...], lanes, val_ref)):
        tall_ref[at * TALL : (at + 1) * TALL, :] = x

    def value_of(v):
        if v < sz.block:
            return tall_ref[pl.ds(v, sz.lists, stride=TALL), :]
        if v == sz.block:
            return dot_rows
        return ans_ref[pl.ds(v - sz.answer, sz.lists, stride=TALL), :]

    pack(sz, sz.two, value_of, msg_ref)


def third_kernel(
    sz, got_ref, rhs_ref, z_ref, q_ref, side_ref, chunk_ref, lane_ref, hot_ref,
    diag_ref, pre_ref, up_ref,
    part_ref, known_ref, res_ref, dir_ref, img_ref,
    val_ref, tall_ref, col_ref, turn_ref,
):
    b, z, q = rhs_ref[...], z_ref[...], q_ref[...]
    values = unpack(sz, sz.two, got_ref, turn_ref)
    sums = col_sum(values[sz.block])
    lane = iota(sums.shape, 1) & (sz.refs - 1)
    res_dot, curve = [
        jnp.sum(jnp.where(lane == at, sums, 0.0), axis=1, keepdims=True) for at in range(2)
    ]
    step = res_dot / curve
    residual = b - step * q
    pre = block_apply(sz, pre_ref, residual)
    gathered = to_lists(
        sz, values[sz.answer :], chunk_ref[...], lane_ref, tall_ref, col_ref
    )
    pushed = scatter(sz, values, val_ref, hot_ref)
    side = side_ref[...] - step * (list_sums(upper_apply(sz, up_ref, gathered)) + pushed)
    image = block_apply(sz, diag_ref, pre) + side
    res_ref[...] = residual
    dir_ref[...] = pre
    img_ref[...] = image
    known = [res_dot, curve, step]
    known_ref[...] = jnp.concatenate([jnp.broadcast_to(x, (1, sz.cams)) for x in known], axis=0)
    dots = [total(residual * pre), total(pre * image), total(pre * q + z * image)]
    row = dots[2]
    lane = iota((1, sz.cams), 1) & 3
    for at in (1, 0):
        row = jnp.where(lane == at, dots[at], row)
    part_ref[...] = jnp.broadcast_to(row, part_ref.shape)


def fourth_kernel(
    part_ref, known_ref, z_ref, q_ref, res_ref, pre_ref, img_ref, out_ref, left_ref
):
    sums = col_sum(part_ref[...])
    lane = iota(sums.shape, 1)
    new_dot, pre_curve, cross = [
        jnp.sum(jnp.where(lane == at, sums, 0.0), axis=1, keepdims=True) for at in range(3)
    ]
    res_dot, curve, step = known_ref[0:1], known_ref[1:2], known_ref[2:3]
    z = z_ref[...]
    beta = new_dot / res_dot
    next_step = new_dot / (pre_curve + beta * (cross + beta * curve))
    out_ref[...] = step * z + next_step * (pre_ref[...] + beta * z)
    left_ref[...] = res_ref[...] - next_step * (img_ref[...] + beta * q_ref[...])


def call(body, name, outs, scratch, *args, space=pltpu.VMEM, cost=0):
    return pl.pallas_call(
        body,
        name=name,
        out_shape=[jax.ShapeDtypeStruct(s, t) for s, t in outs],
        in_specs=[pl.BlockSpec(memory_space=space)] * len(args),
        out_specs=[pl.BlockSpec(memory_space=pltpu.VMEM)] * len(outs),
        scratch_shapes=scratch,
        compiler_params=pltpu.CompilerParams(vmem_limit_bytes=VMEM),
        cost_estimate=pl.CostEstimate(flops=cost, bytes_accessed=cost, transcendentals=0),
    )(*args)


def exchange(sz, msg, rows):
    blocks = msg.reshape(sz.devices, 1, rows * sz.cams)
    got = lax.all_to_all(blocks, "rows", split_axis=0, concat_axis=0, tiled=True)
    return got.reshape(sz.devices * rows, sz.cams)


def local(right_side, diag_blocks, precond, upper_blocks, block_cols, slot_of_camera):
    block, cams = right_side.shape
    lists = block_cols.shape[0]
    sz = Sizes(block, lists, cams, lax.axis_size("rows"))
    field = ((block, cams), F32)
    index = ((lists, cams), I32)
    hot_type = ((sz.entries, cams), BF16)
    upper_blocks = upper_blocks.transpose(1, 2, 0, 3)
    table = slot_of_camera.reshape(-1, cams)
    tall = pltpu.VMEM((lists * TALL, cams), F32)

    def turns(pk):
        return pltpu.VMEM((pk.rows * pk.groups * sz.devices, cams), F32)

    ins = (block_cols, table, right_side, precond, upper_blocks, diag_blocks)
    msg, own, off, chunk, z, lane, right_side, precond, upper_blocks, diag_blocks = call(
        functools.partial(first_kernel, sz), "first",
        [((sz.devices * sz.one.stride, cams), F32), index, index, index, field, hot_type]
        + [(x.shape, x.dtype) for x in ins[2:]],
        [pltpu.VMEM(x.shape, x.dtype) for x in ins[:2]]
        + [tall, tall, pltpu.SemaphoreType.DMA((len(ins),))],
        *(pltpu.with_memory_space_constraint(x, pltpu.HBM) for x in ins), space=pltpu.HBM,
    )
    got = exchange(sz, msg, sz.one.stride)
    cores = [(i, i ^ 1) for i in range(sz.devices)]
    near = lax.ppermute(got, "rows", cores)
    pushed, hot, mine, pick, part, bz = call(
        functools.partial(meanwhile_kernel, sz), "meanwhile",
        [field, hot_type, ((block * lists, cams), F32), ((4 * sz.entries, cams), BF16),
         field, ((1, cams), F32)],
        [tall, turns(sz.one)],
        got, own, off, right_side, z, diag_blocks, upper_blocks, cost=4_000_000,
    )
    msg, q, side = call(
        functools.partial(second_kernel, sz), "second",
        [((sz.devices * sz.two.stride, cams), F32), field, field],
        [tall] * 3,
        near, pushed, hot, mine, pick, bz, z, own, chunk, lane, part, precond,
        upper_blocks,
    )
    got = exchange(sz, msg, sz.two.stride)
    part, known, res, pre, image = call(
        functools.partial(third_kernel, sz), "third",
        [((sz.devices, cams), F32), ((3, cams), F32)] + [field] * 3,
        [tall] * 3 + [turns(sz.two)],
        got, right_side, z, q, side, chunk, lane, hot, diag_blocks, precond, upper_blocks,
    )
    parts = exchange(sz, part, 1)
    return tuple(
        call(
            fourth_kernel, "fourth", [field, field], [],
            parts, known, z, q, res, pre, image,
        )
    )


def solution(mesh):
    return jax.shard_map(
        local,
        mesh=mesh,
        in_specs=(
            P(None, "rows"),
            P(None, None, "rows"),
            P(None, None, "rows"),
            P(None, None, None, "rows"),
            P(None, "rows"),
            P(),
        ),
        out_specs=(P(None, "rows"), P(None, "rows")),
        check_vma=False,
    )
```

```python
import functools
import math

import jax
import jax.numpy as jnp
from jax import lax
from jax.experimental import pallas as pl
from jax.experimental.pallas import tpu as pltpu
from jax.sharding import PartitionSpec as P

VMEM = 24 << 20
TALL = 16
F32 = jnp.float32
BF16 = jnp.bfloat16
I32 = jnp.int32


class Packing:
    def __init__(self, values, refs, cams, skip):
        self.refs = refs
        self.cams = cams
        self.groups = cams // refs
        self.bits = refs.bit_length() - 1
        self.values = values
        self.rows = -(-values // self.groups)
        self.skip = skip
        self.stride = skip + self.rows

    def at(self, v):
        return v // self.rows, v % self.rows

    def group(self, shape):
        return lax.broadcasted_iota(I32, shape, 1) >> self.bits

    def read(self, msg_ref, r, devices):
        return msg_ref[pl.ds(self.skip + r, devices, stride=self.stride), :]


class Sizes:
    def __init__(self, block, lists, cams, devices):
        self.block = block
        self.lists = lists
        self.cams = cams
        self.devices = devices
        self.entries = lists * cams
        self.refs = self.entries // devices
        self.shift = cams.bit_length() - 1
        assert cams == 1 << self.shift and self.refs * devices == self.entries
        assert self.refs == 1 << (self.refs.bit_length() - 1) and lists <= 8
        self.half = (block + 1) // 2
        self.one = Packing(block + 1, self.refs, cams, self.half)
        self.two = Packing(2 * block + 1, self.refs, cams, 0)
        self.answer = block + 1
        assert self.answer % self.two.rows == 0


def split3(x):
    hi = x.astype(BF16)
    rest = x - hi.astype(F32)
    mid = rest.astype(BF16)
    low = (rest - mid.astype(F32)).astype(BF16)
    return hi, mid, low


def stacked(x):
    parts = [p.astype(F32) for p in split3(x)]
    row = lax.broadcasted_iota(I32, (8, x.shape[1]), 0)
    tail = parts[0][8:]
    for at in (1, 2):
        tail = jnp.where(row < 2 * at, tail, pltpu.roll(parts[at][8:], 2 * at, 0))
    return jnp.concatenate([p[:8] for p in parts] + [tail], axis=0).astype(BF16)


def folded(x):
    tail = x[24:]
    tail = tail + pltpu.roll(tail, 6, 0) + pltpu.roll(tail, 4, 0)
    return jnp.concatenate([x[:8] + x[8:16] + x[16:24], tail], axis=0)


def row_sums(arrays):
    shape = arrays[0].shape
    if len(arrays) != 8 or shape[0] != 8:
        return jnp.concatenate([col_sum(x) for x in arrays], axis=0)
    row = lax.broadcasted_iota(I32, shape, 0)
    step = 4
    while step:
        low = (row & step) == 0
        arrays = [
            jnp.where(low, a, b)
            + jnp.where(low, pltpu.roll(a, 8 - step, 0), pltpu.roll(b, step, 0))
            for a, b in zip(arrays[: len(arrays) // 2], arrays[len(arrays) // 2 :])
        ]
        step //= 2
    return arrays[0]


def dot(a, b):
    return lax.dot_general(a, b, (((1,), (0,)), ((), ())), preferred_element_type=F32)


def dot_t(a, b):
    return lax.dot_general(a, b, (((1,), (1,)), ((), ())), preferred_element_type=F32)


def iota(shape, axis):
    return lax.broadcasted_iota(I32, shape, axis)


def onehot(mask):
    return jnp.where(mask, 1.0, 0.0).astype(BF16)


def hot_rows(places, shape):
    rows = iota(shape, 0).astype(F32).astype(BF16)
    same = rows == jnp.broadcast_to(places.astype(F32).astype(BF16), shape)
    return jnp.where(same, jnp.ones(shape, BF16), jnp.zeros(shape, BF16))


def col_sum(x):
    return jnp.sum(x, axis=0, keepdims=True)


def total(x):
    return jnp.sum(col_sum(x), axis=1, keepdims=True)


def eight(x):
    return sum(x[at : at + 8] for at in range(8, x.shape[0], 8)) + x[:8] if x.shape[0] > 8 else x


def block_apply(sz, blocks_ref, v):
    acc = blocks_ref[0] * v[0:1]
    for b in range(1, sz.block):
        acc = acc + blocks_ref[b] * v[b : b + 1]
    return acc


def upper_apply(sz, up_ref, gathered, start=0, partial=None):
    rows = []
    for a in range(sz.block):
        acc = None if partial is None else partial[a]
        for i, x in enumerate(gathered):
            term = up_ref[a, start + i] * x
            acc = term if acc is None else acc + term
        rows.append(acc)
    return rows


def list_sums(rows):
    return jnp.concatenate([row_sums(rows[:8])] + [col_sum(x) for x in rows[8:]], axis=0)


def side_by_side(ref, height):
    blocks = [ref[at : at + height, :] for at in range(0, ref.shape[0], height)]
    return jnp.concatenate(blocks, axis=1)


def bucketed(sz, v, off, up_ref, chunk, lane, val_ref):
    for b in range(sz.block):
        acc = up_ref[0, b] * v[0:1]
        for a in range(1, sz.block):
            acc = acc + up_ref[a, b] * v[a : a + 1]
        val_ref[pl.ds(b, sz.lists, stride=TALL), :] = acc
    if off is not None:
        val_ref[pl.ds(sz.block, sz.lists, stride=TALL), :] = off.astype(F32)
    parts = stacked(side_by_side(val_ref, TALL))
    where = jnp.concatenate([chunk[k : k + 1] for k in range(sz.lists)], axis=1)
    where = jnp.broadcast_to(where.astype(F32).astype(BF16), parts.shape)
    left = [
        jnp.where(where == jnp.full(parts.shape, at, BF16), parts, jnp.zeros(parts.shape, BF16))
        for at in range(sz.lists)
    ]
    res = dot_t(jnp.concatenate(left, axis=0), lane)
    height = parts.shape[0]
    return [folded(res[at * height : (at + 1) * height]) for at in range(sz.lists)]


def pack(sz, pk, value_of, msg_ref):
    group = pk.group((sz.lists, sz.cams))
    values = [value_of(v) for v in range(pk.values)]
    turned = [
        [pltpu.roll(x, t * sz.refs, 1) if t else x for t in range(pk.groups)] for x in values
    ]
    for s in range(pk.groups):
        for r in range(pk.rows):
            out = jnp.zeros((sz.lists, sz.cams), F32)
            for g in range(pk.groups):
                v = g * pk.rows + r
                if v < pk.values:
                    out = jnp.where(group == g, turned[v][(g - s) % pk.groups], out)
            at = pl.ds(s * pk.stride + pk.skip + r, sz.lists, stride=pk.groups * pk.stride)
            msg_ref[at, :] = out


def unpack(sz, pk, msg_ref, turn_ref):
    for r in range(pk.rows):
        x = pk.read(msg_ref, r, sz.devices)
        for t in range(pk.groups):
            at = (r * pk.groups + t) * sz.devices
            turn_ref[at : at + sz.devices, :] = pltpu.roll(x, t * sz.refs, 1) if t else x
    group = pk.group((sz.lists, sz.cams))
    out = []
    for v in range(pk.values):
        g, r = pk.at(v)
        value = None
        for s in range(pk.groups):
            at = (r * pk.groups + (s - g) % pk.groups) * sz.devices + s
            part = turn_ref[pl.ds(at, sz.lists, stride=pk.groups), :]
            value = part if value is None else jnp.where(group == s, part, value)
        out.append(value)
    return out


def scatter(sz, values, tall_ref, hot_ref):
    for b in range(sz.block):
        tall_ref[pl.ds(b, sz.lists, stride=TALL), :] = values[b]
    parts = stacked(side_by_side(tall_ref, TALL))
    return folded(dot_t(parts, side_by_side(hot_ref, sz.cams)))[: sz.block]


def pick_owners(sz, own, off, pick_ref):
    c = sz.cams
    zeros = jnp.zeros((c, c), BF16)
    for k in range(sz.lists):
        hot = hot_rows(off[k : k + 1], (c, c))
        low = jnp.broadcast_to((own[k : k + 1] & 3).astype(F32).astype(BF16), hot.shape)
        for at in range(4):
            row = (k * 4 + at) * c
            pick_ref[row : row + c, :] = jnp.where(low == jnp.full(hot.shape, at, BF16), hot, zeros)


def gather(sz, read, count, own, pick_ref):
    c = sz.cams
    high = sz.devices // 4
    left = []
    for low in range(4):
        rows = []
        for b in range(count):
            rows += [p.astype(F32) for p in split3(read(b, low))]
        left.append(jnp.concatenate(rows, axis=0))
    left = jnp.concatenate(left, axis=1).astype(BF16)
    out = [[] for _ in range(count)]
    for k in range(0, sz.lists, 2):
        owner = jnp.concatenate([own[k : k + 1], own[k + 1 : k + 2]], axis=1)
        right = [pick_ref[at * 4 * c : (at + 1) * 4 * c, :] for at in (k, k + 1)]
        res = dot(left, jnp.concatenate(right, axis=1))
        here = iota((high, 2 * c), 0) == (owner >> 2)
        for b in range(count):
            at = 3 * high * b
            x = res[at : at + high] + res[at + high : at + 2 * high] + res[at + 2 * high :][:high]
            x = eight(jnp.where(here, x, 0.0))
            out[b] += [x[:, :c], x[:, c:]]
    return [row_sums(x) for x in out]


def to_lists(sz, values, chunk, lane_ref, tall_ref, col_ref):
    for b in range(sz.block):
        tall_ref[pl.ds(b, sz.lists, stride=TALL), :] = values[b]
    left = jnp.concatenate(split3(tall_ref[...]), axis=1)
    right = jnp.concatenate([side_by_side(lane_ref, sz.cams)] * 3, axis=0)
    res = dot(left, right)
    for k in range(sz.lists):
        lanes = slice(k * sz.cams, (k + 1) * sz.cams)
        out = res[:TALL, lanes]
        for at in range(1, sz.lists):
            out = jnp.where(chunk[k : k + 1] == at, res[at * TALL : (at + 1) * TALL, lanes], out)
        col_ref[k * TALL : (k + 1) * TALL, :] = out
    return [col_ref[pl.ds(b, sz.lists, stride=TALL), :] for b in range(sz.block)]


def first_kernel(
    sz, cols_hbm, table_hbm, rhs_hbm, pre_hbm, up_hbm, diag_hbm,
    msg_ref, own_ref, off_ref, chunk_ref, z_ref, lane_ref, rhs_ref, pre_ref, up_ref, diag_ref,
    cols_ref, table_ref, val_ref, tall_ref, sems,
):
    pairs = (
        (cols_hbm, cols_ref), (table_hbm, table_ref), (rhs_hbm, rhs_ref), (pre_hbm, pre_ref),
        (up_hbm, up_ref), (diag_hbm, diag_ref),
    )
    copies = [pltpu.make_async_copy(a, b, sems.at[i]) for i, (a, b) in enumerate(pairs)]
    for copy in copies:
        copy.start()
    for copy in copies[:2]:
        copy.wait()
    c = sz.cams
    cols = cols_ref[...]
    table = table_ref[...]
    height = table.shape[0]
    low = cols & (c - 1)
    high = cols >> sz.shift
    left = jnp.concatenate([table >> sz.shift, table & (c - 1)], axis=0).astype(F32).astype(BF16)
    hot = jnp.concatenate([hot_rows(low[k : k + 1], (c, c)) for k in range(sz.lists)], axis=1)
    res = dot(left, hot)
    owns, offs = [], []
    for k in range(sz.lists):
        here = iota((height, c), 0) == high[k : k + 1]
        lanes = slice(k * c, (k + 1) * c)
        owns.append(eight(jnp.where(here, res[:height, lanes], 0.0)))
        offs.append(eight(jnp.where(here, res[height:, lanes], 0.0)))
    own = row_sums(owns).astype(I32)
    off = row_sums(offs).astype(I32)
    own_ref[...] = own
    off_ref[...] = off

    hots = [
        jnp.where(iota((sz.devices, c), 0) == own[k : k + 1], 1.0, 0.0) for k in range(sz.lists)
    ]
    lane = iota((c, 2 * c), 1)
    before = onehot((iota((c, 2 * c), 0) < lane) | (lane >= c))
    counts = dot(jnp.concatenate(hots, axis=0).astype(BF16), before)
    base = jnp.zeros((sz.devices, c), F32)
    places = []
    for k in range(sz.lists):
        part = counts[k * sz.devices : (k + 1) * sz.devices]
        places.append(eight(hots[k] * (part[:, :c] + base)))
        base = base + part[:, c:]
    pos = own * sz.refs + row_sums(places).astype(I32)
    chunk = pos >> sz.shift
    place = pos & (c - 1)
    chunk_ref[...] = chunk
    lanes = [hot_rows(place[k : k + 1], (c, c)) for k in range(sz.lists)]
    for k in range(sz.lists):
        lane_ref[k * c : (k + 1) * c, :] = lanes[k]
    lanes = jnp.concatenate(lanes, axis=1)

    for copy in copies[2:]:
        copy.wait()
    pk = sz.one
    z = block_apply(sz, pre_ref, rhs_ref[...])
    z_ref[...] = z
    for r in range(sz.half):
        for core in range(2):
            row = r + core * (sz.block - sz.half)
            at = pl.ds(core * pk.stride + r, sz.devices // 2, stride=2 * pk.stride)
            msg_ref[at, :] = jnp.broadcast_to(z[row : row + 1], (sz.devices // 2, c))
    for at, x in enumerate(bucketed(sz, z, off, up_ref, chunk, lanes, val_ref)):
        tall_ref[at * TALL : (at + 1) * TALL, :] = x
    pack(sz, pk, lambda v: tall_ref[pl.ds(v, sz.lists, stride=TALL), :], msg_ref)


def meanwhile_kernel(
    sz, got_ref, own_ref, off_ref, rhs_ref, z_ref, diag_ref, up_ref,
    pushed_ref, hot_ref, mine_ref, pick_ref, part_ref, dot_ref,
    val_ref, turn_ref,
):
    c, stride = sz.cams, sz.one.stride
    own = own_ref[...]
    values = unpack(sz, sz.one, got_ref, turn_ref)
    wanted = values[sz.block].astype(I32)
    for at in range(sz.lists):
        hot_ref[at * c : (at + 1) * c, :] = hot_rows(wanted[at : at + 1], (c, c))
    pushed_ref[...] = scatter(sz, values, val_ref, hot_ref)
    pick_owners(sz, own, off_ref[...], pick_ref)

    def read(b, low):
        return got_ref[pl.ds(low * stride + b, sz.devices // 4, stride=4 * stride), :]

    start = (lax.axis_index("rows") & 1) * (sz.block - sz.half)
    mine = gather(sz, read, sz.half, own, pick_ref)
    for a, x in enumerate(upper_apply(sz, up_ref, mine, start)):
        mine_ref[a * sz.lists : (a + 1) * sz.lists, :] = x
    z = z_ref[...]
    part_ref[...] = block_apply(sz, diag_ref, z)
    dot_ref[...] = jnp.broadcast_to(total(rhs_ref[...] * z), dot_ref.shape)


def second_kernel(
    sz, near_ref, pushed_ref, hot_ref, mine_ref, pick_ref, dot_ref, z_ref, own_ref, chunk_ref,
    lane_ref, part_ref, pre_ref, up_ref,
    msg_ref, q_ref, side_ref,
    val_ref, tall_ref, ans_ref,
):
    c, stride = sz.cams, sz.one.stride
    z = z_ref[...]
    even = 1 - (lax.axis_index("rows") & 1)
    rest = sz.block - sz.half
    skip = even * (sz.half - rest)

    def read(row, low):
        return near_ref[pl.ds(low * stride + row + skip, sz.devices // 4, stride=4 * stride), :]

    near = gather(sz, read, rest, own_ref[...], pick_ref)
    mine = [mine_ref[at * sz.lists : (at + 1) * sz.lists, :] for at in range(sz.block)]
    start = even * sz.half
    upper = list_sums(upper_apply(sz, up_ref, near, start, mine))
    side = upper + pushed_ref[...]
    q = part_ref[...] + side
    w = block_apply(sz, pre_ref, q)
    q_ref[...] = q
    side_ref[...] = side
    dots = [dot_ref[...], total(z * q)]
    lane = iota((sz.lists, c), 1) & (sz.refs - 1)
    dot_rows = jnp.zeros((sz.lists, c), F32)
    for at, d in enumerate(dots):
        dot_rows = jnp.where(lane == at, d, dot_rows)
    tall = jnp.concatenate([w, jnp.zeros((TALL - sz.block, c), F32)], axis=0)
    answers = folded(dot(stacked(tall), side_by_side(hot_ref, c)))
    for at in range(sz.lists):
        ans_ref[at * TALL : (at + 1) * TALL, :] = answers[:, at * c : (at + 1) * c]
    lanes = side_by_side(lane_ref, c)
    for at, x in enumerate(bucketed(sz, w, None, up_ref, chunk_ref[...], lanes, val_ref)):
        tall_ref[at * TALL : (at + 1) * TALL, :] = x

    def value_of(v):
        if v < sz.block:
            return tall_ref[pl.ds(v, sz.lists, stride=TALL), :]
        if v == sz.block:
            return dot_rows
        return ans_ref[pl.ds(v - sz.answer, sz.lists, stride=TALL), :]

    pack(sz, sz.two, value_of, msg_ref)


def third_kernel(
    sz, got_ref, rhs_ref, z_ref, q_ref, side_ref, chunk_ref, lane_ref, hot_ref,
    diag_ref, pre_ref, up_ref,
    part_ref, known_ref, res_ref, dir_ref, img_ref,
    val_ref, tall_ref, col_ref, turn_ref,
):
    b, z, q = rhs_ref[...], z_ref[...], q_ref[...]
    values = unpack(sz, sz.two, got_ref, turn_ref)
    sums = col_sum(values[sz.block])
    lane = iota(sums.shape, 1) & (sz.refs - 1)
    res_dot, curve = [
        jnp.sum(jnp.where(lane == at, sums, 0.0), axis=1, keepdims=True) for at in range(2)
    ]
    step = res_dot / curve
    residual = b - step * q
    pre = block_apply(sz, pre_ref, residual)
    gathered = to_lists(
        sz, values[sz.answer :], chunk_ref[...], lane_ref, tall_ref, col_ref
    )
    pushed = scatter(sz, values, val_ref, hot_ref)
    side = side_ref[...] - step * (list_sums(upper_apply(sz, up_ref, gathered)) + pushed)
    image = block_apply(sz, diag_ref, pre) + side
    res_ref[...] = residual
    dir_ref[...] = pre
    img_ref[...] = image
    known = [res_dot, curve, step]
    known_ref[...] = jnp.concatenate([jnp.broadcast_to(x, (1, sz.cams)) for x in known], axis=0)
    dots = [total(residual * pre), total(pre * image), total(pre * q + z * image)]
    row = dots[2]
    lane = iota((1, sz.cams), 1) & 3
    for at in (1, 0):
        row = jnp.where(lane == at, dots[at], row)
    part_ref[...] = jnp.broadcast_to(row, part_ref.shape)


def fourth_kernel(
    part_ref, known_ref, z_ref, q_ref, res_ref, pre_ref, img_ref, out_ref, left_ref
):
    sums = col_sum(part_ref[...])
    lane = iota(sums.shape, 1)
    new_dot, pre_curve, cross = [
        jnp.sum(jnp.where(lane == at, sums, 0.0), axis=1, keepdims=True) for at in range(3)
    ]
    res_dot, curve, step = known_ref[0:1], known_ref[1:2], known_ref[2:3]
    z = z_ref[...]
    beta = new_dot / res_dot
    next_step = new_dot / (pre_curve + beta * (cross + beta * curve))
    out_ref[...] = step * z + next_step * (pre_ref[...] + beta * z)
    left_ref[...] = res_ref[...] - next_step * (img_ref[...] + beta * q_ref[...])


def call(body, name, outs, scratch, *args, space=pltpu.VMEM, cost=0):
    return pl.pallas_call(
        body,
        name=name,
        out_shape=[jax.ShapeDtypeStruct(s, t) for s, t in outs],
        in_specs=[pl.BlockSpec(memory_space=space)] * len(args),
        out_specs=[pl.BlockSpec(memory_space=pltpu.VMEM)] * len(outs),
        scratch_shapes=scratch,
        compiler_params=pltpu.CompilerParams(vmem_limit_bytes=VMEM),
        cost_estimate=pl.CostEstimate(flops=cost, bytes_accessed=cost, transcendentals=0),
    )(*args)


def exchange(sz, msg, rows):
    blocks = msg.reshape(sz.devices, 1, rows * sz.cams)
    got = lax.all_to_all(blocks, "rows", split_axis=0, concat_axis=0, tiled=True)
    return got.reshape(sz.devices * rows, sz.cams)


def local(right_side, diag_blocks, precond, upper_blocks, block_cols, slot_of_camera):
    block, cams = right_side.shape
    lists = block_cols.shape[0]
    sz = Sizes(block, lists, cams, lax.axis_size("rows"))
    field = ((block, cams), F32)
    index = ((lists, cams), I32)
    hot_type = ((sz.entries, cams), BF16)
    upper_blocks = upper_blocks.transpose(1, 2, 0, 3)
    table = slot_of_camera.reshape(-1, cams)
    tall = pltpu.VMEM((lists * TALL, cams), F32)

    def turns(pk):
        return pltpu.VMEM((pk.rows * pk.groups * sz.devices, cams), F32)

    ins = (block_cols, table, right_side, precond, upper_blocks, diag_blocks)
    msg, own, off, chunk, z, lane, right_side, precond, upper_blocks, diag_blocks = call(
        functools.partial(first_kernel, sz), "first",
        [((sz.devices * sz.one.stride, cams), F32), index, index, index, field, hot_type]
        + [(x.shape, x.dtype) for x in ins[2:]],
        [pltpu.VMEM(x.shape, x.dtype) for x in ins[:2]]
        + [tall, tall, pltpu.SemaphoreType.DMA((len(ins),))],
        *(pltpu.with_memory_space_constraint(x, pltpu.HBM) for x in ins), space=pltpu.HBM,
    )
    got = exchange(sz, msg, sz.one.stride)
    cores = [(i, i ^ 1) for i in range(sz.devices)]
    near = lax.ppermute(got, "rows", cores)
    pushed, hot, mine, pick, part, bz = call(
        functools.partial(meanwhile_kernel, sz), "meanwhile",
        [field, hot_type, ((block * lists, cams), F32), ((4 * sz.entries, cams), BF16),
         field, ((1, cams), F32)],
        [tall, turns(sz.one)],
        got, own, off, right_side, z, diag_blocks, upper_blocks, cost=4_000_000,
    )
    msg, q, side = call(
        functools.partial(second_kernel, sz), "second",
        [((sz.devices * sz.two.stride, cams), F32), field, field],
        [tall] * 3,
        near, pushed, hot, mine, pick, bz, z, own, chunk, lane, part, precond,
        upper_blocks,
    )
    got = exchange(sz, msg, sz.two.stride)
    part, known, res, pre, image = call(
        functools.partial(third_kernel, sz), "third",
        [((sz.devices, cams), F32), ((3, cams), F32)] + [field] * 3,
        [tall] * 3 + [turns(sz.two)],
        got, right_side, z, q, side, chunk, lane, hot, diag_blocks, precond, upper_blocks,
    )
    parts = exchange(sz, part, 1)
    return tuple(
        call(
            fourth_kernel, "fourth", [field, field], [],
            parts, known, z, q, res, pre, image,
        )
    )


def solution(mesh):
    return jax.shard_map(
        local,
        mesh=mesh,
        in_specs=(
            P(None, "rows"),
            P(None, None, "rows"),
            P(None, None, "rows"),
            P(None, None, None, "rows"),
            P(None, "rows"),
            P(),
        ),
        out_specs=(P(None, "rows"), P(None, "rows")),
        check_vma=False,
    )
```
